64 devices in a mesh: stage: 4 (over x, y), data: 16 (over z, core).
Axes of the slice: x: 2, y: 2, z: 8, core: 2. Of those that a mesh axis runs over, the one named last changes fastest.
The devices are a block of a 4x4x8 slice.
Arguments:
- grad_attn: float32 [64, 4, 512, 512], P(('stage', 'data')), parts along dimension 0
- grad_shared_in: float32 [64, 2, 512, 176], P(('stage', 'data')), parts along dimension 0
- grad_shared_out: float32 [64, 1, 176, 512], P(('stage', 'data')), parts along dimension 0
- grad_expert_in: float32 [64, 16, 512, 176], P(('stage', 'data')), parts along dimension 0
- grad_expert_out: float32 [64, 8, 176, 512], P(('stage', 'data')), parts along dimension 0
- mom_attn: float32 [16, 512, 512], P('stage', 'data'), parts along dimension 0
- mom_shared_in: float32 [8, 512, 176], P('stage', 'data'), parts along dimension 0
- mom_shared_out: float32 [4, 176, 512], P('stage', 'data'), parts along dimension 0
- mom_expert_in: float32 [64, 512, 176], P('stage', 'data'), parts along dimension 0
- mom_expert_out: float32 [32, 176, 512], P('stage', 'data'), parts along dimension 0
- master_attn: float32 [16, 512, 512], P('stage', 'data'), parts along dimension 0
- master_shared_in: float32 [8, 512, 176], P('stage', 'data'), parts along dimension 0
- master_shared_out: float32 [4, 176, 512], P('stage', 'data'), parts along dimension 0
- master_expert_in: float32 [64, 512, 176], P('stage', 'data'), parts along dimension 0
- master_expert_out: float32 [32, 176, 512], P('stage', 'data'), parts along dimension 0
Outputs:
- output 1: float32 [16, 512, 512], P('stage', 'data'), parts along dimension 0
- output 2: float32 [8, 512, 176], P('stage', 'data'), parts along dimension 0
- output 3: float32 [4, 176, 512], P('stage', 'data'), parts along dimension 0
- output 4: float32 [64, 512, 176], P('stage', 'data'), parts along dimension 0
- output 5: float32 [32, 176, 512], P('stage', 'data'), parts along dimension 0
- output 6: float32 [16, 512, 512], P('stage', 'data'), parts along dimension 0
- output 7: float32 [8, 512, 176], P('stage', 'data'), parts along dimension 0
- output 8: float32 [4, 176, 512], P('stage', 'data'), parts along dimension 0
- output 9: float32 [64, 512, 176], P('stage', 'data'), parts along dimension 0
- output 10: float32 [32, 176, 512], P('stage', 'data'), parts along dimension 0
- output 11: bfloat16 [16, 512, 512], P('stage'), parts along dimension 0
- output 12: bfloat16 [8, 512, 176], P('stage'), parts along dimension 0
- output 13: bfloat16 [4, 176, 512], P('stage'), parts along dimension 0
- output 14: bfloat16 [64, 512, 176], P('stage'), parts along dimension 0
- output 15: bfloat16 [32, 176, 512], P('stage'), parts along dimension 0
There are 4 independent parts. The reference program is written for one: setup_inputs(seed, part) draws one part's arguments, and reference() takes and returns one part's arrays. A program takes and returns all parts, laid end to end along the dimension named above; each array names one.
All inputs are finite; a program needn't handle non-finite values.
Results may differ from the reference program's by a relative error of at most 0.00510666.
Values are sent between devices in bfloat16 or wider.
A program may use at most 768 MiB of HBM per device.

```python
import math
import jax
import jax.numpy as jnp
from jax import lax

DATA_DEVICES = 16
DIM_MODEL = 512
DIM_EXPERT = 176
DIM_SHARED = 176
NUM_EXPERTS = 8
NS_STEPS = 5

MOMENTUM = 0.95
LEARN_RATE = 0.2
WEIGHT_DECAY = 0.25
NORM_EPS = 1e-7
COEF_A = 3.4445
COEF_B = -4.7750
COEF_C = 2.0315
KIND_NAMES = ("attn", "shared_in", "shared_out", "expert_in", "expert_out")


def kind_shapes():
    return (
        (4, DIM_MODEL, DIM_MODEL),
        (2, DIM_MODEL, DIM_SHARED),
        (1, DIM_SHARED, DIM_MODEL),
        (2 * NUM_EXPERTS, DIM_MODEL, DIM_EXPERT),
        (NUM_EXPERTS, DIM_EXPERT, DIM_MODEL),
    )


def setup_inputs(seed: int = 0, part: int = 0) -> dict:
    base_key = jax.random.fold_in(jax.random.key(seed), part)
    mom_scale = DATA_DEVICES ** -0.5
    grads = {}
    moms = {}
    masters = {}
    for kind_index, (kind_name, mat_shape) in enumerate(zip(KIND_NAMES, kind_shapes())):
        grad_key, mom_key, master_key = jax.random.split(jax.random.fold_in(base_key, kind_index), 3)
        grads["grad_" + kind_name] = jax.random.normal(grad_key, (DATA_DEVICES,) + mat_shape, jnp.float32)
        moms["mom_" + kind_name] = mom_scale * jax.random.normal(mom_key, mat_shape, jnp.float32)
        masters["master_" + kind_name] = 0.5 * jax.random.normal(master_key, mat_shape, jnp.float32)
    result = {}
    result.update(grads)
    result.update(moms)
    result.update(masters)
    return result


def orthogonalize(matrix):
    is_tall = matrix.shape[0] > matrix.shape[1]
    frob_norm = jnp.sqrt(jnp.sum(matrix * matrix))
    iterate = (matrix / (frob_norm + NORM_EPS)).astype(jnp.bfloat16)
    if is_tall:
        iterate = iterate.T
    for iteration in range(NS_STEPS):
        gram_mat = jnp.dot(iterate, iterate.T, preferred_element_type=jnp.float32).astype(jnp.bfloat16)
        square = jnp.dot(gram_mat, gram_mat, preferred_element_type=jnp.float32)
        poly_mat = (COEF_B * gram_mat.astype(jnp.float32) + COEF_C * square).astype(jnp.bfloat16)
        update = jnp.dot(poly_mat, iterate, preferred_element_type=jnp.float32)
        iterate = (COEF_A * iterate.astype(jnp.float32) + update).astype(jnp.bfloat16)
    if is_tall:
        iterate = iterate.T
    return iterate


def kind_step(grad_stack, old_mom, master):
    num_rows = old_mom.shape[1]
    num_cols = old_mom.shape[2]
    grad_mean = jnp.sum(grad_stack, axis=0) / DATA_DEVICES
    new_mom = MOMENTUM * old_mom + grad_mean
    ortho_mat = lax.map(orthogonalize, new_mom)
    step_scale = 0.2 * math.sqrt(max(num_rows, num_cols))
    new_master = master - LEARN_RATE * (step_scale * ortho_mat.astype(jnp.float32) + WEIGHT_DECAY * master)
    return new_mom, new_master, new_master.astype(jnp.bfloat16)


def reference(grad_attn, grad_shared_in, grad_shared_out, grad_expert_in, grad_expert_out,
              mom_attn, mom_shared_in, mom_shared_out, mom_expert_in, mom_expert_out,
              master_attn, master_shared_in, master_shared_out, master_expert_in, master_expert_out):
    grad_list = (grad_attn, grad_shared_in, grad_shared_out, grad_expert_in, grad_expert_out)
    mom_list = (mom_attn, mom_shared_in, mom_shared_out, mom_expert_in, mom_expert_out)
    master_list = (master_attn, master_shared_in, master_shared_out, master_expert_in, master_expert_out)
    results = [kind_step(grad_list[kind_index], mom_list[kind_index], master_list[kind_index]) for kind_index in range(5)]
    return (results[0][0], results[1][0], results[2][0], results[3][0], results[4][0],
            results[0][1], results[1][1], results[2][1], results[3][1], results[4][1],
            results[0][2], results[1][2], results[2][2], results[3][2], results[4][2])
```

```python
import functools
import math
import jax
import jax.numpy as jnp
from jax import lax
from jax.experimental import pallas as pl
from jax.experimental.pallas import tpu as pltpu
from jax.sharding import PartitionSpec as P

NS_STEPS = 5
MOMENTUM = 0.95
LEARN_RATE = 0.2
WEIGHT_DECAY = 0.25
NORM_EPS = 1e-7
COEF_A = 3.4445
COEF_B = -4.7750
COEF_C = 2.0315

F32 = jnp.float32
BF16 = jnp.bfloat16
MESH = pl.DeviceIdType.MESH
LANE = 128
NT = (((1,), (1,)), ((), ()))


def round_up(value, step):
    return (value + step - 1) // step * step


def fused_step(n, counts, attn_rows, wide, narrow, *refs):
    c_attn, c_si, c_so, c_ei, c_eo = counts
    c_in, c_out = c_si + c_ei, c_so + c_eo
    nz = n // 2
    hops_far, hops_near = nz // 2, nz - 1 - nz // 2
    tiles = wide // LANE
    in_rows = wide // n
    half_in = in_rows // 2
    rest = narrow - LANE
    out_rows = narrow // n
    out_pad = round_up(out_rows, 16)
    attn_blk = attn_rows * tiles
    small_blk = in_rows + half_in
    small0 = c_attn * attn_blk

    it = iter(refs)
    take = lambda k: [next(it) for _ in range(k)]
    g_attn, g_si, g_so, g_ei, g_eo = take(5)
    m_in = take(5)
    w_in = take(5)
    m_out = take(5)
    w_out = take(5)
    p_attn, p_si, p_so, p_ei, p_eo = take(5)
    (gp, rx0, rxr, ag, mp, wp, nat_m, nat_w, nrm, xtx, rxx, otx, rxo, xb, ab, bb) = take(16)
    (s_load, s_nat, s_d2d, s_rs, r_rs, s_nrm, r_nrm, s_x, r_x, s_o, r_o, s_ag, r_ag, s_agd, r_agd, s_out) = take(16)

    in_w = c_in // 2
    waves = []
    base = 0
    for kind, first, cnt in (("in", 0, in_w), ("in", in_w, c_in - in_w), ("out", c_in, c_out)):
        waves.append(dict(kind=kind, first=first, cnt=cnt, row0=small0 + first * small_blk, blk=small_blk, base=base % n))
        base += cnt
    waves.insert(0, dict(kind="attn", first=0, cnt=c_attn, row0=0, blk=attn_blk, base=base % n))
    n_waves = len(waves)
    for w in waves:
        w["rows"] = w["cnt"] * w["blk"]
        w["half"] = w["rows"] // 2
        w["off"] = w["row0"] // 2
        w["ag_half"] = round_up(w["half"], 16)

    me = lax.axis_index("data")
    z = me // 2
    c = lax.rem(me, 2)
    zmod = lambda v: lax.rem(v + 2 * nz, nz)
    dev = lambda zz, cc: {"data": zz * 2 + cc}
    partner = {"data": z * 2 + (1 - c)}
    others = [lax.rem(me + k, n) for k in range(1, n)]

    def remote(src, dst, ss, rs, where):
        return pltpu.make_async_remote_copy(src_ref=src, dst_ref=dst, send_sem=ss, recv_sem=rs,
                                            device_id=where, device_id_type=MESH)

    barrier = pltpu.get_barrier_semaphore()
    for d in others:
        pl.semaphore_signal(barrier, inc=1, device_id={"data": d}, device_id_type=MESH)

    def nat_copies():
        return [pltpu.make_async_copy(srcs[k], dsts[k], s_nat.at[which, k])
                for which, (srcs, dsts) in enumerate(((m_in, nat_m), (w_in, nat_w))) for k in range(5)]

    def small_pack_in(block):
        zero = jnp.zeros((half_in, LANE // 2 - rest), F32)
        return jnp.concatenate([block[:half_in, LANE:], zero, block[half_in:, LANE:], zero], axis=1)

    def load_and_pack(raw_in, raw_out):
        attn_copies = []
        for m in range(c_attn):
            for t in range(tiles):
                attn_copies.append(pltpu.make_async_copy(
                    g_attn.at[m, :, :, :, pl.ds(LANE * t, LANE)],
                    gp.at[:, :, pl.ds(m * attn_blk + t * attn_rows, attn_rows), :], s_load.at[0]))
        k_cut = in_w - c_si
        loads = [
            pltpu.make_async_copy(g_si, raw_in.at[pl.ds(0, c_si)], s_load.at[1]),
            pltpu.make_async_copy(g_ei.at[pl.ds(0, k_cut)], raw_in.at[pl.ds(c_si, k_cut)], s_load.at[2]),
            pltpu.make_async_copy(g_ei.at[pl.ds(k_cut, c_ei - k_cut)], raw_in.at[pl.ds(in_w, c_ei - k_cut)], s_load.at[3]),
            pltpu.make_async_copy(g_so, raw_out.at[pl.ds(0, c_so)], s_load.at[4]),
            pltpu.make_async_copy(g_eo, raw_out.at[pl.ds(c_so, c_eo)], s_load.at[5]),
        ]
        for cp in attn_copies + loads + nat_copies():
            cp.start()

        def pack_in(j, carry):
            off = pl.multiple_of(small0 + small_blk * j, 8)
            for d in range(n):
                block = raw_in[j, in_rows * d:in_rows * (d + 1), :]
                gp[d // 2, d % 2, pl.ds(off, in_rows), :] = block[:, :LANE]
                gp[d // 2, d % 2, pl.ds(off + in_rows, half_in), :] = small_pack_in(block)
            return carry

        def pack_out(j, carry):
            off = pl.multiple_of(small0 + small_blk * (c_in + j), 8)
            for d in range(n):
                rows = [raw_out[j, out_rows * d:out_rows * (d + 1), LANE * t:LANE * (t + 1)] for t in range(tiles)]
                rows.append(jnp.zeros((small_blk - tiles * out_rows, LANE), F32))
                gp[d // 2, d % 2, pl.ds(off, small_blk), :] = jnp.concatenate(rows, axis=0)
            return carry

        pltpu.make_async_copy(gp.at[:, :, pl.ds(0, small0), :], gp.at[:, :, pl.ds(0, small0), :], s_load.at[0]).wait()
        pl.semaphore_wait(barrier, n - 1)
        d2d(0)
        loads[0].wait()
        loads[1].wait()
        lax.fori_loop(0, in_w, pack_in, 0)
        d2d(1)
        loads[2].wait()
        lax.fori_loop(in_w, c_in, pack_in, 0)
        d2d(2)
        loads[3].wait()
        loads[4].wait()
        lax.fori_loop(0, c_out, pack_out, 0)
        d2d(3)

    pending = []

    def d2d_copy(i):
        sl = pl.ds(waves[i]["row0"], waves[i]["rows"])
        return remote(gp.at[:, 1 - c, sl, :], rx0.at[:, sl, :], s_d2d.at[0, i], s_d2d.at[1, i], partner)

    def d2d(i):
        d2d_copy(i).start()

    hops = lambda h, dr: hops_far if h == dr else hops_near
    rs = {}

    def rs_send(i, h, dr, s):
        w = waves[i]
        length = hops(h, dr)
        step = length - s + 1
        dest = zmod(z + step) if dr == 0 else zmod(z - step)
        sl = pl.ds(w["row0"] + h * w["half"], w["half"])
        osl = pl.ds(w["off"], w["half"])
        val = gp[dest, c, sl, :] + rx0[dest, sl, :]
        if s > 1:
            rs[i, h, dr, s - 1].wait_recv()
            val = val + rxr[dr, h, s - 2, osl, :]
        gp[dest, c, sl, :] = val
        where = dev(zmod(z + 1), c) if dr == 0 else dev(zmod(z - 1), c)
        cp = remote(gp.at[dest, c, sl, :], rxr.at[dr, h, s - 1, osl, :],
                    s_rs.at[i, h * 2 + dr, s - 1], r_rs.at[i, h * 2 + dr, s - 1], where)
        cp.start()
        rs[i, h, dr, s] = cp
        pending.append(cp)

    def rs_finish(i):
        w = waves[i]
        for h in range(2):
            sl = pl.ds(w["row0"] + h * w["half"], w["half"])
            osl = pl.ds(w["off"], w["half"])
            total = gp[z, c, sl, :] + rx0[z, sl, :]
            for dr in range(2):
                last = hops(h, dr)
                rs[i, h, dr, last].wait_recv()
                total = total + rxr[dr, h, last - 1, osl, :]
            mp[sl, :] = MOMENTUM * mp[sl, :] + total / n
        lane = lax.broadcasted_iota(jnp.int32, (1, LANE), 1)
        part = jnp.zeros((1, LANE), F32)
        for m in range(w["cnt"]):
            block = mp[pl.ds(w["row0"] + m * w["blk"], w["blk"]), :]
            sq = jnp.sum(jnp.sum(block * block, axis=0, keepdims=True), axis=1, keepdims=True)
            part = jnp.where(lane == m, sq, part)
        nrm[i, me] = part
        for d in others:
            remote(nrm.at[i, me], nrm.at[i, me], s_nrm.at[i], r_nrm.at[i], {"data": d}).start()

    def nrm_wait(i, sem):
        view = nrm.at[i, pl.ds(0, n - 1)]
        pltpu.make_async_copy(view, view, sem).wait()

    def x_copy(i, m):
        w = waves[i]
        owner = (w["base"] + m) % n
        return remote(xtx[i].at[m], rxx[i].at[me], s_x.at[i, m], r_x.at[i], {"data": owner})

    def x_send(i):
        w = waves[i]
        nrm_wait(i, r_nrm.at[i])
        tot = jnp.zeros((1, LANE), F32)
        for d in range(n):
            tot = tot + nrm[i, d]
        lane = lax.broadcasted_iota(jnp.int32, (1, LANE), 1)
        for m in range(w["cnt"]):
            sq = jnp.sum(jnp.where(lane == m, tot, 0.0), axis=1, keepdims=True)
            x = mp[pl.ds(w["row0"] + m * w["blk"], w["blk"]), :] / (jnp.sqrt(sq) + NORM_EPS)
            if w["kind"] == "out":
                zero = jnp.zeros((out_pad - out_rows, LANE), F32)
                parts = []
                for t in range(tiles):
                    parts += [x[t * out_rows:(t + 1) * out_rows], zero]
                x = jnp.concatenate(parts, axis=0)
            x = x.astype(BF16)
            xtx[i][m] = x
            owner = (w["base"] + m) % n

            @pl.when(me != owner)
            def _():
                x_copy(i, m).start()

            @pl.when(me == owner)
            def _():
                rxx[i][me] = x

    def owned(i):
        w = waves[i]
        mine = lax.rem(me - w["base"] + n, n)
        return mine, mine < w["cnt"]

    def assemble(i):
        kind = waves[i]["kind"]
        rx = rxx[i]
        if kind == "attn":
            for t in range(tiles):
                xb[:, LANE * t:LANE * (t + 1)] = rx[:, attn_rows * t:attn_rows * (t + 1), :].reshape(n * attn_rows, LANE)
        elif kind == "out":
            for t in range(tiles):
                xb[:n * out_pad, LANE * t:LANE * (t + 1)] = rx[:, out_pad * t:out_pad * (t + 1), :].reshape(n * out_pad, LANE)
        else:
            hw = n * half_in
            for k in range(2):
                blk = rx[:, half_in * k:half_in * (k + 1), :].reshape(hw, LANE).astype(F32)
                xb[:LANE, hw * k:hw * (k + 1)] = blk.T.astype(BF16)
            blk = rx[:, in_rows:, :].reshape(hw, LANE).astype(F32).T
            for k in range(2):
                xb[LANE:narrow, hw * k:hw * (k + 1)] = blk[k * (LANE // 2):k * (LANE // 2) + rest].astype(BF16)
            xb[narrow:n * out_pad, :] = jnp.zeros((n * out_pad - narrow, wide), BF16)

    def disassemble(i):
        kind = waves[i]["kind"]
        tx = otx[i]
        if kind == "attn":
            for t in range(tiles):
                tx[:, attn_rows * t:attn_rows * (t + 1), :] = xb[:, LANE * t:LANE * (t + 1)].reshape(n, attn_rows, LANE)
        elif kind == "out":
            for t in range(tiles):
                tx[:, out_pad * t:out_pad * (t + 1), :] = xb[:n * out_pad, LANE * t:LANE * (t + 1)].reshape(n, out_pad, LANE)
        else:
            hw = n * half_in
            for k in range(2):
                blk = xb[:LANE, hw * k:hw * (k + 1)].astype(F32).T
                tx[:, half_in * k:half_in * (k + 1), :] = blk.astype(BF16).reshape(n, half_in, LANE)
            zero = jnp.zeros((LANE // 2 - rest, hw), F32)
            parts = []
            for k in range(2):
                parts += [xb[LANE:narrow, hw * k:hw * (k + 1)].astype(F32), zero]
            blk = jnp.concatenate(parts, axis=0).T
            tx[:, in_rows:, :] = blk.astype(BF16).reshape(n, half_in, LANE)

    def iterate(size):
        cut = min(size, 256)

        def one(_, carry):
            for r in range(size // cut):
                sl = slice(r * cut, (r + 1) * cut)
                gram = lax.dot_general(xb[sl, :], xb[:size, :], NT, preferred_element_type=F32)
                ab[sl, :size] = gram.astype(BF16)
            for r in range(size // cut):
                sl = slice(r * cut, (r + 1) * cut)
                square = jnp.dot(ab[sl, :size], ab[:size, :size], preferred_element_type=F32)
                bb[sl, :size] = (COEF_B * ab[sl, :size].astype(F32) + COEF_C * square).astype(BF16)
            for r in range(wide // 256):
                sl = slice(r * 256, (r + 1) * 256)
                update = jnp.dot(bb[:size, :size], xb[:size, sl], preferred_element_type=F32)
                xb[:size, sl] = (COEF_A * xb[:size, sl].astype(F32) + update).astype(BF16)
            return carry

        lax.fori_loop(0, NS_STEPS, one, 0)

    def o_copy(i, mine, d):
        return remote(otx[i].at[d], rxo[i].at[mine], s_o.at[i], r_o.at[i], {"data": d})

    def owner_work(i):
        mine, yes = owned(i)

        @pl.when(yes)
        def _():
            view = rxx[i].at[pl.ds(0, n - 1)]
            pltpu.make_async_copy(view, view, r_x.at[i]).wait()
            assemble(i)
            iterate(n * attn_rows if waves[i]["kind"] == "attn" else n * out_pad)
            disassemble(i)
            for d in others:
                o_copy(i, mine, d).start()
            rxo[i][mine] = otx[i][me]

    def master(i):
        w = waves[i]
        mine, yes = owned(i)
        cnt = w["cnt"]

        @pl.when(yes)
        def _():
            view = rxo[i].at[pl.ds(0, cnt - 1)]
            pltpu.make_async_copy(view, view, r_o.at[i]).wait()

        @pl.when(jnp.logical_not(yes))
        def _():
            pltpu.make_async_copy(rxo[i], rxo[i], r_o.at[i]).wait()

        step_scale = 0.2 * math.sqrt(wide)
        for m in range(cnt):
            sl = pl.ds(w["row0"] + m * w["blk"], w["blk"])
            o = rxo[i][m].astype(F32)
            if w["kind"] == "out":
                parts = [o[out_pad * t:out_pad * t + out_rows] for t in range(tiles)]
                parts.append(jnp.zeros((small_blk - tiles * out_rows, LANE), F32))
                o = jnp.concatenate(parts, axis=0)
            old = wp[sl, :]
            new = old - LEARN_RATE * (step_scale * o + WEIGHT_DECAY * old)
            wp[sl, :] = new
            ag[z, c, sl, :] = new.astype(BF16)

    agc = {}
    agd = {}

    def ag_rows(i, h):
        w = waves[i]
        if h == 0:
            return pl.ds(w["row0"], w["ag_half"])
        return pl.ds(w["row0"] + w["ag_half"], w["rows"] - w["ag_half"])

    def ag_to_partner(i, h, src, key):
        part = ag.at[src, c, ag_rows(i, h), :]
        cp = remote(part, part, s_agd.at[i, h, key], r_agd.at[i, h, key], partner)
        cp.start()
        agd[i, h, key] = cp
        pending.append(cp)

    def ag_send(i, h, dr, s):
        length = hops(h, dr)
        src = z if s == 1 else (zmod(z - (s - 1)) if dr == 0 else zmod(z + (s - 1)))
        if s > 1:
            agc[i, h, dr, s - 1].wait_recv()
        if s <= length:
            part = ag.at[src, c, ag_rows(i, h), :]
            where = dev(zmod(z + 1), c) if dr == 0 else dev(zmod(z - 1), c)
            cp = remote(part, part, s_ag.at[i, h * 2 + dr, s - 1], r_ag.at[i, h * 2 + dr, s - 1], where)
            cp.start()
            agc[i, h, dr, s] = cp
            pending.append(cp)
        if s > 1:
            ag_to_partner(i, h, src, (s - 1) if dr == 0 else nz - (s - 1))
        elif dr == 0:
            ag_to_partner(i, h, src, 0)

    out_copies = []

    def out_copy(src, dst, k):
        cp = pltpu.make_async_copy(src, dst, s_out.at[k])
        cp.start()
        out_copies.append(cp)

    def native_outputs():
        for which, (src, nat, outs) in enumerate(((mp, nat_m, m_out), (wp, nat_w, w_out))):
            for m in range(c_attn):
                for t in range(tiles):
                    nat[0][m, :, LANE * t:LANE * (t + 1)] = src[pl.ds(m * attn_blk + t * attn_rows, attn_rows), :]
            j = 0
            for k, cnt in ((1, c_si), (3, c_ei)):
                for m in range(cnt):
                    off = small0 + small_blk * j
                    nat[k][m, :, :LANE] = src[off:off + in_rows, :]
                    rem_blk = src[off + in_rows:off + small_blk, :]
                    nat[k][m, :half_in, LANE:] = rem_blk[:, :rest]
                    nat[k][m, half_in:, LANE:] = rem_blk[:, LANE // 2:LANE // 2 + rest]
                    j += 1
            for k, cnt in ((2, c_so), (4, c_eo)):
                for m in range(cnt):
                    off = small0 + small_blk * j
                    for t in range(tiles):
                        nat[k][m, :, LANE * t:LANE * (t + 1)] = src[off + t * out_rows:off + (t + 1) * out_rows, :]
                    j += 1
            for k in range(5):
                out_copy(nat[k], outs[k], which * 5 + k)

    def native_inputs():
        for cp in nat_copies():
            cp.wait()
        for nat, dst in ((nat_m, mp), (nat_w, wp)):
            for m in range(c_attn):
                for t in range(tiles):
                    dst[pl.ds(m * attn_blk + t * attn_rows, attn_rows), :] = nat[0][m, :, LANE * t:LANE * (t + 1)]
            j = 0
            for k, cnt in ((1, c_si), (3, c_ei)):
                for m in range(cnt):
                    off = small0 + small_blk * j
                    block = nat[k][m]
                    dst[off:off + in_rows, :] = block[:, :LANE]
                    dst[off + in_rows:off + small_blk, :] = small_pack_in(block)
                    j += 1
            for k, cnt in ((2, c_so), (4, c_eo)):
                for m in range(cnt):
                    off = small0 + small_blk * j
                    rows = [nat[k][m, :, LANE * t:LANE * (t + 1)] for t in range(tiles)]
                    rows.append(jnp.zeros((small_blk - tiles * out_rows, LANE), F32))
                    dst[off:off + small_blk, :] = jnp.concatenate(rows, axis=0)
                    j += 1

    def unpack(i, stage_in, stage_out, flat):
        w = waves[i]
        for h in range(2):
            for key in range(nz):
                agd[i, h, key].wait_recv()
        if w["kind"] == "attn":
            for m in range(c_attn):
                for t in range(tiles):
                    out_copies.append(pltpu.make_async_copy(
                        ag.at[:, :, pl.ds(m * attn_blk + t * attn_rows, attn_rows), :],
                        p_attn.at[m, :, :, :, pl.ds(LANE * t, LANE)], s_out.at[10 + m * tiles + t]))
                    out_copies[-1].start()
        elif w["kind"] == "in":
            def body(j, carry):
                off = pl.multiple_of(small0 + small_blk * j, 16)
                for d in range(n):
                    blk = ag[d // 2, d % 2, pl.ds(off, small_blk), :]
                    r = in_rows * d
                    stage_in[j, r:r + in_rows, :LANE] = blk[:in_rows]
                    tail = blk[in_rows:].astype(F32)
                    stage_in[j, r:r + half_in, LANE:] = tail[:, :rest].astype(BF16)
                    stage_in[j, r + half_in:r + in_rows, LANE:] = tail[:, LANE // 2:LANE // 2 + rest].astype(BF16)
                return carry
            lax.fori_loop(w["first"], w["first"] + w["cnt"], body, 0)
            k = 10 + c_attn * tiles
            if w["first"] == 0:
                out_copy(stage_in.at[pl.ds(0, c_si)], p_si, k)
                out_copy(stage_in.at[pl.ds(c_si, in_w - c_si)], p_ei.at[pl.ds(0, in_w - c_si)], k + 1)
            else:
                out_copy(stage_in.at[pl.ds(in_w, c_in - in_w)], p_ei.at[pl.ds(in_w - c_si, c_in - in_w)], k + 2)
        else:
            def body(j, carry):
                off = pl.multiple_of(small0 + small_blk * (c_in + j), 16)
                for d in range(n):
                    blk = ag[d // 2, d % 2, pl.ds(off, small_blk), :].astype(F32)
                    for t in range(tiles):
                        flat[out_rows * d:out_rows * (d + 1), LANE * t:LANE * (t + 1)] = blk[t * out_rows:(t + 1) * out_rows]
                stage_out[j] = flat[...].astype(BF16)
                return carry
            lax.fori_loop(0, c_out, body, 0)
            k = 13 + c_attn * tiles
            out_copy(stage_out.at[pl.ds(0, c_so)], p_so, k)
            out_copy(stage_out.at[pl.ds(c_so, c_eo)], p_eo, k + 1)

    pl.run_scoped(load_and_pack, pltpu.VMEM((c_in, wide, narrow), F32), pltpu.VMEM((c_out, narrow, wide), F32))
    def main_phase(stage_in, stage_out, flat):
        native_inputs()
        order = range(n_waves)
        for i in order:
            d2d_copy(i).wait_recv()
            for h in range(2):
                for dr in range(2):
                    rs_send(i, h, dr, 1)
        for s in range(2, hops_far + 1):
            for i in order:
                for h in range(2):
                    for dr in range(2):
                        if s <= hops(h, dr):
                            rs_send(i, h, dr, s)
        for i in order:
            rs_finish(i)
        for i in order:
            x_send(i)
        for i in order:
            owner_work(i)
        for i in order:
            master(i)
            for h in range(2):
                for dr in range(2):
                    ag_send(i, h, dr, 1)
        native_outputs()
        for s in range(2, hops_far + 2):
            for i in order:
                for h in range(2):
                    for dr in range(2):
                        if s <= hops(h, dr) + 1:
                            ag_send(i, h, dr, s)

        for i in order:
            unpack(i, stage_in, stage_out, flat)
        for cp in out_copies:
            cp.wait()

        for cp in pending:
            cp.wait_send()
        for i in order:
            d2d_copy(i).wait_send()
            nrm_wait(i, s_nrm.at[i])
            for m in range(waves[i]["cnt"]):
                owner = (waves[i]["base"] + m) % n

                @pl.when(me != owner)
                def _():
                    x_copy(i, m).wait_send()
            mine, yes = owned(i)

            @pl.when(yes)
            def _():
                view = otx[i].at[pl.ds(0, n - 1)]
                pltpu.make_async_copy(view, view, s_o.at[i]).wait()

    pl.run_scoped(main_phase, pltpu.VMEM((c_in, wide, narrow), BF16), pltpu.VMEM((c_out, narrow, wide), BF16),
                  pltpu.VMEM((narrow, wide), F32))


def solution(mesh):
    n = mesh.shape["data"]
    nz = n // 2

    def local_step(*arrays):
        grads, moms, masters = arrays[:5], arrays[5:10], arrays[10:]
        counts = tuple(m.shape[0] for m in moms)
        attn_rows, wide = moms[0].shape[1:]
        narrow = moms[1].shape[2]
        c_attn, c_si, c_so, c_ei, c_eo = counts
        c_in, c_out = c_si + c_ei, c_so + c_eo
        tiles = wide // LANE
        small_blk = wide // n + wide // n // 2
        out_pad = round_up(narrow // n, 16)
        attn_blk = attn_rows * tiles
        rows = c_attn * attn_blk + (c_in + c_out) * small_blk
        grads = [g[0] for g in grads]
        grads[0] = grads[0].reshape(c_attn, nz, 2, attn_rows, wide)
        hops = nz // 2

        sds = jax.ShapeDtypeStruct
        out_shape = [sds(m.shape, F32) for m in moms] * 2
        out_shape += [sds((c_attn, nz, 2, attn_rows, wide), BF16)]
        out_shape += [sds((c_si, wide, narrow), BF16), sds((c_so, narrow, wide), BF16),
                      sds((c_ei, wide, narrow), BF16), sds((c_eo, narrow, wide), BF16)]
        w_cnt = (c_attn, c_in // 2, c_in - c_in // 2, c_out)
        w_blk = (attn_blk, small_blk, small_blk, out_pad * tiles)
        dma = lambda *shape: pltpu.SemaphoreType.DMA(shape)
        vm = pltpu.VMEM
        scratch = [
            vm((nz, 2, rows, LANE), F32),
            vm((nz, rows, LANE), F32),
            vm((2, 2, hops, rows // 2, LANE), F32),
            vm((nz, 2, rows, LANE), BF16),
            vm((rows, LANE), F32),
            vm((rows, LANE), F32),
            [vm(m.shape, F32) for m in moms],
            [vm(m.shape, F32) for m in moms],
            vm((4, n, 1, LANE), F32),
            [vm((k, b, LANE), BF16) for k, b in zip(w_cnt, w_blk)],
            [vm((n, b, LANE), BF16) for b in w_blk],
            [vm((n, b, LANE), BF16) for b in w_blk],
            [vm((k, b, LANE), BF16) for k, b in zip(w_cnt, w_blk)],
            vm((n * attn_rows, wide), BF16),
            vm((n * attn_rows, n * attn_rows), BF16),
            vm((n * attn_rows, n * attn_rows), BF16),
            dma(6), dma(2, 5), dma(2, 4), dma(4, 4, hops), dma(4, 4, hops),
            dma(4), dma(4), dma(4, max(w_cnt)), dma(4), dma(4), dma(4),
            dma(4, 4, hops), dma(4, 4, hops), dma(4, 2, nz), dma(4, 2, nz),
            dma(15 + c_attn * tiles),
        ]
        any_spec = pl.BlockSpec(memory_space=pl.ANY)
        call = pl.pallas_call(
            functools.partial(fused_step, n, counts, attn_rows, wide, narrow),
            out_shape=out_shape,
            in_specs=[any_spec] * 15,
            out_specs=[any_spec] * 15,
            scratch_shapes=scratch,
            compiler_params=pltpu.CompilerParams(
                collective_id=0, has_side_effects=True, vmem_limit_bytes=67043328),
            name="muon_step",
        )
        outs = list(call(*grads, *moms, *masters))
        outs[10] = outs[10].reshape(c_attn, n * attn_rows, wide)
        return tuple(outs)

    grad_spec = P(("stage", "data"), None, None, None)
    row_spec = P("stage", "data", None)
    full_spec = P("stage", None, None)
    in_specs = (grad_spec,) * 5 + (row_spec,) * 10
    out_specs = (row_spec,) * 10 + (full_spec,) * 5
    return jax.shard_map(local_step, mesh=mesh, in_specs=in_specs, out_specs=out_specs, check_vma=False)
```

```python
import functools
import math
import jax
import jax.numpy as jnp
from jax import lax
from jax.experimental import pallas as pl
from jax.experimental.pallas import tpu as pltpu
from jax.sharding import PartitionSpec as P

NS_STEPS = 5
MOMENTUM = 0.95
LEARN_RATE = 0.2
WEIGHT_DECAY = 0.25
NORM_EPS = 1e-7
COEF_A = 3.4445
COEF_B = -4.7750
COEF_C = 2.0315

F32 = jnp.float32
BF16 = jnp.bfloat16
MESH = pl.DeviceIdType.MESH
LANE = 128
NT = (((1,), (1,)), ((), ()))


def round_up(value, step):
    return (value + step - 1) // step * step


def fused_step(n, counts, attn_rows, wide, narrow, *refs):
    c_attn, c_si, c_so, c_ei, c_eo = counts
    c_in, c_out = c_si + c_ei, c_so + c_eo
    nz = n // 2
    hops_far, hops_near = nz // 2, nz - 1 - nz // 2
    tiles = wide // LANE
    in_rows = wide // n
    groups = LANE // in_rows
    out_rows = narrow // n
    out_pad = round_up(out_rows, 16)
    attn_blk = attn_rows * tiles
    small_blk = round_up(tiles * out_rows, 16)
    cuts = [(q * small_blk, min(small_blk, narrow - q * small_blk)) for q in range(groups)]
    small0 = c_attn * attn_blk

    it = iter(refs)
    take = lambda k: [next(it) for _ in range(k)]
    g_attn, g_si, g_so, g_ei, g_eo = take(5)
    m_in = take(5)
    w_in = take(5)
    m_out = take(5)
    w_out = take(5)
    p_attn, p_si, p_so, p_ei, p_eo = take(5)
    (gp, rx0, rxr, ag, mp, wp, nat_m, nat_w, nrm, xtx, rxx, otx, rxo, xb, ab, bb) = take(16)
    (s_load, s_nat, s_d2d, s_rs, r_rs, s_nrm, r_nrm, s_x, r_x, s_o, r_o, s_ag, r_ag, s_agd, r_agd, s_out) = take(16)

    in_w = c_in // 2
    waves = []
    base = 0
    for kind, first, cnt in (("in", 0, in_w), ("in", in_w, c_in - in_w), ("out", c_in, c_out)):
        waves.append(dict(kind=kind, first=first, cnt=cnt, row0=small0 + first * small_blk, blk=small_blk, base=base % n))
        base += cnt
    waves.insert(0, dict(kind="attn", first=0, cnt=c_attn, row0=0, blk=attn_blk, base=base % n))
    n_waves = len(waves)
    for w in waves:
        w["rows"] = w["cnt"] * w["blk"]
        w["half"] = w["rows"] // 2
        w["off"] = w["row0"] // 2
        w["ag_half"] = round_up(w["half"], 16)

    me = lax.axis_index("data")
    z = me // 2
    c = lax.rem(me, 2)
    zmod = lambda v: lax.rem(v + 2 * nz, nz)
    dev = lambda zz, cc: {"data": zz * 2 + cc}
    partner = {"data": z * 2 + (1 - c)}
    others = [lax.rem(me + k, n) for k in range(1, n)]

    def remote(src, dst, ss, rs, where):
        return pltpu.make_async_remote_copy(src_ref=src, dst_ref=dst, send_sem=ss, recv_sem=rs,
                                            device_id=where, device_id_type=MESH)

    barrier = pltpu.get_barrier_semaphore()
    for d in others:
        pl.semaphore_signal(barrier, inc=1, device_id={"data": d}, device_id_type=MESH)

    def nat_copies():
        return [pltpu.make_async_copy(srcs[k], dsts[k], s_nat.at[which, k])
                for which, (srcs, dsts) in enumerate(((m_in, nat_m), (w_in, nat_w))) for k in range(5)]

    def lane_swap(blocks):
        lane = lax.broadcasted_iota(jnp.int32, (1, LANE), 1)
        blocks = list(blocks)
        dist = groups // 2
        while dist:
            width = dist * in_rows
            low = lax.rem(lane // width, 2) == 0
            for q in range(groups):
                if (q // dist) % 2 == 0:
                    x, y = blocks[q], blocks[q + dist]
                    blocks[q] = jnp.where(low, x, pltpu.roll(y, width, axis=1))
                    blocks[q + dist] = jnp.where(low, pltpu.roll(x, LANE - width, axis=1), y)
            dist //= 2
        return blocks

    def pad_rows(x, rows):
        if x.shape[0] == rows:
            return x
        return jnp.concatenate([x, jnp.zeros((rows - x.shape[0], x.shape[1]), x.dtype)], axis=0)

    def load_and_pack(raw_in, raw_out):
        attn_copies = []
        for m in range(c_attn):
            for t in range(tiles):
                attn_copies.append(pltpu.make_async_copy(
                    g_attn.at[m, :, :, :, pl.ds(LANE * t, LANE)],
                    gp.at[:, :, pl.ds(m * attn_blk + t * attn_rows, attn_rows), :], s_load.at[0]))
        k_cut = in_w - c_si
        loads = [
            pltpu.make_async_copy(g_si, raw_in.at[pl.ds(0, c_si)], s_load.at[1]),
            pltpu.make_async_copy(g_ei.at[pl.ds(0, k_cut)], raw_in.at[pl.ds(c_si, k_cut)], s_load.at[2]),
            pltpu.make_async_copy(g_ei.at[pl.ds(k_cut, c_ei - k_cut)], raw_in.at[pl.ds(in_w, c_ei - k_cut)], s_load.at[3]),
            pltpu.make_async_copy(g_so, raw_out.at[pl.ds(0, c_so)], s_load.at[4]),
            pltpu.make_async_copy(g_eo, raw_out.at[pl.ds(c_so, c_eo)], s_load.at[5]),
        ]
        for cp in attn_copies + loads + nat_copies():
            cp.start()

        def pack_in(j, carry):
            off = pl.multiple_of(small0 + small_blk * j, 8)
            for t in range(tiles):
                cols = slice(LANE * t, LANE * (t + 1))
                got = lane_swap([pad_rows(raw_in[j, r:r + k, cols], small_blk) for r, k in cuts])
                for p in range(groups):
                    d = groups * t + p
                    gp[d // 2, d % 2, pl.ds(off, small_blk), :] = got[p]
            return carry

        def pack_out(j, carry):
            off = pl.multiple_of(small0 + small_blk * (c_in + j), 8)
            for d in range(n):
                rows = [raw_out[j, out_rows * d:out_rows * (d + 1), LANE * t:LANE * (t + 1)] for t in range(tiles)]
                rows.append(jnp.zeros((small_blk - tiles * out_rows, LANE), F32))
                gp[d // 2, d % 2, pl.ds(off, small_blk), :] = jnp.concatenate(rows, axis=0)
            return carry

        pltpu.make_async_copy(gp.at[:, :, pl.ds(0, small0), :], gp.at[:, :, pl.ds(0, small0), :], s_load.at[0]).wait()
        pl.semaphore_wait(barrier, n - 1)
        d2d(0)
        loads[0].wait()
        loads[1].wait()
        lax.fori_loop(0, in_w, pack_in, 0)
        d2d(1)
        loads[2].wait()
        lax.fori_loop(in_w, c_in, pack_in, 0)
        d2d(2)
        loads[3].wait()
        loads[4].wait()
        lax.fori_loop(0, c_out, pack_out, 0)
        d2d(3)

    pending = []

    def d2d_copy(i):
        sl = pl.ds(waves[i]["row0"], waves[i]["rows"])
        return remote(gp.at[:, 1 - c, sl, :], rx0.at[:, sl, :], s_d2d.at[0, i], s_d2d.at[1, i], partner)

    def d2d(i):
        d2d_copy(i).start()

    hops = lambda h, dr: hops_far if h == dr else hops_near
    rs = {}

    def rs_send(i, h, dr, s):
        w = waves[i]
        length = hops(h, dr)
        step = length - s + 1
        dest = zmod(z + step) if dr == 0 else zmod(z - step)
        sl = pl.ds(w["row0"] + h * w["half"], w["half"])
        osl = pl.ds(w["off"], w["half"])
        val = gp[dest, c, sl, :] + rx0[dest, sl, :]
        if s > 1:
            rs[i, h, dr, s - 1].wait_recv()
            val = val + rxr[dr, h, s - 2, osl, :]
        gp[dest, c, sl, :] = val
        where = dev(zmod(z + 1), c) if dr == 0 else dev(zmod(z - 1), c)
        cp = remote(gp.at[dest, c, sl, :], rxr.at[dr, h, s - 1, osl, :],
                    s_rs.at[i, h * 2 + dr, s - 1], r_rs.at[i, h * 2 + dr, s - 1], where)
        cp.start()
        rs[i, h, dr, s] = cp
        pending.append(cp)

    def rs_finish(i):
        w = waves[i]
        for h in range(2):
            sl = pl.ds(w["row0"] + h * w["half"], w["half"])
            osl = pl.ds(w["off"], w["half"])
            total = gp[z, c, sl, :] + rx0[z, sl, :]
            for dr in range(2):
                last = hops(h, dr)
                rs[i, h, dr, last].wait_recv()
                total = total + rxr[dr, h, last - 1, osl, :]
            mp[sl, :] = MOMENTUM * mp[sl, :] + total / n
        lane = lax.broadcasted_iota(jnp.int32, (1, LANE), 1)
        part = jnp.zeros((1, LANE), F32)
        for m in range(w["cnt"]):
            block = mp[pl.ds(w["row0"] + m * w["blk"], w["blk"]), :]
            sq = jnp.sum(jnp.sum(block * block, axis=0, keepdims=True), axis=1, keepdims=True)
            part = jnp.where(lane == m, sq, part)
        nrm[i, me] = part
        for d in others:
            remote(nrm.at[i, me], nrm.at[i, me], s_nrm.at[i], r_nrm.at[i], {"data": d}).start()

    def nrm_wait(i, sem):
        view = nrm.at[i, pl.ds(0, n - 1)]
        pltpu.make_async_copy(view, view, sem).wait()

    def x_copy(i, m):
        w = waves[i]
        owner = (w["base"] + m) % n
        return remote(xtx[i].at[m], rxx[i].at[me], s_x.at[i, m], r_x.at[i], {"data": owner})

    def x_send(i):
        w = waves[i]
        nrm_wait(i, r_nrm.at[i])
        tot = jnp.zeros((1, LANE), F32)
        for d in range(n):
            tot = tot + nrm[i, d]
        lane = lax.broadcasted_iota(jnp.int32, (1, LANE), 1)
        for m in range(w["cnt"]):
            sq = jnp.sum(jnp.where(lane == m, tot, 0.0), axis=1, keepdims=True)
            x = mp[pl.ds(w["row0"] + m * w["blk"], w["blk"]), :] / (jnp.sqrt(sq) + NORM_EPS)
            if w["kind"] == "out":
                zero = jnp.zeros((out_pad - out_rows, LANE), F32)
                parts = []
                for t in range(tiles):
                    parts += [x[t * out_rows:(t + 1) * out_rows], zero]
                x = jnp.concatenate(parts, axis=0)
            x = x.astype(BF16)
            xtx[i][m] = x
            owner = (w["base"] + m) % n

            @pl.when(me != owner)
            def _():
                x_copy(i, m).start()

            @pl.when(me == owner)
            def _():
                rxx[i][me] = x

    def owned(i):
        w = waves[i]
        mine = lax.rem(me - w["base"] + n, n)
        return mine, mine < w["cnt"]

    def assemble(i):
        kind = waves[i]["kind"]
        rx = rxx[i]
        if kind == "attn":
            for t in range(tiles):
                xb[:, LANE * t:LANE * (t + 1)] = rx[:, attn_rows * t:attn_rows * (t + 1), :].reshape(n * attn_rows, LANE)
        elif kind == "out":
            for t in range(tiles):
                xb[:n * out_pad, LANE * t:LANE * (t + 1)] = rx[:, out_pad * t:out_pad * (t + 1), :].reshape(n * out_pad, LANE)
        else:
            for t in range(tiles):
                got = lane_swap([rx[groups * t + p].astype(F32) for p in range(groups)])
                for q, (r, k) in enumerate(cuts):
                    xb[r:r + k, LANE * t:LANE * (t + 1)] = got[q][:k].astype(BF16)
            xb[narrow:n * out_pad, :] = jnp.zeros((n * out_pad - narrow, wide), BF16)

    def disassemble(i):
        kind = waves[i]["kind"]
        tx = otx[i]
        if kind == "attn":
            for t in range(tiles):
                tx[:, attn_rows * t:attn_rows * (t + 1), :] = xb[:, LANE * t:LANE * (t + 1)].reshape(n, attn_rows, LANE)
        elif kind == "out":
            for t in range(tiles):
                tx[:, out_pad * t:out_pad * (t + 1), :] = xb[:n * out_pad, LANE * t:LANE * (t + 1)].reshape(n, out_pad, LANE)
        else:
            for t in range(tiles):
                cols = slice(LANE * t, LANE * (t + 1))
                got = lane_swap([pad_rows(xb[r:r + k, cols].astype(F32), small_blk) for r, k in cuts])
                for p in range(groups):
                    tx[groups * t + p] = got[p].astype(BF16)

    def iterate(size):
        cut = min(size, 256)

        def one(_, carry):
            for r in range(size // cut):
                sl = slice(r * cut, (r + 1) * cut)
                gram = lax.dot_general(xb[sl, :], xb[:size, :], NT, preferred_element_type=F32)
                ab[sl, :size] = gram.astype(BF16)
            for r in range(size // cut):
                sl = slice(r * cut, (r + 1) * cut)
                square = jnp.dot(ab[sl, :size], ab[:size, :size], preferred_element_type=F32)
                bb[sl, :size] = (COEF_B * ab[sl, :size].astype(F32) + COEF_C * square).astype(BF16)
            for r in range(wide // 256):
                sl = slice(r * 256, (r + 1) * 256)
                update = jnp.dot(bb[:size, :size], xb[:size, sl], preferred_element_type=F32)
                xb[:size, sl] = (COEF_A * xb[:size, sl].astype(F32) + update).astype(BF16)
            return carry

        lax.fori_loop(0, NS_STEPS, one, 0)

    def o_copy(i, mine, d):
        return remote(otx[i].at[d], rxo[i].at[mine], s_o.at[i], r_o.at[i], {"data": d})

    def owner_work(i):
        mine, yes = owned(i)

        @pl.when(yes)
        def _():
            view = rxx[i].at[pl.ds(0, n - 1)]
            pltpu.make_async_copy(view, view, r_x.at[i]).wait()
            assemble(i)
            iterate(n * attn_rows if waves[i]["kind"] == "attn" else n * out_pad)
            disassemble(i)
            for d in others:
                o_copy(i, mine, d).start()
            rxo[i][mine] = otx[i][me]

    def master(i):
        w = waves[i]
        mine, yes = owned(i)
        cnt = w["cnt"]

        @pl.when(yes)
        def _():
            view = rxo[i].at[pl.ds(0, cnt - 1)]
            pltpu.make_async_copy(view, view, r_o.at[i]).wait()

        @pl.when(jnp.logical_not(yes))
        def _():
            pltpu.make_async_copy(rxo[i], rxo[i], r_o.at[i]).wait()

        step_scale = 0.2 * math.sqrt(wide)
        for m in range(cnt):
            sl = pl.ds(w["row0"] + m * w["blk"], w["blk"])
            o = rxo[i][m].astype(F32)
            if w["kind"] == "out":
                parts = [o[out_pad * t:out_pad * t + out_rows] for t in range(tiles)]
                parts.append(jnp.zeros((small_blk - tiles * out_rows, LANE), F32))
                o = jnp.concatenate(parts, axis=0)
            old = wp[sl, :]
            new = old - LEARN_RATE * (step_scale * o + WEIGHT_DECAY * old)
            wp[sl, :] = new
            ag[z, c, sl, :] = new.astype(BF16)

    agc = {}
    agd = {}

    def ag_rows(i, h):
        w = waves[i]
        if h == 0:
            return pl.ds(w["row0"], w["ag_half"])
        return pl.ds(w["row0"] + w["ag_half"], w["rows"] - w["ag_half"])

    def ag_to_partner(i, h, src, key):
        part = ag.at[src, c, ag_rows(i, h), :]
        cp = remote(part, part, s_agd.at[i, h, key], r_agd.at[i, h, key], partner)
        cp.start()
        agd[i, h, key] = cp
        pending.append(cp)

    def ag_send(i, h, dr, s):
        length = hops(h, dr)
        src = z if s == 1 else (zmod(z - (s - 1)) if dr == 0 else zmod(z + (s - 1)))
        if s > 1:
            agc[i, h, dr, s - 1].wait_recv()
        if s <= length:
            part = ag.at[src, c, ag_rows(i, h), :]
            where = dev(zmod(z + 1), c) if dr == 0 else dev(zmod(z - 1), c)
            cp = remote(part, part, s_ag.at[i, h * 2 + dr, s - 1], r_ag.at[i, h * 2 + dr, s - 1], where)
            cp.start()
            agc[i, h, dr, s] = cp
            pending.append(cp)
        if s > 1:
            ag_to_partner(i, h, src, (s - 1) if dr == 0 else nz - (s - 1))
        elif dr == 0:
            ag_to_partner(i, h, src, 0)

    out_copies = []

    def out_copy(src, dst, k):
        cp = pltpu.make_async_copy(src, dst, s_out.at[k])
        cp.start()
        out_copies.append(cp)

    def native_outputs():
        for which, (src, nat, outs) in enumerate(((mp, nat_m, m_out), (wp, nat_w, w_out))):
            for m in range(c_attn):
                for t in range(tiles):
                    nat[0][m, :, LANE * t:LANE * (t + 1)] = src[pl.ds(m * attn_blk + t * attn_rows, attn_rows), :]
            j = 0
            for k, cnt in ((1, c_si), (3, c_ei)):
                for m in range(0, cnt, groups):
                    some = min(groups, cnt - m)
                    off = small0 + small_blk * (j + m)
                    got = [src[off + small_blk * p:off + small_blk * (p + 1), :] for p in range(some)]
                    got += [jnp.zeros((small_blk, LANE), F32)] * (groups - some)
                    block = pad_rows(jnp.concatenate(lane_swap(got), axis=0), 2 * LANE).T
                    for p in range(some):
                        nat[k][m + p] = block[in_rows * p:in_rows * (p + 1), :narrow]
                j += cnt
            for k, cnt in ((2, c_so), (4, c_eo)):
                for m in range(cnt):
                    off = small0 + small_blk * j
                    for t in range(tiles):
                        nat[k][:, m, LANE * t:LANE * (t + 1)] = src[off + t * out_rows:off + (t + 1) * out_rows, :]
                    j += 1
            for k in range(5):
                out_copy(nat[k], outs[k], which * 5 + k)

    def native_inputs():
        for cp in nat_copies():
            cp.wait()
        for nat, dst in ((nat_m, mp), (nat_w, wp)):
            for m in range(c_attn):
                for t in range(tiles):
                    dst[pl.ds(m * attn_blk + t * attn_rows, attn_rows), :] = nat[0][m, :, LANE * t:LANE * (t + 1)]
            j = 0
            for k, cnt in ((1, c_si), (3, c_ei)):
                for m in range(0, cnt, groups):
                    some = min(groups, cnt - m)
                    block = pad_rows(jnp.concatenate([nat[k][m + p] for p in range(some)], axis=0), LANE)
                    block = jnp.concatenate([block, jnp.zeros((LANE, 2 * LANE - narrow), F32)], axis=1).T
                    got = lane_swap([block[small_blk * q:small_blk * (q + 1)] for q in range(groups)])
                    for p in range(some):
                        dst[pl.ds(small0 + small_blk * (j + m + p), small_blk), :] = got[p]
                j += cnt
            for k, cnt in ((2, c_so), (4, c_eo)):
                for m in range(cnt):
                    rows = [nat[k][:, m, LANE * t:LANE * (t + 1)] for t in range(tiles)]
                    dst[pl.ds(small0 + small_blk * j, small_blk), :] = pad_rows(jnp.concatenate(rows, axis=0), small_blk)
                    j += 1

    def unpack(i, stage_in, stage_out, flat):
        w = waves[i]
        for h in range(2):
            for key in range(nz):
                agd[i, h, key].wait_recv()
        if w["kind"] == "attn":
            for m in range(c_attn):
                for t in range(tiles):
                    out_copies.append(pltpu.make_async_copy(
                        ag.at[:, :, pl.ds(m * attn_blk + t * attn_rows, attn_rows), :],
                        p_attn.at[m, :, :, :, pl.ds(LANE * t, LANE)], s_out.at[10 + m * tiles + t]))
                    out_copies[-1].start()
        elif w["kind"] == "in":
            def body(j, carry):
                off = pl.multiple_of(small0 + small_blk * j, 16)
                for t in range(tiles):
                    devs = [groups * t + p for p in range(groups)]
                    got = lane_swap([ag[d // 2, d % 2, pl.ds(off, small_blk), :].astype(F32) for d in devs])
                    for q, (r, k) in enumerate(cuts):
                        stage_in[j, r:r + k, LANE * t:LANE * (t + 1)] = got[q][:k].astype(BF16)
                return carry
            lax.fori_loop(w["first"], w["first"] + w["cnt"], body, 0)
            k = 10 + c_attn * tiles
            if w["first"] == 0:
                out_copy(stage_in.at[pl.ds(0, c_si)], p_si, k)
                out_copy(stage_in.at[pl.ds(c_si, in_w - c_si)], p_ei.at[pl.ds(0, in_w - c_si)], k + 1)
            else:
                out_copy(stage_in.at[pl.ds(in_w, c_in - in_w)], p_ei.at[pl.ds(in_w - c_si, c_in - in_w)], k + 2)
        else:
            def body(j, carry):
                off = pl.multiple_of(small0 + small_blk * (c_in + j), 16)
                for d in range(n):
                    blk = ag[d // 2, d % 2, pl.ds(off, small_blk), :].astype(F32)
                    for t in range(tiles):
                        flat[out_rows * d:out_rows * (d + 1), LANE * t:LANE * (t + 1)] = blk[t * out_rows:(t + 1) * out_rows]
                stage_out[j] = flat[...].astype(BF16)
                return carry
            lax.fori_loop(0, c_out, body, 0)
            k = 13 + c_attn * tiles
            out_copy(stage_out.at[pl.ds(0, c_so)], p_so, k)
            out_copy(stage_out.at[pl.ds(c_so, c_eo)], p_eo, k + 1)

    pl.run_scoped(load_and_pack, pltpu.VMEM((c_in, narrow, wide), F32), pltpu.VMEM((c_out, narrow, wide), F32))
    def main_phase(stage_in, stage_out, flat):
        native_inputs()
        order = range(n_waves)
        for i in order:
            d2d_copy(i).wait_recv()
            for h in range(2):
                for dr in range(2):
                    rs_send(i, h, dr, 1)
        for s in range(2, hops_far + 1):
            for i in order:
                for h in range(2):
                    for dr in range(2):
                        if s <= hops(h, dr):
                            rs_send(i, h, dr, s)
        for i in order:
            rs_finish(i)
        for i in order:
            x_send(i)
        for i in order:
            owner_work(i)
        for i in order:
            master(i)
            for h in range(2):
                for dr in range(2):
                    ag_send(i, h, dr, 1)
        native_outputs()
        for s in range(2, hops_far + 2):
            for i in order:
                for h in range(2):
                    for dr in range(2):
                        if s <= hops(h, dr) + 1:
                            ag_send(i, h, dr, s)

        for i in order:
            unpack(i, stage_in, stage_out, flat)
        for cp in out_copies:
            cp.wait()

        for cp in pending:
            cp.wait_send()
        for i in order:
            d2d_copy(i).wait_send()
            nrm_wait(i, s_nrm.at[i])
            for m in range(waves[i]["cnt"]):
                owner = (waves[i]["base"] + m) % n

                @pl.when(me != owner)
                def _():
                    x_copy(i, m).wait_send()
            mine, yes = owned(i)

            @pl.when(yes)
            def _():
                view = otx[i].at[pl.ds(0, n - 1)]
                pltpu.make_async_copy(view, view, s_o.at[i]).wait()

    pl.run_scoped(main_phase, pltpu.VMEM((c_in, narrow, wide), BF16), pltpu.VMEM((c_out, narrow, wide), BF16),
                  pltpu.VMEM((narrow, wide), F32))


def hand_over(shapes):
    count = len(shapes)
    pieces = []
    for k, x in enumerate(shapes):
        parts = next((p for p in (4, 2) if x.shape[0] % p == 0 and x.size > 400000), 1)
        step = x.shape[0] // parts
        pieces += [(k, p * step, step) for p in range(parts)]

    def kernel(*refs):
        src, dst, buf, sem_in, sem_out = refs[:count], refs[count:2 * count], refs[2 * count:3 * count], refs[-2], refs[-1]
        first = [pltpu.make_async_copy(src[k].at[pl.ds(r, m)], buf[k].at[pl.ds(r, m)], sem_in.at[i])
                 for i, (k, r, m) in enumerate(pieces)]
        second = [pltpu.make_async_copy(buf[k].at[pl.ds(r, m)], dst[k].at[pl.ds(r, m)], sem_out.at[i])
                  for i, (k, r, m) in enumerate(pieces)]
        for cp in first:
            cp.start()
        for one, two in zip(first, second):
            one.wait()
            two.start()
        for cp in second:
            cp.wait()

    any_spec = pl.BlockSpec(memory_space=pl.ANY)
    return pl.pallas_call(
        kernel, out_shape=shapes, in_specs=[any_spec] * count, out_specs=[any_spec] * count,
        scratch_shapes=[pltpu.VMEM(x.shape, x.dtype) for x in shapes]
        + [pltpu.SemaphoreType.DMA((len(pieces),)), pltpu.SemaphoreType.DMA((len(pieces),))],
        name="hand_over")


def solution(mesh):
    n = mesh.shape["data"]
    nz = n // 2

    def local_step(*arrays):
        grads, moms, masters = arrays[:5], arrays[5:10], arrays[10:]
        counts = tuple(m.shape[0] for m in moms)
        attn_rows, wide = moms[0].shape[1:]
        narrow = moms[1].shape[2]
        c_attn, c_si, c_so, c_ei, c_eo = counts
        c_in, c_out = c_si + c_ei, c_so + c_eo
        tiles = wide // LANE
        small_blk = round_up(tiles * (narrow // n), 16)
        out_pad = round_up(narrow // n, 16)
        attn_blk = attn_rows * tiles
        rows = c_attn * attn_blk + (c_in + c_out) * small_blk
        turn = lambda x: jnp.swapaxes(x, -1, -2)
        grads = [g[0] for g in grads]
        grads[1], grads[3] = turn(grads[1]), turn(grads[3])
        flip = lambda arrs: [jnp.swapaxes(x, 0, 1) if k in (2, 4) else x for k, x in enumerate(arrs)]
        moms, masters = flip(moms), flip(masters)
        grads[0] = grads[0].reshape(c_attn, nz, 2, attn_rows, wide)
        hops = nz // 2

        sds = jax.ShapeDtypeStruct
        out_shape = [sds(m.shape, F32) for m in moms] * 2
        out_shape += [sds((c_attn, nz, 2, attn_rows, wide), BF16)]
        out_shape += [sds((k, narrow, wide), BF16) for k in counts[1:]]
        w_cnt = (c_attn, c_in // 2, c_in - c_in // 2, c_out)
        w_blk = (attn_blk, small_blk, small_blk, out_pad * tiles)
        dma = lambda *shape: pltpu.SemaphoreType.DMA(shape)
        vm = pltpu.VMEM
        scratch = [
            vm((nz, 2, rows, LANE), F32),
            vm((nz, rows, LANE), F32),
            vm((2, 2, hops, rows // 2, LANE), F32),
            vm((nz, 2, rows, LANE), BF16),
            vm((rows, LANE), F32),
            vm((rows, LANE), F32),
            [vm(m.shape, F32) for m in moms],
            [vm(m.shape, F32) for m in moms],
            vm((4, n, 1, LANE), F32),
            [vm((k, b, LANE), BF16) for k, b in zip(w_cnt, w_blk)],
            [vm((n, b, LANE), BF16) for b in w_blk],
            [vm((n, b, LANE), BF16) for b in w_blk],
            [vm((k, b, LANE), BF16) for k, b in zip(w_cnt, w_blk)],
            vm((n * attn_rows, wide), BF16),
            vm((n * attn_rows, n * attn_rows), BF16),
            vm((n * attn_rows, n * attn_rows), BF16),
            dma(6), dma(2, 5), dma(2, 4), dma(4, 4, hops), dma(4, 4, hops),
            dma(4), dma(4), dma(4, max(w_cnt)), dma(4), dma(4), dma(4),
            dma(4, 4, hops), dma(4, 4, hops), dma(4, 2, nz), dma(4, 2, nz),
            dma(15 + c_attn * tiles),
        ]
        any_spec = pl.BlockSpec(memory_space=pl.ANY)
        call = pl.pallas_call(
            functools.partial(fused_step, n, counts, attn_rows, wide, narrow),
            out_shape=out_shape,
            in_specs=[any_spec] * 15,
            out_specs=[any_spec] * 15,
            scratch_shapes=scratch,
            compiler_params=pltpu.CompilerParams(
                collective_id=0, has_side_effects=True, vmem_limit_bytes=67043328),
            name="muon_step",
        )
        outs = list(hand_over(out_shape)(*call(*grads, *moms, *masters)))
        outs[:5], outs[5:10] = flip(outs[:5]), flip(outs[5:10])
        outs[10] = outs[10].reshape(c_attn, n * attn_rows, wide)
        outs[11], outs[13] = turn(outs[11]), turn(outs[13])
        return tuple(outs)

    grad_spec = P(("stage", "data"), None, None, None)
    row_spec = P("stage", "data", None)
    full_spec = P("stage", None, None)
    in_specs = (grad_spec,) * 5 + (row_spec,) * 10
    out_specs = (row_spec,) * 10 + (full_spec,) * 5
    return jax.shard_map(local_step, mesh=mesh, in_specs=in_specs, out_specs=out_specs, check_vma=False)
```

```python
import functools
import math
import jax
import jax.numpy as jnp
from jax import lax
from jax.experimental import pallas as pl
from jax.experimental.pallas import tpu as pltpu
from jax.sharding import PartitionSpec as P

NS_STEPS = 5
MOMENTUM = 0.95
LEARN_RATE = 0.2
WEIGHT_DECAY = 0.25
NORM_EPS = 1e-7
COEF_A = 3.4445
COEF_B = -4.7750
COEF_C = 2.0315

F32 = jnp.float32
BF16 = jnp.bfloat16
MESH = pl.DeviceIdType.MESH
LANE = 128
NT = (((1,), (1,)), ((), ()))


def round_up(value, step):
    return (value + step - 1) // step * step


def fused_step(n, counts, attn_rows, wide, narrow, *refs):
    c_attn, c_si, c_so, c_ei, c_eo = counts
    c_in, c_out = c_si + c_ei, c_so + c_eo
    nz = n // 2
    hops_far, hops_near = nz // 2, nz - 1 - nz // 2
    tiles = wide // LANE
    in_rows = wide // n
    groups = LANE // in_rows
    out_rows = narrow // n
    out_pad = round_up(out_rows, 16)
    attn_blk = attn_rows * tiles
    small_blk = round_up(tiles * out_rows, 16)
    cuts = [(q * small_blk, min(small_blk, narrow - q * small_blk)) for q in range(groups)]
    small0 = c_attn * attn_blk

    it = iter(refs)
    take = lambda k: [next(it) for _ in range(k)]
    g_attn, g_si, g_so, g_ei, g_eo = take(5)
    m_in = take(5)
    w_in = take(5)
    m_out = take(5)
    w_out = take(5)
    p_attn, p_si, p_so, p_ei, p_eo = take(5)
    (gp, rx0, rxr, ag, mp, wp, nat_m, nat_w, nrm, xtx, rxx, otx, rxo, xb, ab, bb,
     raw_in, raw_out, stage_in, stage_out, flat) = take(21)
    (s_load, s_nat, s_d2d, s_rs, r_rs, s_nrm, r_nrm, s_x, r_x, s_o, r_o, s_ag, r_ag, s_agd, r_agd, s_out) = take(16)

    in_w = c_in // 2
    waves = []
    base = 0
    for kind, first, cnt in (("in", 0, in_w), ("in", in_w, c_in - in_w), ("out", c_in, c_out)):
        waves.append(dict(kind=kind, first=first, cnt=cnt, row0=small0 + first * small_blk, blk=small_blk, base=base % n))
        base += cnt
    waves.insert(0, dict(kind="attn", first=0, cnt=c_attn, row0=0, blk=attn_blk, base=base % n))
    n_waves = len(waves)
    for w in waves:
        w["rows"] = w["cnt"] * w["blk"]
        w["half"] = w["rows"] // 2
        w["off"] = w["row0"] // 2
        w["ag_half"] = round_up(w["half"], 16)

    me = lax.axis_index("data")
    z = me // 2
    c = lax.rem(me, 2)
    zmod = lambda v: lax.rem(v + 2 * nz, nz)
    dev = lambda zz, cc: {"data": zz * 2 + cc}
    partner = {"data": z * 2 + (1 - c)}
    others = [lax.rem(me + k, n) for k in range(1, n)]

    def remote(src, dst, ss, rs, where):
        return pltpu.make_async_remote_copy(src_ref=src, dst_ref=dst, send_sem=ss, recv_sem=rs,
                                            device_id=where, device_id_type=MESH)

    barrier = pltpu.get_barrier_semaphore()
    for d in others:
        pl.semaphore_signal(barrier, inc=1, device_id={"data": d}, device_id_type=MESH)

    def nat_copies():
        return [pltpu.make_async_copy(srcs[k], dsts[k], s_nat.at[which, k])
                for which, (srcs, dsts) in enumerate(((m_in, nat_m), (w_in, nat_w))) for k in range(5)]

    def lane_swap(blocks):
        lane = lax.broadcasted_iota(jnp.int32, (1, LANE), 1)
        blocks = list(blocks)
        dist = groups // 2
        while dist:
            width = dist * in_rows
            low = lax.rem(lane // width, 2) == 0
            for q in range(groups):
                if (q // dist) % 2 == 0:
                    x, y = blocks[q], blocks[q + dist]
                    blocks[q] = jnp.where(low, x, pltpu.roll(y, width, axis=1))
                    blocks[q + dist] = jnp.where(low, pltpu.roll(x, LANE - width, axis=1), y)
            dist //= 2
        return blocks

    def pad_rows(x, rows):
        if x.shape[0] == rows:
            return x
        return jnp.concatenate([x, jnp.zeros((rows - x.shape[0], x.shape[1]), x.dtype)], axis=0)

    k_cut = in_w - c_si

    def loads():
        return [
            pltpu.make_async_copy(g_si, raw_in.at[pl.ds(0, c_si)], s_load.at[1]),
            pltpu.make_async_copy(g_ei.at[pl.ds(0, k_cut)], raw_in.at[pl.ds(c_si, k_cut)], s_load.at[2]),
            pltpu.make_async_copy(g_ei.at[pl.ds(k_cut, c_ei - k_cut)], raw_in.at[pl.ds(in_w, c_ei - k_cut)], s_load.at[3]),
            pltpu.make_async_copy(g_so, raw_out.at[pl.ds(0, c_so)], s_load.at[4]),
            pltpu.make_async_copy(g_eo, raw_out.at[pl.ds(c_so, c_eo)], s_load.at[5]),
        ]

    def start_loads():
        for m in range(c_attn):
            for t in range(tiles):
                pltpu.make_async_copy(
                    g_attn.at[m, :, :, :, pl.ds(LANE * t, LANE)],
                    gp.at[:, :, pl.ds(m * attn_blk + t * attn_rows, attn_rows), :], s_load.at[0]).start()
        for cp in loads() + nat_copies():
            cp.start()

    def pack_in(j, carry):
        off = pl.multiple_of(small0 + small_blk * j, 8)
        for t in range(tiles):
            cols = slice(LANE * t, LANE * (t + 1))
            got = lane_swap([pad_rows(raw_in[j, r:r + k, cols], small_blk) for r, k in cuts])
            for p in range(groups):
                d = groups * t + p
                gp[d // 2, d % 2, pl.ds(off, small_blk), :] = got[p]
        return carry

    def pack_out(j, carry):
        off = pl.multiple_of(small0 + small_blk * (c_in + j), 8)
        for d in range(n):
            rows = [raw_out[j, out_rows * d:out_rows * (d + 1), LANE * t:LANE * (t + 1)] for t in range(tiles)]
            gp[d // 2, d % 2, pl.ds(off, small_blk), :] = pad_rows(jnp.concatenate(rows, axis=0), small_blk)
        return carry

    def pack(i):
        load = loads()
        if i == 0:
            view = gp.at[:, :, pl.ds(0, small0), :]
            pltpu.make_async_copy(view, view, s_load.at[0]).wait()
            pl.semaphore_wait(barrier, n - 1)
        elif i == 1:
            load[0].wait()
            load[1].wait()
            lax.fori_loop(0, in_w, pack_in, 0)
        elif i == 2:
            load[2].wait()
            lax.fori_loop(in_w, c_in, pack_in, 0)
        else:
            load[3].wait()
            load[4].wait()
            lax.fori_loop(0, c_out, pack_out, 0)
        for k in near_last:
            d2d_copy(i, k).start()

    pending = []

    near_last = [hops_far]
    for k in range(hops_near, 0, -1):
        near_last += [k, nz - k]
    near_last.append(0)
    d2d_seen = set()

    def d2d_copy(i, k):
        sl = pl.ds(waves[i]["row0"], waves[i]["rows"])
        dest = zmod(z + k)
        return remote(gp.at[dest, 1 - c, sl, :], rx0.at[dest, sl, :], s_d2d.at[0, i, k], s_d2d.at[1, i, k], partner)

    def d2d_wait(i, k):
        if (i, k) not in d2d_seen:
            d2d_seen.add((i, k))
            d2d_copy(i, k).wait_recv()

    hops = lambda h, dr: hops_far if h == dr else hops_near
    rs = {}

    def rs_send(i, h, dr, s):
        w = waves[i]
        length = hops(h, dr)
        step = length - s + 1
        dest = zmod(z + step) if dr == 0 else zmod(z - step)
        d2d_wait(i, step if dr == 0 else nz - step)
        sl = pl.ds(w["row0"] + h * w["half"], w["half"])
        osl = pl.ds(w["off"], w["half"])
        val = gp[dest, c, sl, :] + rx0[dest, sl, :]
        if s > 1:
            rs[i, h, dr, s - 1].wait_recv()
            val = val + rxr[dr, h, s - 2, osl, :]
        gp[dest, c, sl, :] = val
        where = dev(zmod(z + 1), c) if dr == 0 else dev(zmod(z - 1), c)
        cp = remote(gp.at[dest, c, sl, :], rxr.at[dr, h, s - 1, osl, :],
                    s_rs.at[i, h * 2 + dr, s - 1], r_rs.at[i, h * 2 + dr, s - 1], where)
        cp.start()
        rs[i, h, dr, s] = cp
        pending.append(cp)

    def rs_finish(i):
        w = waves[i]
        d2d_wait(i, 0)
        for h in range(2):
            sl = pl.ds(w["row0"] + h * w["half"], w["half"])
            osl = pl.ds(w["off"], w["half"])
            total = gp[z, c, sl, :] + rx0[z, sl, :]
            for dr in range(2):
                last = hops(h, dr)
                rs[i, h, dr, last].wait_recv()
                total = total + rxr[dr, h, last - 1, osl, :]
            mp[sl, :] = MOMENTUM * mp[sl, :] + total / n
        lane = lax.broadcasted_iota(jnp.int32, (1, LANE), 1)
        part = jnp.zeros((1, LANE), F32)
        for m in range(w["cnt"]):
            block = mp[pl.ds(w["row0"] + m * w["blk"], w["blk"]), :]
            sq = jnp.sum(jnp.sum(block * block, axis=0, keepdims=True), axis=1, keepdims=True)
            part = jnp.where(lane == m, sq, part)
        nrm[i, me] = part
        for d in others:
            remote(nrm.at[i, me], nrm.at[i, me], s_nrm.at[i], r_nrm.at[i], {"data": d}).start()

    def nrm_wait(i, sem):
        view = nrm.at[i, pl.ds(0, n - 1)]
        pltpu.make_async_copy(view, view, sem).wait()

    def x_copy(i, m):
        w = waves[i]
        owner = (w["base"] + m) % n
        return remote(xtx[i].at[m], rxx[i].at[me], s_x.at[i, m], r_x.at[i], {"data": owner})

    def x_send(i):
        w = waves[i]
        nrm_wait(i, r_nrm.at[i])
        tot = jnp.zeros((1, LANE), F32)
        for d in range(n):
            tot = tot + nrm[i, d]
        lane = lax.broadcasted_iota(jnp.int32, (1, LANE), 1)
        for m in range(w["cnt"]):
            sq = jnp.sum(jnp.where(lane == m, tot, 0.0), axis=1, keepdims=True)
            x = mp[pl.ds(w["row0"] + m * w["blk"], w["blk"]), :] / (jnp.sqrt(sq) + NORM_EPS)
            if w["kind"] == "out":
                zero = jnp.zeros((out_pad - out_rows, LANE), F32)
                parts = []
                for t in range(tiles):
                    parts += [x[t * out_rows:(t + 1) * out_rows], zero]
                x = jnp.concatenate(parts, axis=0)
            x = x.astype(BF16)
            xtx[i][m] = x
            owner = (w["base"] + m) % n

            @pl.when(me != owner)
            def _():
                x_copy(i, m).start()

            @pl.when(me == owner)
            def _():
                rxx[i][me] = x

    def owned(i):
        w = waves[i]
        mine = lax.rem(me - w["base"] + n, n)
        return mine, mine < w["cnt"]

    def assemble(i):
        kind = waves[i]["kind"]
        rx = rxx[i]
        if kind == "attn":
            for t in range(tiles):
                xb[:, LANE * t:LANE * (t + 1)] = rx[:, attn_rows * t:attn_rows * (t + 1), :].reshape(n * attn_rows, LANE)
        elif kind == "out":
            for t in range(tiles):
                xb[:n * out_pad, LANE * t:LANE * (t + 1)] = rx[:, out_pad * t:out_pad * (t + 1), :].reshape(n * out_pad, LANE)
        else:
            for t in range(tiles):
                got = lane_swap([rx[groups * t + p].astype(F32) for p in range(groups)])
                for q, (r, k) in enumerate(cuts):
                    xb[r:r + k, LANE * t:LANE * (t + 1)] = got[q][:k].astype(BF16)
            xb[narrow:n * out_pad, :] = jnp.zeros((n * out_pad - narrow, wide), BF16)

    def disassemble(i):
        kind = waves[i]["kind"]
        tx = otx[i]
        if kind == "attn":
            for t in range(tiles):
                tx[:, attn_rows * t:attn_rows * (t + 1), :] = xb[:, LANE * t:LANE * (t + 1)].reshape(n, attn_rows, LANE)
        elif kind == "out":
            for t in range(tiles):
                tx[:, out_pad * t:out_pad * (t + 1), :] = xb[:n * out_pad, LANE * t:LANE * (t + 1)].reshape(n, out_pad, LANE)
        else:
            for t in range(tiles):
                cols = slice(LANE * t, LANE * (t + 1))
                got = lane_swap([pad_rows(xb[r:r + k, cols].astype(F32), small_blk) for r, k in cuts])
                for p in range(groups):
                    tx[groups * t + p] = got[p].astype(BF16)

    def iterate(size, steps):
        cut = min(size, 256)

        def one(_, carry):
            for r in range(size // cut):
                sl = slice(r * cut, (r + 1) * cut)
                gram = lax.dot_general(xb[sl, :], xb[:size, :], NT, preferred_element_type=F32)
                ab[sl, :size] = gram.astype(BF16)
            for r in range(size // cut):
                sl = slice(r * cut, (r + 1) * cut)
                square = jnp.dot(ab[sl, :size], ab[:size, :size], preferred_element_type=F32)
                bb[sl, :size] = (COEF_B * ab[sl, :size].astype(F32) + COEF_C * square).astype(BF16)
            for r in range(wide // 256):
                sl = slice(r * 256, (r + 1) * 256)
                update = jnp.dot(bb[:size, :size], xb[:size, sl], preferred_element_type=F32)
                xb[:size, sl] = (COEF_A * xb[:size, sl].astype(F32) + update).astype(BF16)
            return carry

        lax.fori_loop(0, steps, one, 0)

    def o_copy(i, mine, d):
        return remote(otx[i].at[d], rxo[i].at[mine], s_o.at[i], r_o.at[i], {"data": d})

    def owner_work(i, begin, steps, end):
        mine, yes = owned(i)

        @pl.when(yes)
        def _():
            if begin:
                view = rxx[i].at[pl.ds(0, n - 1)]
                pltpu.make_async_copy(view, view, r_x.at[i]).wait()
                assemble(i)
            iterate(n * attn_rows if waves[i]["kind"] == "attn" else n * out_pad, steps)
            if end:
                disassemble(i)
                for d in others:
                    o_copy(i, mine, d).start()
                rxo[i][mine] = otx[i][me]

    def master(i):
        w = waves[i]
        mine, yes = owned(i)
        cnt = w["cnt"]

        @pl.when(yes)
        def _():
            view = rxo[i].at[pl.ds(0, cnt - 1)]
            pltpu.make_async_copy(view, view, r_o.at[i]).wait()

        @pl.when(jnp.logical_not(yes))
        def _():
            pltpu.make_async_copy(rxo[i], rxo[i], r_o.at[i]).wait()

        step_scale = 0.2 * math.sqrt(wide)
        for m in range(cnt):
            sl = pl.ds(w["row0"] + m * w["blk"], w["blk"])
            o = rxo[i][m].astype(F32)
            if w["kind"] == "out":
                parts = [o[out_pad * t:out_pad * t + out_rows] for t in range(tiles)]
                parts.append(jnp.zeros((small_blk - tiles * out_rows, LANE), F32))
                o = jnp.concatenate(parts, axis=0)
            old = wp[sl, :]
            new = old - LEARN_RATE * (step_scale * o + WEIGHT_DECAY * old)
            wp[sl, :] = new
            ag[z, c, sl, :] = new.astype(BF16)

    agc = {}
    agd = {}

    def ag_rows(i, h):
        w = waves[i]
        if h == 0:
            return pl.ds(w["row0"], w["ag_half"])
        return pl.ds(w["row0"] + w["ag_half"], w["rows"] - w["ag_half"])

    def ag_to_partner(i, h, src, key):
        part = ag.at[src, c, ag_rows(i, h), :]
        cp = remote(part, part, s_agd.at[i, h, key], r_agd.at[i, h, key], partner)
        cp.start()
        agd[i, h, key] = cp
        pending.append(cp)

    def ag_send(i, h, dr, s):
        length = hops(h, dr)
        src = z if s == 1 else (zmod(z - (s - 1)) if dr == 0 else zmod(z + (s - 1)))
        if s > 1:
            agc[i, h, dr, s - 1].wait_recv()
        if s <= length:
            part = ag.at[src, c, ag_rows(i, h), :]
            where = dev(zmod(z + 1), c) if dr == 0 else dev(zmod(z - 1), c)
            cp = remote(part, part, s_ag.at[i, h * 2 + dr, s - 1], r_ag.at[i, h * 2 + dr, s - 1], where)
            cp.start()
            agc[i, h, dr, s] = cp
            pending.append(cp)
        if s > 1:
            ag_to_partner(i, h, src, (s - 1) if dr == 0 else nz - (s - 1))
        elif dr == 0:
            ag_to_partner(i, h, src, 0)

    out_copies = []

    def out_copy(src, dst, k):
        cp = pltpu.make_async_copy(src, dst, s_out.at[k])
        cp.start()
        out_copies.append(cp)

    def native_outputs(which):
        for src, nat, outs in (((mp, nat_m, m_out), (wp, nat_w, w_out))[which],):
            for m in range(c_attn):
                for t in range(tiles):
                    nat[0][m, :, LANE * t:LANE * (t + 1)] = src[pl.ds(m * attn_blk + t * attn_rows, attn_rows), :]
            j = 0
            for k, cnt in ((1, c_si), (3, c_ei)):
                for m in range(0, cnt, groups):
                    some = min(groups, cnt - m)
                    off = small0 + small_blk * (j + m)
                    got = [src[off + small_blk * p:off + small_blk * (p + 1), :] for p in range(some)]
                    got += [jnp.zeros((small_blk, LANE), F32)] * (groups - some)
                    block = pad_rows(jnp.concatenate(lane_swap(got), axis=0), 2 * LANE).T
                    for p in range(some):
                        nat[k][m + p] = block[in_rows * p:in_rows * (p + 1), :narrow]
                j += cnt
            for k, cnt in ((2, c_so), (4, c_eo)):
                for m in range(cnt):
                    off = small0 + small_blk * j
                    for t in range(tiles):
                        nat[k][:, m, LANE * t:LANE * (t + 1)] = src[off + t * out_rows:off + (t + 1) * out_rows, :]
                    j += 1
            for k in range(5):
                out_copy(nat[k], outs[k], which * 5 + k)

    def native_inputs(which):
        for cp in nat_copies()[5 * which:5 * which + 5]:
            cp.wait()
        for nat, dst in (((nat_m, mp), (nat_w, wp))[which],):
            for m in range(c_attn):
                for t in range(tiles):
                    dst[pl.ds(m * attn_blk + t * attn_rows, attn_rows), :] = nat[0][m, :, LANE * t:LANE * (t + 1)]
            j = 0
            for k, cnt in ((1, c_si), (3, c_ei)):
                for m in range(0, cnt, groups):
                    some = min(groups, cnt - m)
                    block = pad_rows(jnp.concatenate([nat[k][m + p] for p in range(some)], axis=0), LANE)
                    block = jnp.concatenate([block, jnp.zeros((LANE, 2 * LANE - narrow), F32)], axis=1).T
                    got = lane_swap([block[small_blk * q:small_blk * (q + 1)] for q in range(groups)])
                    for p in range(some):
                        dst[pl.ds(small0 + small_blk * (j + m + p), small_blk), :] = got[p]
                j += cnt
            for k, cnt in ((2, c_so), (4, c_eo)):
                for m in range(cnt):
                    rows = [nat[k][:, m, LANE * t:LANE * (t + 1)] for t in range(tiles)]
                    dst[pl.ds(small0 + small_blk * j, small_blk), :] = pad_rows(jnp.concatenate(rows, axis=0), small_blk)
                    j += 1

    def unpack(i):
        w = waves[i]
        for h in range(2):
            for key in range(nz):
                agd[i, h, key].wait_recv()
        if w["kind"] == "attn":
            for m in range(c_attn):
                for t in range(tiles):
                    out_copies.append(pltpu.make_async_copy(
                        ag.at[:, :, pl.ds(m * attn_blk + t * attn_rows, attn_rows), :],
                        p_attn.at[m, :, :, :, pl.ds(LANE * t, LANE)], s_out.at[10 + m * tiles + t]))
                    out_copies[-1].start()
        elif w["kind"] == "in":
            def body(j, carry):
                off = pl.multiple_of(small0 + small_blk * j, 16)
                for t in range(tiles):
                    devs = [groups * t + p for p in range(groups)]
                    got = lane_swap([ag[d // 2, d % 2, pl.ds(off, small_blk), :].astype(F32) for d in devs])
                    for q, (r, k) in enumerate(cuts):
                        stage_in[j, r:r + k, LANE * t:LANE * (t + 1)] = got[q][:k].astype(BF16)
                return carry
            lax.fori_loop(w["first"], w["first"] + w["cnt"], body, 0)
            k = 10 + c_attn * tiles
            if w["first"] == 0:
                out_copy(stage_in.at[pl.ds(0, c_si)], p_si, k)
                out_copy(stage_in.at[pl.ds(c_si, in_w - c_si)], p_ei.at[pl.ds(0, in_w - c_si)], k + 1)
            else:
                out_copy(stage_in.at[pl.ds(in_w, c_in - in_w)], p_ei.at[pl.ds(in_w - c_si, c_in - in_w)], k + 2)
        else:
            def body(j, carry):
                off = pl.multiple_of(small0 + small_blk * (c_in + j), 16)
                for d in range(n):
                    blk = ag[d // 2, d % 2, pl.ds(off, small_blk), :].astype(F32)
                    for t in range(tiles):
                        flat[out_rows * d:out_rows * (d + 1), LANE * t:LANE * (t + 1)] = blk[t * out_rows:(t + 1) * out_rows]
                stage_out[j] = flat[...].astype(BF16)
                return carry
            lax.fori_loop(0, c_out, body, 0)
            k = 13 + c_attn * tiles
            out_copy(stage_out.at[pl.ds(0, c_so)], p_so, k)
            out_copy(stage_out.at[pl.ds(c_so, c_eo)], p_eo, k + 1)

    def rs_stage(i, s):
        for h in range(2):
            for dr in range(2):
                if s <= hops(h, dr):
                    rs_send(i, h, dr, s)

    def ag_stage(i, s):
        for h in range(2):
            for dr in range(2):
                if s <= hops(h, dr) + 1:
                    ag_send(i, h, dr, s)

    start_loads()
    pack(0)
    pack(1)
    rs_stage(0, 1)
    native_inputs(0)
    rs_stage(0, 2)
    pack(2)
    rs_stage(0, 3)
    rs_stage(1, 1)
    pack(3)
    rs_stage(0, 4)
    rs_stage(1, 2)
    native_inputs(1)
    rs_stage(1, 3)
    rs_stage(2, 1)
    rs_finish(0)
    rs_stage(1, 4)
    rs_stage(2, 2)
    x_send(0)
    rs_stage(2, 3)
    rs_stage(3, 1)
    rs_finish(1)
    owner_work(0, True, 1, False)
    x_send(1)
    rs_stage(2, 4)
    rs_stage(3, 2)
    owner_work(0, False, 2, False)
    rs_stage(3, 3)
    rs_finish(2)
    owner_work(0, False, NS_STEPS - 3, True)
    rs_stage(3, 4)
    x_send(2)
    owner_work(1, True, NS_STEPS, True)
    master(0)
    ag_stage(0, 1)
    rs_finish(3)
    ag_stage(0, 2)
    owner_work(2, True, NS_STEPS, True)
    x_send(3)
    master(1)
    ag_stage(1, 1)
    ag_stage(0, 3)
    owner_work(3, True, NS_STEPS, True)
    master(2)
    ag_stage(2, 1)
    ag_stage(1, 2)
    ag_stage(0, 4)
    master(3)
    ag_stage(3, 1)
    ag_stage(2, 2)
    ag_stage(1, 3)
    ag_stage(0, 5)
    native_outputs(0)
    ag_stage(3, 2)
    ag_stage(2, 3)
    ag_stage(1, 4)
    native_outputs(1)
    ag_stage(3, 3)
    ag_stage(2, 4)
    ag_stage(1, 5)
    unpack(0)
    ag_stage(3, 4)
    ag_stage(2, 5)
    unpack(1)
    ag_stage(3, 5)
    unpack(2)
    unpack(3)

    for cp in out_copies:
        cp.wait()
    for cp in pending:
        cp.wait_send()
    for i in range(n_waves):
        for k in range(nz):
            d2d_copy(i, k).wait_send()
        nrm_wait(i, s_nrm.at[i])
        for m in range(waves[i]["cnt"]):
            owner = (waves[i]["base"] + m) % n

            @pl.when(me != owner)
            def _():
                x_copy(i, m).wait_send()
        mine, yes = owned(i)

        @pl.when(yes)
        def _():
            view = otx[i].at[pl.ds(0, n - 1)]
            pltpu.make_async_copy(view, view, s_o.at[i]).wait()


def hand_over(shapes):
    count = len(shapes)
    pieces = []
    for k, x in enumerate(shapes):
        parts = next((p for p in (4, 2) if x.shape[0] % p == 0 and x.size > 400000), 1)
        step = x.shape[0] // parts
        pieces += [(k, p * step, step) for p in range(parts)]

    def kernel(*refs):
        src, dst, buf, sem_in, sem_out = refs[:count], refs[count:2 * count], refs[2 * count:3 * count], refs[-2], refs[-1]
        first = [pltpu.make_async_copy(src[k].at[pl.ds(r, m)], buf[k].at[pl.ds(r, m)], sem_in.at[i])
                 for i, (k, r, m) in enumerate(pieces)]
        second = [pltpu.make_async_copy(buf[k].at[pl.ds(r, m)], dst[k].at[pl.ds(r, m)], sem_out.at[i])
                  for i, (k, r, m) in enumerate(pieces)]
        for cp in first:
            cp.start()
        for one, two in zip(first, second):
            one.wait()
            two.start()
        for cp in second:
            cp.wait()

    any_spec = pl.BlockSpec(memory_space=pl.ANY)
    return pl.pallas_call(
        kernel, out_shape=shapes, in_specs=[any_spec] * count, out_specs=[any_spec] * count,
        scratch_shapes=[pltpu.VMEM(x.shape, x.dtype) for x in shapes]
        + [pltpu.SemaphoreType.DMA((len(pieces),)), pltpu.SemaphoreType.DMA((len(pieces),))],
        name="hand_over")


def solution(mesh):
    n = mesh.shape["data"]
    nz = n // 2

    def local_step(*arrays):
        grads, moms, masters = arrays[:5], arrays[5:10], arrays[10:]
        counts = tuple(m.shape[0] for m in moms)
        attn_rows, wide = moms[0].shape[1:]
        narrow = moms[1].shape[2]
        c_attn, c_si, c_so, c_ei, c_eo = counts
        c_in, c_out = c_si + c_ei, c_so + c_eo
        tiles = wide // LANE
        small_blk = round_up(tiles * (narrow // n), 16)
        out_pad = round_up(narrow // n, 16)
        attn_blk = attn_rows * tiles
        rows = c_attn * attn_blk + (c_in + c_out) * small_blk
        turn = lambda x: jnp.swapaxes(x, -1, -2)
        grads = [g[0] for g in grads]
        grads[1], grads[3] = turn(grads[1]), turn(grads[3])
        flip = lambda arrs: [jnp.swapaxes(x, 0, 1) if k in (2, 4) else x for k, x in enumerate(arrs)]
        moms, masters = flip(moms), flip(masters)
        grads[0] = grads[0].reshape(c_attn, nz, 2, attn_rows, wide)
        hops = nz // 2

        sds = jax.ShapeDtypeStruct
        out_shape = [sds(m.shape, F32) for m in moms] * 2
        out_shape += [sds((c_attn, nz, 2, attn_rows, wide), BF16)]
        out_shape += [sds((k, narrow, wide), BF16) for k in counts[1:]]
        w_cnt = (c_attn, c_in // 2, c_in - c_in // 2, c_out)
        w_blk = (attn_blk, small_blk, small_blk, out_pad * tiles)
        dma = lambda *shape: pltpu.SemaphoreType.DMA(shape)
        vm = pltpu.VMEM
        scratch = [
            vm((nz, 2, rows, LANE), F32),
            vm((nz, rows, LANE), F32),
            vm((2, 2, hops, rows // 2, LANE), F32),
            vm((nz, 2, rows, LANE), BF16),
            vm((rows, LANE), F32),
            vm((rows, LANE), F32),
            [vm(m.shape, F32) for m in moms],
            [vm(m.shape, F32) for m in moms],
            vm((4, n, 1, LANE), F32),
            [vm((k, b, LANE), BF16) for k, b in zip(w_cnt, w_blk)],
            [vm((n, b, LANE), BF16) for b in w_blk],
            [vm((n, b, LANE), BF16) for b in w_blk],
            [vm((k, b, LANE), BF16) for k, b in zip(w_cnt, w_blk)],
            vm((n * attn_rows, wide), BF16),
            vm((n * attn_rows, n * attn_rows), BF16),
            vm((n * attn_rows, n * attn_rows), BF16),
            vm((c_in, narrow, wide), F32),
            vm((c_out, narrow, wide), F32),
            vm((c_in, narrow, wide), BF16),
            vm((c_out, narrow, wide), BF16),
            vm((narrow, wide), F32),
            dma(6), dma(2, 5), dma(2, 4, nz), dma(4, 4, hops), dma(4, 4, hops),
            dma(4), dma(4), dma(4, max(w_cnt)), dma(4), dma(4), dma(4),
            dma(4, 4, hops), dma(4, 4, hops), dma(4, 2, nz), dma(4, 2, nz),
            dma(15 + c_attn * tiles),
        ]
        any_spec = pl.BlockSpec(memory_space=pl.ANY)
        call = pl.pallas_call(
            functools.partial(fused_step, n, counts, attn_rows, wide, narrow),
            out_shape=out_shape,
            in_specs=[any_spec] * 15,
            out_specs=[any_spec] * 15,
            scratch_shapes=scratch,
            compiler_params=pltpu.CompilerParams(
                collective_id=0, has_side_effects=True, vmem_limit_bytes=67043328),
            name="muon_step",
        )
        outs = list(hand_over(out_shape)(*call(*grads, *moms, *masters)))
        outs[:5], outs[5:10] = flip(outs[:5]), flip(outs[5:10])
        outs[10] = outs[10].reshape(c_attn, n * attn_rows, wide)
        outs[11], outs[13] = turn(outs[11]), turn(outs[13])
        return tuple(outs)

    grad_spec = P(("stage", "data"), None, None, None)
    row_spec = P("stage", "data", None)
    full_spec = P("stage", None, None)
    in_specs = (grad_spec,) * 5 + (row_spec,) * 10
    out_specs = (row_spec,) * 10 + (full_spec,) * 5
    return jax.shard_map(local_step, mesh=mesh, in_specs=in_specs, out_specs=out_specs, check_vma=False)
```

```python
import functools
import math
import jax
import jax.numpy as jnp
from jax import lax
from jax.experimental import pallas as pl
from jax.experimental.pallas import tpu as pltpu
from jax.sharding import PartitionSpec as P

NS_STEPS = 5
MOMENTUM = 0.95
LEARN_RATE = 0.2
WEIGHT_DECAY = 0.25
NORM_EPS = 1e-7
COEF_A = 3.4445
COEF_B = -4.7750
COEF_C = 2.0315

SCHEDULE = (
    ("pack", 0), ("rs", 0, 0, 1), ("pack", 1), ("rs", 0, 1, 1), ("rs", 0, 0, 2), ("rs", 0, 1, 2), ("pack", 2),
    ("rs", 0, 0, 3), ("nat", 1), ("rs", 0, 1, 3), ("rs", 1, 0, 1), ("rs", 0, 0, 4), ("nat", 0), ("rs", 0, 1, 4),
    ("rs", 1, 1, 1), ("pack", 3), ("fin", 0), ("rs", 1, 0, 2), ("rs", 1, 1, 2), ("rs", 1, 0, 3), ("rs", 2, 0, 1),
    ("rs", 1, 0, 4), ("rs", 2, 1, 1), ("rs", 1, 1, 3), ("rs", 1, 1, 4), ("x", 0), ("rs", 2, 0, 2), ("rs", 2, 1, 2),
    ("rs", 3, 1, 1), ("fin", 1), ("own", 0, 1), ("rs", 2, 0, 3), ("own", 0, 2), ("rs", 2, 1, 3), ("rs", 3, 0, 1),
    ("own", 0, 3), ("rs", 2, 0, 4), ("rs", 2, 1, 4), ("x", 1), ("fin", 2), ("rs", 3, 0, 2), ("rs", 3, 1, 2),
    ("mas", 0), ("rs", 3, 0, 3), ("rs", 3, 1, 3), ("ag", 0, 1, 1), ("own", 1, 0), ("rs", 3, 0, 4), ("rs", 3, 1, 4),
    ("x", 2), ("ag", 0, 0, 1), ("fin", 3), ("ag", 0, 0, 2), ("ag", 0, 1, 2), ("mas", 1), ("ag", 1, 0, 1),
    ("ag", 1, 1, 1), ("own", 2, 0), ("x", 3), ("ag", 0, 0, 3), ("ag", 0, 1, 3), ("ag", 1, 0, 2), ("ag", 0, 0, 4),
    ("ag", 1, 1, 2), ("mas", 2), ("ag", 2, 0, 1), ("ag", 2, 1, 1), ("own", 3, 0), ("ag", 1, 1, 3), ("ag", 0, 1, 4),
    ("natout", 0), ("ag", 0, 0, 5), ("ag", 1, 0, 3), ("ag", 2, 0, 2), ("ag", 0, 1, 5), ("ag", 2, 1, 2), ("mas", 3),
    ("ag", 3, 1, 1), ("ag", 3, 0, 1), ("ag", 2, 0, 3), ("ag", 1, 1, 4), ("ag", 2, 1, 3), ("ag", 1, 0, 4),
    ("ag", 3, 0, 2), ("ag", 3, 1, 2), ("ag", 1, 1, 5), ("ag", 2, 0, 4), ("ag", 1, 0, 5), ("ag", 2, 1, 4),
    ("natout", 1), ("un", 0), ("ag", 3, 1, 3), ("ag", 3, 0, 3), ("un", 1), ("ag", 2, 0, 5), ("ag", 2, 1, 5),
    ("ag", 3, 0, 4), ("ag", 3, 1, 4), ("un", 2), ("ag", 3, 0, 5), ("ag", 3, 1, 5), ("un", 3),
)

F32 = jnp.float32
BF16 = jnp.bfloat16
MESH = pl.DeviceIdType.MESH
LANE = 128
NT = (((1,), (1,)), ((), ()))


def round_up(value, step):
    return (value + step - 1) // step * step


def fused_step(n, counts, attn_rows, wide, narrow, *refs):
    c_attn, c_si, c_so, c_ei, c_eo = counts
    c_in, c_out = c_si + c_ei, c_so + c_eo
    nz = n // 2
    hops_far, hops_near = nz // 2, nz - 1 - nz // 2
    tiles = wide // LANE
    in_rows = wide // n
    groups = LANE // in_rows
    out_rows = narrow // n
    out_pad = round_up(out_rows, 16)
    attn_blk = attn_rows * tiles
    out_blk = tiles * out_rows
    small_blk = round_up(out_blk, 16)
    cuts = [(q * small_blk, min(small_blk, narrow - q * small_blk)) for q in range(groups)]

    it = iter(refs)
    take = lambda k: [next(it) for _ in range(k)]
    g_attn, g_si, g_so, g_ei, g_eo = take(5)
    m_in = take(5)
    w_in = take(5)
    m_out = take(5)
    w_out = take(5)
    p_attn, p_si, p_so, p_ei, p_eo = take(5)
    (gp, rx0, rxr, ag, mp, wp, nat_m, nat_w, nrm, xtx, rxx, otx, rxo, xb, ab, bb,
     raw_in, raw_out, stage_in, stage_out) = take(20)
    (s_load, s_nat, s_d2d, s_rs, r_rs, s_nrm, r_nrm, s_x, r_x, s_o, r_o, s_ag, r_ag, s_agd, r_agd, s_out) = take(16)

    quad = narrow
    n_quads = c_ei // groups
    quads_b = n_quads // 2
    mats_b, mats_c = c_si + groups * quads_b, groups * (n_quads - quads_b)
    rows_b, rows_c = c_si * small_blk + quads_b * quad, (n_quads - quads_b) * quad
    rows_d = round_up(c_out * out_blk, 16)
    waves = [dict(kind="attn", cnt=c_attn, rows=c_attn * attn_blk, base=(c_in + c_out) % n),
             dict(kind="in", cnt=mats_b, rows=rows_b, base=0, shared=c_si, quads=quads_b, first=0),
             dict(kind="in", cnt=mats_c, rows=rows_c, base=mats_b % n, shared=0, quads=n_quads - quads_b, first=quads_b),
             dict(kind="out", cnt=c_out, rows=rows_d, base=c_in % n)]
    n_waves = len(waves)
    start = 0
    for w in waves:
        w["row0"] = start
        start += w["rows"]
        w["half"] = w["rows"] // 2
        w["off"] = w["row0"] // 2
        w["ag_half"] = round_up(w["half"], 16)
        w["quad0"] = w["row0"] + w.get("shared", 0) * small_blk
    out0 = waves[3]["row0"]

    me = lax.axis_index("data")
    z = me // 2
    c = lax.rem(me, 2)
    zmod = lambda v: lax.rem(v + 2 * nz, nz)
    dev = lambda zz, cc: {"data": zz * 2 + cc}
    partner = {"data": z * 2 + (1 - c)}
    others = [lax.rem(me + k, n) for k in range(1, n)]

    def remote(src, dst, ss, rs, where):
        return pltpu.make_async_remote_copy(src_ref=src, dst_ref=dst, send_sem=ss, recv_sem=rs,
                                            device_id=where, device_id_type=MESH)

    barrier = pltpu.get_barrier_semaphore()
    for d in others:
        pl.semaphore_signal(barrier, inc=1, device_id={"data": d}, device_id_type=MESH)

    def nat_copies():
        return [pltpu.make_async_copy(srcs[k], dsts[k], s_nat.at[which, k])
                for which, (srcs, dsts) in enumerate(((m_in, nat_m), (w_in, nat_w))) for k in range(5)]

    def lane_swap(blocks):
        lane = lax.broadcasted_iota(jnp.int32, (1, LANE), 1)
        blocks = list(blocks)
        dist = groups // 2
        while dist:
            width = dist * in_rows
            low = lax.rem(lane // width, 2) == 0
            for q in range(groups):
                if (q // dist) % 2 == 0:
                    x, y = blocks[q], blocks[q + dist]
                    if 2 * width == LANE:
                        turned = pltpu.roll(jnp.where(low, y, x), width, axis=1)
                        blocks[q] = jnp.where(low, x, turned)
                        blocks[q + dist] = jnp.where(low, turned, y)
                    else:
                        blocks[q] = jnp.where(low, x, pltpu.roll(y, width, axis=1))
                        blocks[q + dist] = jnp.where(low, pltpu.roll(x, LANE - width, axis=1), y)
            dist //= 2
        return blocks

    def pad_rows(x, rows):
        if x.shape[0] == rows:
            return x
        return jnp.concatenate([x, jnp.zeros((rows - x.shape[0], x.shape[1]), x.dtype)], axis=0)

    cut_in, cut_out = groups * quads_b, c_eo // groups

    def loads():
        return [
            pltpu.make_async_copy(g_si, raw_in.at[pl.ds(0, c_si)], s_load.at[1]),
            pltpu.make_async_copy(g_ei.at[pl.ds(0, cut_in)], raw_in.at[pl.ds(c_si, cut_in)], s_load.at[2]),
            pltpu.make_async_copy(g_ei.at[pl.ds(cut_in, c_ei - cut_in)], raw_in.at[pl.ds(c_si + cut_in, c_ei - cut_in)], s_load.at[3]),
            pltpu.make_async_copy(g_so, raw_out.at[pl.ds(c_eo, c_so)], s_load.at[4]),
            pltpu.make_async_copy(g_eo, raw_out.at[pl.ds(0, c_eo)], s_load.at[5]),
        ]

    def start_loads():
        for m in range(c_attn):
            for t in range(tiles):
                pltpu.make_async_copy(
                    g_attn.at[m, :, :, :, pl.ds(LANE * t, LANE)],
                    gp.at[:, :, pl.ds(m * attn_blk + t * attn_rows, attn_rows), :], s_load.at[0]).start()
        for cp in loads() + nat_copies():
            cp.start()

    def pack_in(i):
        w = waves[i]
        for j in range(w["shared"]):
            for t in range(tiles):
                cols = slice(LANE * t, LANE * (t + 1))
                got = lane_swap([pad_rows(raw_in[j, r:r + k, cols], small_blk) for r, k in cuts])
                for p in range(groups):
                    d = groups * t + p
                    gp[d // 2, d % 2, pl.ds(w["row0"] + small_blk * j, small_blk), :] = got[p]

        def body(j, carry):
            off = pl.multiple_of(w["quad0"] + quad * j, 8)
            first = c_si + groups * (w["first"] + j)
            for t in range(tiles):
                got = lane_swap([raw_in[first + p, :, LANE * t:LANE * (t + 1)] for p in range(groups)])
                for p in range(groups):
                    d = groups * t + p
                    gp[d // 2, d % 2, pl.ds(off, quad), :] = got[p]
            return carry

        lax.fori_loop(0, w["quads"], body, 0)

    def out_piece(m, d):
        return [raw_out[m, out_rows * d:out_rows * (d + 1), LANE * t:LANE * (t + 1)] for t in range(tiles)]

    def pack_out():
        def body(j, carry):
            off = pl.multiple_of(out0 + groups * out_blk * j, 8)
            for d in range(n):
                rows = sum([out_piece(groups * j + p, d) for p in range(groups)], [])
                gp[d // 2, d % 2, pl.ds(off, groups * out_blk), :] = jnp.concatenate(rows, axis=0)
            return carry

        lax.fori_loop(0, cut_out, body, 0)
        tail = rows_d - c_eo * out_blk
        for d in range(n):
            rows = sum([out_piece(m, d) for m in range(c_eo, c_out)], [])
            gp[d // 2, d % 2, pl.ds(out0 + c_eo * out_blk, tail), :] = pad_rows(jnp.concatenate(rows, axis=0), tail)

    def pack(i):
        load = loads
        if i == 0:
            view = gp.at[:, :, pl.ds(0, waves[0]["rows"]), :]
            pltpu.make_async_copy(view, view, s_load.at[0]).wait()
            pl.semaphore_wait(barrier, n - 1)
        elif i == 1:
            load()[0].wait()
            load()[1].wait()
            pack_in(1)
        elif i == 2:
            load()[2].wait()
            pack_in(2)
        else:
            load()[3].wait()
            load()[4].wait()
            pack_out()
        for k in near_last:
            d2d_copy(i, k).start()

    pending = []

    near_last = [hops_far]
    for k in range(hops_near, 0, -1):
        near_last += [k, nz - k]
    near_last.append(0)
    d2d_seen = set()

    def d2d_copy(i, k):
        sl = pl.ds(waves[i]["row0"], waves[i]["rows"])
        dest = zmod(z + k)
        return remote(gp.at[dest, 1 - c, sl, :], rx0.at[dest, sl, :], s_d2d.at[0, i, k], s_d2d.at[1, i, k], partner)

    def d2d_wait(i, k):
        if (i, k) not in d2d_seen:
            d2d_seen.add((i, k))
            d2d_copy(i, k).wait_recv()

    def mat_rows(i):
        w = waves[i]
        if w["kind"] == "attn":
            return [(m, pl.ds(attn_blk * m, attn_blk), None) for m in range(w["cnt"])]
        if w["kind"] == "out":
            return [(m, pl.ds(out0 + out_blk * m, out_blk), None) for m in range(w["cnt"])]
        got = [(m, pl.ds(w["row0"] + small_blk * m, small_blk), None) for m in range(w["shared"])]
        for j in range(w["quads"]):
            got += [(w["shared"] + groups * j + p, pl.ds(w["quad0"] + quad * j, quad), p) for p in range(groups)]
        return got

    hops = lambda h, dr: hops_far if h == dr else hops_near
    rs = {}

    def rs_send(i, h, dr, s):
        w = waves[i]
        length = hops(h, dr)
        step = length - s + 1
        dest = zmod(z + step) if dr == 0 else zmod(z - step)
        d2d_wait(i, step if dr == 0 else nz - step)
        sl = pl.ds(w["row0"] + h * w["half"], w["half"])
        osl = pl.ds(w["off"], w["half"])
        val = gp[dest, c, sl, :] + rx0[dest, sl, :]
        if s > 1:
            rs[i, h, dr, s - 1].wait_recv()
            val = val + rxr[dr, h, s - 2, osl, :]
        gp[dest, c, sl, :] = val
        where = dev(zmod(z + 1), c) if dr == 0 else dev(zmod(z - 1), c)
        cp = remote(gp.at[dest, c, sl, :], rxr.at[dr, h, s - 1, osl, :],
                    s_rs.at[i, h * 2 + dr, s - 1], r_rs.at[i, h * 2 + dr, s - 1], where)
        cp.start()
        rs[i, h, dr, s] = cp
        pending.append(cp)

    def rs_finish(i):
        w = waves[i]
        d2d_wait(i, 0)
        for h in range(2):
            sl = pl.ds(w["row0"] + h * w["half"], w["half"])
            osl = pl.ds(w["off"], w["half"])
            total = gp[z, c, sl, :] + rx0[z, sl, :]
            for dr in range(2):
                last = hops(h, dr)
                rs[i, h, dr, last].wait_recv()
                total = total + rxr[dr, h, last - 1, osl, :]
            mp[sl, :] = MOMENTUM * mp[sl, :] + total / n
        lane = lax.broadcasted_iota(jnp.int32, (1, LANE), 1)
        part = jnp.zeros((1, LANE), F32)
        for m, where, keep in mat_rows(i):
            block = mp[where, :]
            sq = jnp.sum(block * block, axis=0, keepdims=True)
            if keep is not None:
                sq = jnp.where(lane // in_rows == keep, sq, 0.0)
            part = jnp.where(lane == m, jnp.sum(sq, axis=1, keepdims=True), part)
        nrm[i, me] = part
        for d in others:
            remote(nrm.at[i, me], nrm.at[i, me], s_nrm.at[i], r_nrm.at[i], {"data": d}).start()

    def nrm_wait(i, sem):
        view = nrm.at[i, pl.ds(0, n - 1)]
        pltpu.make_async_copy(view, view, sem).wait()

    def x_copy(i, m):
        w = waves[i]
        owner = (w["base"] + m) % n
        return remote(xtx[i].at[m], rxx[i].at[me], s_x.at[i, m], r_x.at[i], {"data": owner})

    def x_send(i):
        w = waves[i]
        nrm_wait(i, r_nrm.at[i])
        tot = jnp.zeros((1, LANE), F32)
        for d in range(n):
            tot = tot + nrm[i, d]
        lane = lax.broadcasted_iota(jnp.int32, (1, LANE), 1)
        norms = [jnp.sqrt(jnp.sum(jnp.where(lane == m, tot, 0.0), axis=1, keepdims=True)) + NORM_EPS for m in range(w["cnt"])]
        blocks = []
        if w["kind"] == "in":
            for m in range(w["shared"]):
                blocks.append(mp[pl.ds(w["row0"] + small_blk * m, small_blk), :] / norms[m])
            for j in range(w["quads"]):
                m = w["shared"] + groups * j
                norm = norms[m]
                for p in range(1, groups):
                    norm = jnp.where(lane // in_rows == p, norms[m + p], norm)
                x = mp[pl.ds(w["quad0"] + quad * j, quad), :] / norm
                blocks += lane_swap([pad_rows(x[r:r + k], small_blk) for r, k in cuts])
        else:
            for m, where, _ in mat_rows(i):
                x = mp[where, :] / norms[m]
                if w["kind"] == "out":
                    zero = jnp.zeros((out_pad - out_rows, LANE), F32)
                    parts = []
                    for t in range(tiles):
                        parts += [x[t * out_rows:(t + 1) * out_rows], zero]
                    x = jnp.concatenate(parts, axis=0)
                blocks.append(x)
        for m, x in enumerate(blocks):
            x = x.astype(BF16)
            xtx[i][m] = x
            owner = (w["base"] + m) % n

            @pl.when(me != owner)
            def _():
                x_copy(i, m).start()

            @pl.when(me == owner)
            def _():
                rxx[i][me] = x

    def owned(i):
        w = waves[i]
        mine = lax.rem(me - w["base"] + n, n)
        return mine, mine < w["cnt"]

    def assemble(i):
        kind = waves[i]["kind"]
        rx = rxx[i]
        if kind == "attn":
            for t in range(tiles):
                xb[:, LANE * t:LANE * (t + 1)] = rx[:, attn_rows * t:attn_rows * (t + 1), :].reshape(n * attn_rows, LANE)
        elif kind == "out":
            for t in range(tiles):
                xb[:n * out_pad, LANE * t:LANE * (t + 1)] = rx[:, out_pad * t:out_pad * (t + 1), :].reshape(n * out_pad, LANE)
        else:
            for t in range(tiles):
                got = lane_swap([rx[groups * t + p].astype(F32) for p in range(groups)])
                for q, (r, k) in enumerate(cuts):
                    xb[r:r + k, LANE * t:LANE * (t + 1)] = got[q][:k].astype(BF16)
            xb[narrow:n * out_pad, :] = jnp.zeros((n * out_pad - narrow, wide), BF16)

    def disassemble(i):
        kind = waves[i]["kind"]
        tx = otx[i]
        if kind == "attn":
            for t in range(tiles):
                tx[:, attn_rows * t:attn_rows * (t + 1), :] = xb[:, LANE * t:LANE * (t + 1)].reshape(n, attn_rows, LANE)
        elif kind == "out":
            for t in range(tiles):
                tx[:, out_pad * t:out_pad * (t + 1), :] = xb[:n * out_pad, LANE * t:LANE * (t + 1)].reshape(n, out_pad, LANE)
        else:
            for t in range(tiles):
                cols = slice(LANE * t, LANE * (t + 1))
                got = lane_swap([pad_rows(xb[r:r + k, cols].astype(F32), small_blk) for r, k in cuts])
                for p in range(groups):
                    tx[groups * t + p] = got[p].astype(BF16)

    def iterate(size, steps):
        cut = min(size, 256)

        def one(_, carry):
            for r in range(size // cut):
                sl = slice(r * cut, (r + 1) * cut)
                gram = lax.dot_general(xb[sl, :], xb[:size, :], NT, preferred_element_type=F32)
                ab[sl, :size] = gram.astype(BF16)
            for r in range(size // cut):
                sl = slice(r * cut, (r + 1) * cut)
                square = jnp.dot(ab[sl, :size], ab[:size, :size], preferred_element_type=F32)
                bb[sl, :size] = (COEF_B * ab[sl, :size].astype(F32) + COEF_C * square).astype(BF16)
            for r in range(wide // 256):
                sl = slice(r * 256, (r + 1) * 256)
                update = jnp.dot(bb[:size, :size], xb[:size, sl], preferred_element_type=F32)
                xb[:size, sl] = (COEF_A * xb[:size, sl].astype(F32) + update).astype(BF16)
            return carry

        lax.fori_loop(0, steps, one, 0)

    def o_copy(i, mine, d):
        return remote(otx[i].at[d], rxo[i].at[mine], s_o.at[i], r_o.at[i], {"data": d})

    def owner_work(i, begin, steps, end):
        mine, yes = owned(i)

        @pl.when(yes)
        def _():
            if begin:
                view = rxx[i].at[pl.ds(0, n - 1)]
                pltpu.make_async_copy(view, view, r_x.at[i]).wait()
                assemble(i)
            iterate(n * attn_rows if waves[i]["kind"] == "attn" else n * out_pad, steps)
            if end:
                disassemble(i)
                for d in others:
                    o_copy(i, mine, d).start()
                rxo[i][mine] = otx[i][me]

    def master(i):
        w = waves[i]
        mine, yes = owned(i)
        cnt = w["cnt"]

        @pl.when(yes)
        def _():
            view = rxo[i].at[pl.ds(0, cnt - 1)]
            pltpu.make_async_copy(view, view, r_o.at[i]).wait()

        @pl.when(jnp.logical_not(yes))
        def _():
            pltpu.make_async_copy(rxo[i], rxo[i], r_o.at[i]).wait()

        step_scale = 0.2 * math.sqrt(wide)

        def update(where, o):
            old = wp[where, :]
            wp[where, :] = old - LEARN_RATE * (step_scale * o + WEIGHT_DECAY * old)

        if w["kind"] == "in":
            for m in range(w["shared"]):
                update(pl.ds(w["row0"] + small_blk * m, small_blk), rxo[i][m].astype(F32))
            for j in range(w["quads"]):
                m = w["shared"] + groups * j
                got = lane_swap([rxo[i][m + p].astype(F32) for p in range(groups)])
                o = jnp.concatenate([got[q][:k] for q, (r, k) in enumerate(cuts)], axis=0)
                update(pl.ds(w["quad0"] + quad * j, quad), o)
        else:
            for m, where, _ in mat_rows(i):
                o = rxo[i][m].astype(F32)
                if w["kind"] == "out":
                    o = jnp.concatenate([o[out_pad * t:out_pad * t + out_rows] for t in range(tiles)], axis=0)
                update(where, o)
        sl = pl.ds(w["row0"], w["rows"])
        ag[z, c, sl, :] = wp[sl, :].astype(BF16)

    agc = {}
    agd = {}

    def ag_rows(i, h):
        w = waves[i]
        if h == 0:
            return pl.ds(w["row0"], w["ag_half"])
        return pl.ds(w["row0"] + w["ag_half"], w["rows"] - w["ag_half"])

    def ag_to_partner(i, h, src, key):
        part = ag.at[src, c, ag_rows(i, h), :]
        cp = remote(part, part, s_agd.at[i, h, key], r_agd.at[i, h, key], partner)
        cp.start()
        agd[i, h, key] = cp
        pending.append(cp)

    def ag_send(i, h, dr, s):
        length = hops(h, dr)
        src = z if s == 1 else (zmod(z - (s - 1)) if dr == 0 else zmod(z + (s - 1)))
        if s > 1:
            agc[i, h, dr, s - 1].wait_recv()
        if s <= length:
            part = ag.at[src, c, ag_rows(i, h), :]
            where = dev(zmod(z + 1), c) if dr == 0 else dev(zmod(z - 1), c)
            cp = remote(part, part, s_ag.at[i, h * 2 + dr, s - 1], r_ag.at[i, h * 2 + dr, s - 1], where)
            cp.start()
            agc[i, h, dr, s] = cp
            pending.append(cp)
        if s > 1:
            ag_to_partner(i, h, src, (s - 1) if dr == 0 else nz - (s - 1))
        elif dr == 0:
            ag_to_partner(i, h, src, 0)

    out_copies = []

    def out_copy(src, dst, k):
        cp = pltpu.make_async_copy(src, dst, s_out.at[k])
        cp.start()
        out_copies.append(cp)

    def quad_row(j):
        return waves[1]["quad0"] + quad * j if j < quads_b else waves[2]["quad0"] + quad * (j - quads_b)

    def out_rows_of():
        return [(4, m, out0 + out_blk * m) for m in range(c_eo)] + [(2, m, out0 + out_blk * (c_eo + m)) for m in range(c_so)]

    def native_outputs(which):
        for src, nat, outs in (((mp, nat_m, m_out), (wp, nat_w, w_out))[which],):
            for m in range(c_attn):
                for t in range(tiles):
                    nat[0][m, :, LANE * t:LANE * (t + 1)] = src[pl.ds(m * attn_blk + t * attn_rows, attn_rows), :]
            some = c_si
            off = waves[1]["row0"]
            got = [src[off + small_blk * p:off + small_blk * (p + 1), :] for p in range(some)]
            got += [jnp.zeros((small_blk, LANE), F32)] * (groups - some)
            block = pad_rows(jnp.concatenate(lane_swap(got), axis=0), 2 * LANE).T
            for p in range(some):
                nat[1][p] = block[in_rows * p:in_rows * (p + 1), :narrow]
            for j in range(n_quads):
                block = pad_rows(src[pl.ds(quad_row(j), quad), :], 2 * LANE).T
                for p in range(groups):
                    nat[3][groups * j + p] = block[in_rows * p:in_rows * (p + 1), :narrow]
            for k, m, off in out_rows_of():
                for t in range(tiles):
                    nat[k][:, m, LANE * t:LANE * (t + 1)] = src[off + t * out_rows:off + (t + 1) * out_rows, :]
            for k in range(5):
                out_copy(nat[k], outs[k], which * 5 + k)

    def native_inputs(which):
        for cp in nat_copies()[5 * which:5 * which + 5]:
            cp.wait()
        for nat, dst in (((nat_m, mp), (nat_w, wp))[which],):
            for m in range(c_attn):
                for t in range(tiles):
                    dst[pl.ds(m * attn_blk + t * attn_rows, attn_rows), :] = nat[0][m, :, LANE * t:LANE * (t + 1)]
            wider = lambda x: jnp.concatenate([x, jnp.zeros((LANE, 2 * LANE - narrow), F32)], axis=1)
            block = pad_rows(jnp.concatenate([nat[1][p] for p in range(c_si)], axis=0), LANE)
            block = wider(block).T
            got = lane_swap([block[small_blk * q:small_blk * (q + 1)] for q in range(groups)])
            for p in range(c_si):
                dst[pl.ds(waves[1]["row0"] + small_blk * p, small_blk), :] = got[p]
            for j in range(n_quads):
                block = jnp.concatenate([nat[3][groups * j + p] for p in range(groups)], axis=0)
                dst[pl.ds(quad_row(j), quad), :] = wider(block).T[:quad]
            for k, m, off in out_rows_of():
                rows = [nat[k][:, m, LANE * t:LANE * (t + 1)] for t in range(tiles)]
                dst[pl.ds(off, out_blk), :] = jnp.concatenate(rows, axis=0)
            spare = rows_d - c_out * out_blk
            if spare:
                dst[pl.ds(out0 + c_out * out_blk, spare), :] = jnp.zeros((spare, LANE), F32)

    def unpack(i):
        w = waves[i]
        for h in range(2):
            for key in range(nz):
                agd[i, h, key].wait_recv()
        if w["kind"] == "attn":
            for m in range(c_attn):
                for t in range(tiles):
                    out_copies.append(pltpu.make_async_copy(
                        ag.at[:, :, pl.ds(m * attn_blk + t * attn_rows, attn_rows), :],
                        p_attn.at[m, :, :, :, pl.ds(LANE * t, LANE)], s_out.at[10 + m * tiles + t]))
                    out_copies[-1].start()
        elif w["kind"] == "in":
            for j in range(w["shared"]):
                sl = pl.ds(w["row0"] + small_blk * j, small_blk)
                for t in range(tiles):
                    devs = [groups * t + p for p in range(groups)]
                    got = lane_swap([ag[d // 2, d % 2, sl, :].astype(F32) for d in devs])
                    for q, (r, k) in enumerate(cuts):
                        stage_in[j, r:r + k, LANE * t:LANE * (t + 1)] = got[q][:k].astype(BF16)

            def body(j, carry):
                off = pl.multiple_of(w["quad0"] + quad * j, 16)
                first = c_si + groups * (w["first"] + j)
                for t in range(tiles):
                    devs = [groups * t + p for p in range(groups)]
                    got = lane_swap([ag[d // 2, d % 2, pl.ds(off, quad), :].astype(F32) for d in devs])
                    for p in range(groups):
                        stage_in[first + p, :, LANE * t:LANE * (t + 1)] = got[p].astype(BF16)
                return carry

            lax.fori_loop(0, w["quads"], body, 0)
            k = 10 + c_attn * tiles
            if w["shared"]:
                out_copy(stage_in.at[pl.ds(0, c_si)], p_si, k)
            first, cnt = groups * w["first"], groups * w["quads"]
            out_copy(stage_in.at[pl.ds(c_si + first, cnt)], p_ei.at[pl.ds(first, cnt)], k + 1 + (w["first"] > 0))
        else:
            def put(blk, m, first, d):
                for t in range(tiles):
                    r = out_blk * m + t * out_rows
                    raw_out[first + m, out_rows * d:out_rows * (d + 1), LANE * t:LANE * (t + 1)] = blk[r:r + out_rows]

            def body(j, carry):
                off = pl.multiple_of(out0 + groups * out_blk * j, 16)
                for d in range(n):
                    blk = ag[d // 2, d % 2, pl.ds(off, groups * out_blk), :].astype(F32)
                    for p in range(groups):
                        put(blk, p, groups * j, d)
                for p in range(groups):
                    stage_out[groups * j + p] = raw_out[groups * j + p].astype(BF16)
                return carry

            lax.fori_loop(0, cut_out, body, 0)
            for d in range(n):
                blk = ag[d // 2, d % 2, pl.ds(out0 + c_eo * out_blk, rows_d - c_eo * out_blk), :].astype(F32)
                for m in range(c_so):
                    put(blk, m, c_eo, d)
            for m in range(c_eo, c_out):
                stage_out[m] = raw_out[m].astype(BF16)
            k = 13 + c_attn * tiles
            out_copy(stage_out.at[pl.ds(c_eo, c_so)], p_so, k)
            out_copy(stage_out.at[pl.ds(0, c_eo)], p_eo, k + 1)

    def both(func, length, i, h, s):
        for dr in range(2):
            if s <= hops(h, dr) + length:
                func(i, h, dr, s)

    def own(i, part):
        begin, steps, end = ((True, NS_STEPS, True), (True, 1, False), (False, 2, False), (False, NS_STEPS - 3, True))[part]
        owner_work(i, begin, steps, end)

    acts = dict(pack=pack, nat=native_inputs, rs=functools.partial(both, rs_send, 0), fin=rs_finish, x=x_send, own=own,
                mas=master, ag=functools.partial(both, ag_send, 1), natout=native_outputs, un=unpack)
    start_loads()
    for name, *where in SCHEDULE:
        acts[name](*where)

    for cp in out_copies:
        cp.wait()
    for cp in pending:
        cp.wait_send()
    for i in range(n_waves):
        for k in range(nz):
            d2d_copy(i, k).wait_send()
        nrm_wait(i, s_nrm.at[i])
        for m in range(waves[i]["cnt"]):
            owner = (waves[i]["base"] + m) % n

            @pl.when(me != owner)
            def _():
                x_copy(i, m).wait_send()
        mine, yes = owned(i)

        @pl.when(yes)
        def _():
            view = otx[i].at[pl.ds(0, n - 1)]
            pltpu.make_async_copy(view, view, s_o.at[i]).wait()


def hand_over(shapes):
    count = len(shapes)
    pieces = []
    for k, x in enumerate(shapes):
        parts = next((p for p in (4, 2) if x.shape[0] % p == 0 and x.size > 400000), 1)
        step = x.shape[0] // parts
        pieces += [(k, p * step, step) for p in range(parts)]

    def kernel(*refs):
        src, dst, buf, sem_in, sem_out = refs[:count], refs[count:2 * count], refs[2 * count:3 * count], refs[-2], refs[-1]
        first = [pltpu.make_async_copy(src[k].at[pl.ds(r, m)], buf[k].at[pl.ds(r, m)], sem_in.at[i])
                 for i, (k, r, m) in enumerate(pieces)]
        second = [pltpu.make_async_copy(buf[k].at[pl.ds(r, m)], dst[k].at[pl.ds(r, m)], sem_out.at[i])
                  for i, (k, r, m) in enumerate(pieces)]
        for cp in first:
            cp.start()
        for one, two in zip(first, second):
            one.wait()
            two.start()
        for cp in second:
            cp.wait()

    any_spec = pl.BlockSpec(memory_space=pl.ANY)
    return pl.pallas_call(
        kernel, out_shape=shapes, in_specs=[any_spec] * count, out_specs=[any_spec] * count,
        scratch_shapes=[pltpu.VMEM(x.shape, x.dtype) for x in shapes]
        + [pltpu.SemaphoreType.DMA((len(pieces),)), pltpu.SemaphoreType.DMA((len(pieces),))],
        name="hand_over")


def solution(mesh):
    n = mesh.shape["data"]
    nz = n // 2

    def local_step(*arrays):
        grads, moms, masters = arrays[:5], arrays[5:10], arrays[10:]
        counts = tuple(m.shape[0] for m in moms)
        attn_rows, wide = moms[0].shape[1:]
        narrow = moms[1].shape[2]
        c_attn, c_si, c_so, c_ei, c_eo = counts
        c_in, c_out = c_si + c_ei, c_so + c_eo
        tiles = wide // LANE
        groups = LANE // (wide // n)
        out_blk = tiles * (narrow // n)
        small_blk = round_up(out_blk, 16)
        out_pad = round_up(narrow // n, 16)
        attn_blk = attn_rows * tiles
        rows = c_attn * attn_blk + c_si * small_blk + c_ei // groups * narrow + round_up(c_out * out_blk, 16)
        mats_b = c_si + groups * (c_ei // groups // 2)
        turn = lambda x: jnp.swapaxes(x, -1, -2)
        grads = [g[0] for g in grads]
        grads[1], grads[3] = turn(grads[1]), turn(grads[3])
        flip = lambda arrs: [jnp.swapaxes(x, 0, 1) if k in (2, 4) else x for k, x in enumerate(arrs)]
        moms, masters = flip(moms), flip(masters)
        grads[0] = grads[0].reshape(c_attn, nz, 2, attn_rows, wide)
        hops = nz // 2

        sds = jax.ShapeDtypeStruct
        out_shape = [sds(m.shape, F32) for m in moms] * 2
        out_shape += [sds((c_attn, nz, 2, attn_rows, wide), BF16)]
        out_shape += [sds((k, narrow, wide), BF16) for k in counts[1:]]
        w_cnt = (c_attn, mats_b, c_in - mats_b, c_out)
        w_blk = (attn_blk, small_blk, small_blk, out_pad * tiles)
        dma = lambda *shape: pltpu.SemaphoreType.DMA(shape)
        vm = pltpu.VMEM
        scratch = [
            vm((nz, 2, rows, LANE), F32),
            vm((nz, rows, LANE), F32),
            vm((2, 2, hops, rows // 2, LANE), F32),
            vm((nz, 2, rows, LANE), BF16),
            vm((rows, LANE), F32),
            vm((rows, LANE), F32),
            [vm(m.shape, F32) for m in moms],
            [vm(m.shape, F32) for m in moms],
            vm((4, n, 1, LANE), F32),
            [vm((k, b, LANE), BF16) for k, b in zip(w_cnt, w_blk)],
            [vm((n, b, LANE), BF16) for b in w_blk],
            [vm((n, b, LANE), BF16) for b in w_blk],
            [vm((k, b, LANE), BF16) for k, b in zip(w_cnt, w_blk)],
            vm((n * attn_rows, wide), BF16),
            vm((n * attn_rows, n * attn_rows), BF16),
            vm((n * attn_rows, n * attn_rows), BF16),
            vm((c_in, narrow, wide), F32),
            vm((c_out, narrow, wide), F32),
            vm((c_in, narrow, wide), BF16),
            vm((c_out, narrow, wide), BF16),
            dma(6), dma(2, 5), dma(2, 4, nz), dma(4, 4, hops), dma(4, 4, hops),
            dma(4), dma(4), dma(4, max(w_cnt)), dma(4), dma(4), dma(4),
            dma(4, 4, hops), dma(4, 4, hops), dma(4, 2, nz), dma(4, 2, nz),
            dma(15 + c_attn * tiles),
        ]
        any_spec = pl.BlockSpec(memory_space=pl.ANY)
        call = pl.pallas_call(
            functools.partial(fused_step, n, counts, attn_rows, wide, narrow),
            out_shape=out_shape,
            in_specs=[any_spec] * 15,
            out_specs=[any_spec] * 15,
            scratch_shapes=scratch,
            compiler_params=pltpu.CompilerParams(
                collective_id=0, has_side_effects=True, vmem_limit_bytes=67043328),
            name="muon_step",
        )
        outs = list(hand_over(out_shape)(*call(*grads, *moms, *masters)))
        outs[:5], outs[5:10] = flip(outs[:5]), flip(outs[5:10])
        outs[10] = outs[10].reshape(c_attn, n * attn_rows, wide)
        outs[11], outs[13] = turn(outs[11]), turn(outs[13])
        return tuple(outs)

    grad_spec = P(("stage", "data"), None, None, None)
    row_spec = P("stage", "data", None)
    full_spec = P("stage", None, None)
    in_specs = (grad_spec,) * 5 + (row_spec,) * 10
    out_specs = (row_spec,) * 10 + (full_spec,) * 5
    return jax.shard_map(local_step, mesh=mesh, in_specs=in_specs, out_specs=out_specs, check_vma=False)
```

```python
import functools
import math
import jax
import jax.numpy as jnp
from jax import lax
from jax.experimental import pallas as pl
from jax.experimental.pallas import tpu as pltpu
from jax.sharding import PartitionSpec as P

NS_STEPS = 5
MOMENTUM = 0.95
LEARN_RATE = 0.2
WEIGHT_DECAY = 0.25
NORM_EPS = 1e-7
COEF_A = 3.4445
COEF_B = -4.7750
COEF_C = 2.0315

SCHEDULE = (
    ("pack", 0), ("rs", 0, 0, 1), ("rs", 0, 1, 1), ("pack", 1), ("rs", 0, 0, 2), ("pack", 2), ("rs", 0, 1, 2),
    ("rs", 1, 1, 1), ("nat", 1), ("rs", 1, 0, 1), ("rs", 1, 1, 2), ("rs", 0, 1, 3), ("rs", 1, 0, 2),
    ("rs", 0, 0, 3), ("pack", 3), ("nat", 0), ("rs", 1, 1, 3), ("rs", 0, 0, 4), ("rs", 0, 1, 4), ("rs", 3, 0, 1),
    ("rs", 3, 1, 1), ("fin", 0), ("rs", 1, 0, 3), ("rs", 2, 1, 1), ("rs", 3, 1, 2), ("rs", 1, 1, 4),
    ("rs", 1, 0, 4), ("rs", 3, 0, 2), ("rs", 2, 0, 1), ("rs", 3, 1, 3), ("fin", 1), ("x", 0), ("rs", 2, 1, 2),
    ("rs", 3, 0, 3), ("rs", 2, 0, 2), ("x", 1), ("rs", 3, 1, 4), ("own", 0, 1), ("rs", 2, 1, 3), ("own", 0, 2),
    ("rs", 3, 0, 4), ("own", 0, 3), ("own", 1, 0), ("fin", 3), ("rs", 2, 0, 3), ("rs", 2, 0, 4), ("mas", 0),
    ("ag", 0, 1, 1), ("rs", 2, 1, 4), ("ag", 0, 0, 1), ("mas", 1), ("fin", 2), ("ag", 1, 1, 1), ("ag", 1, 0, 1),
    ("ag", 1, 1, 2), ("x", 3), ("x", 2), ("ag", 1, 1, 3), ("ag", 0, 1, 2), ("natout", 0), ("ag", 1, 0, 2),
    ("ag", 1, 1, 4), ("own", 2, 0), ("own", 3, 0), ("ag", 0, 0, 2), ("ag", 1, 1, 5), ("ag", 1, 0, 3), ("mas", 2),
    ("ag", 0, 1, 3), ("ag", 2, 1, 1), ("ag", 2, 0, 1), ("mas", 3), ("ag", 1, 0, 4), ("ag", 2, 1, 2),
    ("ag", 3, 1, 1), ("ag", 3, 0, 1), ("ag", 2, 0, 2), ("ag", 3, 1, 2), ("ag", 3, 0, 2), ("ag", 1, 0, 5),
    ("ag", 2, 0, 3), ("ag", 2, 1, 3), ("ag", 3, 0, 3), ("ag", 3, 1, 3), ("ag", 2, 0, 4), ("ag", 2, 1, 4),
    ("ag", 0, 0, 3), ("un", 1), ("ag", 2, 0, 5), ("ag", 0, 1, 4), ("ag", 2, 1, 5), ("ag", 3, 1, 4),
    ("ag", 3, 0, 4), ("natout", 1), ("ag", 0, 0, 4), ("un", 2), ("ag", 3, 0, 5), ("ag", 3, 1, 5), ("ag", 0, 1, 5),
    ("ag", 0, 0, 5), ("un", 3), ("un", 0),
)

FIRST_PART = 0.68

F32 = jnp.float32
BF16 = jnp.bfloat16
MESH = pl.DeviceIdType.MESH
LANE = 128
NT = (((1,), (1,)), ((), ()))


def round_up(value, step):
    return (value + step - 1) // step * step


def fused_step(n, counts, attn_rows, wide, narrow, *refs):
    c_attn, c_si, c_so, c_ei, c_eo = counts
    c_in, c_out = c_si + c_ei, c_so + c_eo
    nz = n // 2
    hops_far, hops_near = nz // 2, nz - 1 - nz // 2
    tiles = wide // LANE
    in_rows = wide // n
    groups = LANE // in_rows
    out_rows = narrow // n
    out_pad = round_up(out_rows, 16)
    attn_blk = attn_rows * tiles
    out_blk = tiles * out_rows
    small_blk = round_up(out_blk, 16)
    cuts = [(q * small_blk, min(small_blk, narrow - q * small_blk)) for q in range(groups)]

    it = iter(refs)
    take = lambda k: [next(it) for _ in range(k)]
    g_attn, g_si, g_so, g_ei, g_eo = take(5)
    m_in = take(5)
    w_in = take(5)
    m_out = take(5)
    w_out = take(5)
    p_attn, p_si, p_so, p_ei, p_eo = take(5)
    (gp, rx0, rxr, ag, mp, wp, nat_m, nat_w, nrm, xtx, rxx, otx, rxo, xb, ab, bb,
     raw_in, raw_out, stage_in, stage_out) = take(20)
    (s_load, s_nat, s_d2d, s_rs, r_rs, s_nrm, r_nrm, s_x, r_x, s_o, r_o, s_ag, r_ag, s_agd, r_agd, s_out) = take(16)

    quad = narrow
    n_quads = c_ei // groups
    quads_b = n_quads // 2
    mats_b, mats_c = c_si + groups * quads_b, groups * (n_quads - quads_b)
    rows_b, rows_c = c_si * small_blk + quads_b * quad, (n_quads - quads_b) * quad
    rows_d = round_up(c_out * out_blk, 16)
    waves = [dict(kind="attn", cnt=c_attn, rows=c_attn * attn_blk, base=(c_in + c_out) % n),
             dict(kind="in", cnt=mats_b, rows=rows_b, base=0, shared=c_si, quads=quads_b, first=0),
             dict(kind="in", cnt=mats_c, rows=rows_c, base=mats_b % n, shared=0, quads=n_quads - quads_b, first=quads_b),
             dict(kind="out", cnt=c_out, rows=rows_d, base=c_in % n)]
    n_waves = len(waves)
    start = 0
    for w in waves:
        w["row0"] = start
        start += w["rows"]
        split = int(w["rows"] * FIRST_PART / 16 + 0.5) * 16
        w["halves"] = (pl.ds(w["row0"], split), pl.ds(w["row0"] + split, w["rows"] - split))
        w["quad0"] = w["row0"] + w.get("shared", 0) * small_blk
    out0 = waves[3]["row0"]

    me = lax.axis_index("data")
    z = me // 2
    c = lax.rem(me, 2)
    zmod = lambda v: lax.rem(v + 2 * nz, nz)
    dev = lambda zz, cc: {"data": zz * 2 + cc}
    partner = {"data": z * 2 + (1 - c)}
    others = [lax.rem(me + k, n) for k in range(1, n)]

    def remote(src, dst, ss, rs, where):
        return pltpu.make_async_remote_copy(src_ref=src, dst_ref=dst, send_sem=ss, recv_sem=rs,
                                            device_id=where, device_id_type=MESH)

    barrier = pltpu.get_barrier_semaphore()
    for d in others:
        pl.semaphore_signal(barrier, inc=1, device_id={"data": d}, device_id_type=MESH)

    def nat_copies():
        return [pltpu.make_async_copy(srcs[k], dsts[k], s_nat.at[which, k])
                for which, (srcs, dsts) in enumerate(((m_in, nat_m), (w_in, nat_w))) for k in range(5)]

    def lane_swap(blocks):
        lane = lax.broadcasted_iota(jnp.int32, (1, LANE), 1)
        blocks = list(blocks)
        dist = groups // 2
        while dist:
            width = dist * in_rows
            low = lax.rem(lane // width, 2) == 0
            for q in range(groups):
                if (q // dist) % 2 == 0:
                    x, y = blocks[q], blocks[q + dist]
                    if 2 * width == LANE:
                        turned = pltpu.roll(jnp.where(low, y, x), width, axis=1)
                        blocks[q] = jnp.where(low, x, turned)
                        blocks[q + dist] = jnp.where(low, turned, y)
                    else:
                        blocks[q] = jnp.where(low, x, pltpu.roll(y, width, axis=1))
                        blocks[q + dist] = jnp.where(low, pltpu.roll(x, LANE - width, axis=1), y)
            dist //= 2
        return blocks

    def pad_rows(x, rows):
        if x.shape[0] == rows:
            return x
        return jnp.concatenate([x, jnp.zeros((rows - x.shape[0], x.shape[1]), x.dtype)], axis=0)

    cut_in, cut_out = groups * quads_b, c_eo // groups

    def loads():
        return [
            pltpu.make_async_copy(g_si, raw_in.at[pl.ds(0, c_si)], s_load.at[1]),
            pltpu.make_async_copy(g_ei.at[pl.ds(0, cut_in)], raw_in.at[pl.ds(c_si, cut_in)], s_load.at[2]),
            pltpu.make_async_copy(g_ei.at[pl.ds(cut_in, c_ei - cut_in)], raw_in.at[pl.ds(c_si + cut_in, c_ei - cut_in)], s_load.at[3]),
            pltpu.make_async_copy(g_so, raw_out.at[pl.ds(c_eo, c_so)], s_load.at[4]),
            pltpu.make_async_copy(g_eo, raw_out.at[pl.ds(0, c_eo)], s_load.at[5]),
        ]

    def start_loads():
        for m in range(c_attn):
            for t in range(tiles):
                pltpu.make_async_copy(
                    g_attn.at[m, :, :, :, pl.ds(LANE * t, LANE)],
                    gp.at[:, :, pl.ds(m * attn_blk + t * attn_rows, attn_rows), :], s_load.at[0]).start()
        for cp in loads() + nat_copies():
            cp.start()

    def pack_in(i):
        w = waves[i]
        for j in range(w["shared"]):
            for t in range(tiles):
                cols = slice(LANE * t, LANE * (t + 1))
                got = lane_swap([pad_rows(raw_in[j, r:r + k, cols], small_blk) for r, k in cuts])
                for p in range(groups):
                    d = groups * t + p
                    gp[d // 2, d % 2, pl.ds(w["row0"] + small_blk * j, small_blk), :] = got[p]

        def body(j, carry):
            off = pl.multiple_of(w["quad0"] + quad * j, 8)
            first = c_si + groups * (w["first"] + j)
            for t in range(tiles):
                got = lane_swap([raw_in[first + p, :, LANE * t:LANE * (t + 1)] for p in range(groups)])
                for p in range(groups):
                    d = groups * t + p
                    gp[d // 2, d % 2, pl.ds(off, quad), :] = got[p]
            return carry

        lax.fori_loop(0, w["quads"], body, 0)

    def out_piece(m, d):
        return [raw_out[m, out_rows * d:out_rows * (d + 1), LANE * t:LANE * (t + 1)] for t in range(tiles)]

    def pack_out():
        def body(j, carry):
            off = pl.multiple_of(out0 + groups * out_blk * j, 8)
            for d in range(n):
                rows = sum([out_piece(groups * j + p, d) for p in range(groups)], [])
                gp[d // 2, d % 2, pl.ds(off, groups * out_blk), :] = jnp.concatenate(rows, axis=0)
            return carry

        lax.fori_loop(0, cut_out, body, 0)
        tail = rows_d - c_eo * out_blk
        for d in range(n):
            rows = sum([out_piece(m, d) for m in range(c_eo, c_out)], [])
            gp[d // 2, d % 2, pl.ds(out0 + c_eo * out_blk, tail), :] = pad_rows(jnp.concatenate(rows, axis=0), tail)

    def pack(i):
        load = loads
        if i == 0:
            view = gp.at[:, :, pl.ds(0, waves[0]["rows"]), :]
            pltpu.make_async_copy(view, view, s_load.at[0]).wait()
            pl.semaphore_wait(barrier, n - 1)
        elif i == 1:
            load()[0].wait()
            load()[1].wait()
            pack_in(1)
        elif i == 2:
            load()[2].wait()
            pack_in(2)
        else:
            load()[3].wait()
            load()[4].wait()
            pack_out()
        for k in near_last:
            d2d_copy(i, k).start()

    pending = []

    near_last = [hops_far]
    for k in range(hops_near, 0, -1):
        near_last += [k, nz - k]
    near_last.append(0)
    d2d_seen = set()

    def d2d_copy(i, k):
        sl = pl.ds(waves[i]["row0"], waves[i]["rows"])
        dest = zmod(z + k)
        return remote(gp.at[dest, 1 - c, sl, :], rx0.at[dest, sl, :], s_d2d.at[0, i, k], s_d2d.at[1, i, k], partner)

    def d2d_wait(i, k):
        if (i, k) not in d2d_seen:
            d2d_seen.add((i, k))
            d2d_copy(i, k).wait_recv()

    def mat_rows(i):
        w = waves[i]
        if w["kind"] == "attn":
            return [(m, pl.ds(attn_blk * m, attn_blk), None) for m in range(w["cnt"])]
        if w["kind"] == "out":
            return [(m, pl.ds(out0 + out_blk * m, out_blk), None) for m in range(w["cnt"])]
        got = [(m, pl.ds(w["row0"] + small_blk * m, small_blk), None) for m in range(w["shared"])]
        for j in range(w["quads"]):
            got += [(w["shared"] + groups * j + p, pl.ds(w["quad0"] + quad * j, quad), p) for p in range(groups)]
        return got

    hops = lambda h, dr: hops_far if h == dr else hops_near
    rs = {}

    def rs_send(i, h, dr, s):
        w = waves[i]
        length = hops(h, dr)
        step = length - s + 1
        dest = zmod(z + step) if dr == 0 else zmod(z - step)
        d2d_wait(i, step if dr == 0 else nz - step)
        sl = w["halves"][h]
        val = gp[dest, c, sl, :] + rx0[dest, sl, :]
        if s > 1:
            rs[i, h, dr, s - 1].wait_recv()
            val = val + rxr[dr, s - 2, sl, :]
        gp[dest, c, sl, :] = val
        where = dev(zmod(z + 1), c) if dr == 0 else dev(zmod(z - 1), c)
        cp = remote(gp.at[dest, c, sl, :], rxr.at[dr, s - 1, sl, :],
                    s_rs.at[i, h * 2 + dr, s - 1], r_rs.at[i, h * 2 + dr, s - 1], where)
        cp.start()
        rs[i, h, dr, s] = cp
        pending.append(cp)

    def rs_finish(i):
        w = waves[i]
        d2d_wait(i, 0)
        for h in range(2):
            sl = w["halves"][h]
            total = gp[z, c, sl, :] + rx0[z, sl, :]
            for dr in range(2):
                last = hops(h, dr)
                rs[i, h, dr, last].wait_recv()
                total = total + rxr[dr, last - 1, sl, :]
            mp[sl, :] = MOMENTUM * mp[sl, :] + total / n
        lane = lax.broadcasted_iota(jnp.int32, (1, LANE), 1)
        part = jnp.zeros((1, LANE), F32)
        for m, where, keep in mat_rows(i):
            block = mp[where, :]
            sq = jnp.sum(block * block, axis=0, keepdims=True)
            if keep is not None:
                sq = jnp.where(lane // in_rows == keep, sq, 0.0)
            part = jnp.where(lane == m, jnp.sum(sq, axis=1, keepdims=True), part)
        nrm[i, me] = part
        for d in others:
            remote(nrm.at[i, me], nrm.at[i, me], s_nrm.at[i], r_nrm.at[i], {"data": d}).start()

    def nrm_wait(i, sem):
        view = nrm.at[i, pl.ds(0, n - 1)]
        pltpu.make_async_copy(view, view, sem).wait()

    def x_copy(i, m):
        w = waves[i]
        owner = (w["base"] + m) % n
        return remote(xtx[i].at[m], rxx[i].at[me], s_x.at[i, m], r_x.at[i], {"data": owner})

    def x_send(i):
        w = waves[i]
        nrm_wait(i, r_nrm.at[i])
        tot = jnp.zeros((1, LANE), F32)
        for d in range(n):
            tot = tot + nrm[i, d]
        lane = lax.broadcasted_iota(jnp.int32, (1, LANE), 1)
        norms = [jnp.sqrt(jnp.sum(jnp.where(lane == m, tot, 0.0), axis=1, keepdims=True)) + NORM_EPS for m in range(w["cnt"])]
        blocks = []
        if w["kind"] == "in":
            for m in range(w["shared"]):
                blocks.append(mp[pl.ds(w["row0"] + small_blk * m, small_blk), :] / norms[m])
            for j in range(w["quads"]):
                m = w["shared"] + groups * j
                norm = norms[m]
                for p in range(1, groups):
                    norm = jnp.where(lane // in_rows == p, norms[m + p], norm)
                x = mp[pl.ds(w["quad0"] + quad * j, quad), :] / norm
                blocks += lane_swap([pad_rows(x[r:r + k], small_blk) for r, k in cuts])
        else:
            for m, where, _ in mat_rows(i):
                x = mp[where, :] / norms[m]
                if w["kind"] == "out":
                    zero = jnp.zeros((out_pad - out_rows, LANE), F32)
                    parts = []
                    for t in range(tiles):
                        parts += [x[t * out_rows:(t + 1) * out_rows], zero]
                    x = jnp.concatenate(parts, axis=0)
                blocks.append(x)
        for m, x in enumerate(blocks):
            x = x.astype(BF16)
            xtx[i][m] = x
            owner = (w["base"] + m) % n

            @pl.when(me != owner)
            def _():
                x_copy(i, m).start()

            @pl.when(me == owner)
            def _():
                rxx[i][me] = x

    def owned(i):
        w = waves[i]
        mine = lax.rem(me - w["base"] + n, n)
        return mine, mine < w["cnt"]

    def assemble(i):
        kind = waves[i]["kind"]
        rx = rxx[i]
        if kind == "attn":
            for t in range(tiles):
                xb[:, LANE * t:LANE * (t + 1)] = rx[:, attn_rows * t:attn_rows * (t + 1), :].reshape(n * attn_rows, LANE)
        elif kind == "out":
            for t in range(tiles):
                xb[:n * out_pad, LANE * t:LANE * (t + 1)] = rx[:, out_pad * t:out_pad * (t + 1), :].reshape(n * out_pad, LANE)
        else:
            for t in range(tiles):
                got = lane_swap([rx[groups * t + p].astype(F32) for p in range(groups)])
                for q, (r, k) in enumerate(cuts):
                    xb[r:r + k, LANE * t:LANE * (t + 1)] = got[q][:k].astype(BF16)
            xb[narrow:n * out_pad, :] = jnp.zeros((n * out_pad - narrow, wide), BF16)

    def disassemble(i):
        kind = waves[i]["kind"]
        tx = otx[i]
        if kind == "attn":
            for t in range(tiles):
                tx[:, attn_rows * t:attn_rows * (t + 1), :] = xb[:, LANE * t:LANE * (t + 1)].reshape(n, attn_rows, LANE)
        elif kind == "out":
            for t in range(tiles):
                tx[:, out_pad * t:out_pad * (t + 1), :] = xb[:n * out_pad, LANE * t:LANE * (t + 1)].reshape(n, out_pad, LANE)
        else:
            for t in range(tiles):
                cols = slice(LANE * t, LANE * (t + 1))
                got = lane_swap([pad_rows(xb[r:r + k, cols].astype(F32), small_blk) for r, k in cuts])
                for p in range(groups):
                    tx[groups * t + p] = got[p].astype(BF16)

    def iterate(size, steps):
        cut = min(size, 256)

        def one(_, carry):
            for r in range(size // cut):
                sl = slice(r * cut, (r + 1) * cut)
                gram = lax.dot_general(xb[sl, :], xb[:size, :], NT, preferred_element_type=F32)
                ab[sl, :size] = gram.astype(BF16)
            for r in range(size // cut):
                sl = slice(r * cut, (r + 1) * cut)
                square = jnp.dot(ab[sl, :size], ab[:size, :size], preferred_element_type=F32)
                bb[sl, :size] = (COEF_B * ab[sl, :size].astype(F32) + COEF_C * square).astype(BF16)
            for r in range(wide // 256):
                sl = slice(r * 256, (r + 1) * 256)
                update = jnp.dot(bb[:size, :size], xb[:size, sl], preferred_element_type=F32)
                xb[:size, sl] = (COEF_A * xb[:size, sl].astype(F32) + update).astype(BF16)
            return carry

        lax.fori_loop(0, steps, one, 0)

    def o_copy(i, mine, d):
        return remote(otx[i].at[d], rxo[i].at[mine], s_o.at[i], r_o.at[i], {"data": d})

    def owner_work(i, begin, steps, end):
        mine, yes = owned(i)

        @pl.when(yes)
        def _():
            if begin:
                view = rxx[i].at[pl.ds(0, n - 1)]
                pltpu.make_async_copy(view, view, r_x.at[i]).wait()
                assemble(i)
            iterate(n * attn_rows if waves[i]["kind"] == "attn" else n * out_pad, steps)
            if end:
                disassemble(i)
                for d in others:
                    o_copy(i, mine, d).start()
                rxo[i][mine] = otx[i][me]

    def master(i):
        w = waves[i]
        mine, yes = owned(i)
        cnt = w["cnt"]

        @pl.when(yes)
        def _():
            view = rxo[i].at[pl.ds(0, cnt - 1)]
            pltpu.make_async_copy(view, view, r_o.at[i]).wait()

        @pl.when(jnp.logical_not(yes))
        def _():
            pltpu.make_async_copy(rxo[i], rxo[i], r_o.at[i]).wait()

        step_scale = 0.2 * math.sqrt(wide)

        def update(where, o):
            old = wp[where, :]
            wp[where, :] = old - LEARN_RATE * (step_scale * o + WEIGHT_DECAY * old)

        if w["kind"] == "in":
            for m in range(w["shared"]):
                update(pl.ds(w["row0"] + small_blk * m, small_blk), rxo[i][m].astype(F32))
            for j in range(w["quads"]):
                m = w["shared"] + groups * j
                got = lane_swap([rxo[i][m + p].astype(F32) for p in range(groups)])
                o = jnp.concatenate([got[q][:k] for q, (r, k) in enumerate(cuts)], axis=0)
                update(pl.ds(w["quad0"] + quad * j, quad), o)
        else:
            for m, where, _ in mat_rows(i):
                o = rxo[i][m].astype(F32)
                if w["kind"] == "out":
                    o = jnp.concatenate([o[out_pad * t:out_pad * t + out_rows] for t in range(tiles)], axis=0)
                update(where, o)
        sl = pl.ds(w["row0"], w["rows"])
        ag[z, c, sl, :] = wp[sl, :].astype(BF16)

    agc = {}
    agd = {}

    def ag_rows(i, h):
        return waves[i]["halves"][h]

    def ag_to_partner(i, h, src, key):
        part = ag.at[src, c, ag_rows(i, h), :]
        cp = remote(part, part, s_agd.at[i, h, key], r_agd.at[i, h, key], partner)
        cp.start()
        agd[i, h, key] = cp
        pending.append(cp)

    def ag_send(i, h, dr, s):
        length = hops(h, dr)
        src = z if s == 1 else (zmod(z - (s - 1)) if dr == 0 else zmod(z + (s - 1)))
        if s > 1:
            agc[i, h, dr, s - 1].wait_recv()
        if s <= length:
            part = ag.at[src, c, ag_rows(i, h), :]
            where = dev(zmod(z + 1), c) if dr == 0 else dev(zmod(z - 1), c)
            cp = remote(part, part, s_ag.at[i, h * 2 + dr, s - 1], r_ag.at[i, h * 2 + dr, s - 1], where)
            cp.start()
            agc[i, h, dr, s] = cp
            pending.append(cp)
        if s > 1:
            ag_to_partner(i, h, src, (s - 1) if dr == 0 else nz - (s - 1))
        elif dr == 0:
            ag_to_partner(i, h, src, 0)

    out_copies = []

    def out_copy(src, dst, k):
        cp = pltpu.make_async_copy(src, dst, s_out.at[k])
        cp.start()
        out_copies.append(cp)

    def quad_row(j):
        return waves[1]["quad0"] + quad * j if j < quads_b else waves[2]["quad0"] + quad * (j - quads_b)

    def out_rows_of():
        return [(4, m, out0 + out_blk * m) for m in range(c_eo)] + [(2, m, out0 + out_blk * (c_eo + m)) for m in range(c_so)]

    def native_outputs(which):
        for src, nat, outs in (((mp, nat_m, m_out), (wp, nat_w, w_out))[which],):
            for m in range(c_attn):
                for t in range(tiles):
                    nat[0][m, :, LANE * t:LANE * (t + 1)] = src[pl.ds(m * attn_blk + t * attn_rows, attn_rows), :]
            some = c_si
            off = waves[1]["row0"]
            got = [src[off + small_blk * p:off + small_blk * (p + 1), :] for p in range(some)]
            got += [jnp.zeros((small_blk, LANE), F32)] * (groups - some)
            block = pad_rows(jnp.concatenate(lane_swap(got), axis=0), 2 * LANE).T
            for p in range(some):
                nat[1][p] = block[in_rows * p:in_rows * (p + 1), :narrow]
            for j in range(n_quads):
                block = pad_rows(src[pl.ds(quad_row(j), quad), :], 2 * LANE).T
                for p in range(groups):
                    nat[3][groups * j + p] = block[in_rows * p:in_rows * (p + 1), :narrow]
            for k, m, off in out_rows_of():
                for t in range(tiles):
                    nat[k][:, m, LANE * t:LANE * (t + 1)] = src[off + t * out_rows:off + (t + 1) * out_rows, :]
            for k in range(5):
                out_copy(nat[k], outs[k], which * 5 + k)

    def native_inputs(which):
        for cp in nat_copies()[5 * which:5 * which + 5]:
            cp.wait()
        for nat, dst in (((nat_m, mp), (nat_w, wp))[which],):
            for m in range(c_attn):
                for t in range(tiles):
                    dst[pl.ds(m * attn_blk + t * attn_rows, attn_rows), :] = nat[0][m, :, LANE * t:LANE * (t + 1)]
            wider = lambda x: jnp.concatenate([x, jnp.zeros((LANE, 2 * LANE - narrow), F32)], axis=1)
            block = pad_rows(jnp.concatenate([nat[1][p] for p in range(c_si)], axis=0), LANE)
            block = wider(block).T
            got = lane_swap([block[small_blk * q:small_blk * (q + 1)] for q in range(groups)])
            for p in range(c_si):
                dst[pl.ds(waves[1]["row0"] + small_blk * p, small_blk), :] = got[p]
            for j in range(n_quads):
                block = jnp.concatenate([nat[3][groups * j + p] for p in range(groups)], axis=0)
                dst[pl.ds(quad_row(j), quad), :] = wider(block).T[:quad]
            for k, m, off in out_rows_of():
                rows = [nat[k][:, m, LANE * t:LANE * (t + 1)] for t in range(tiles)]
                dst[pl.ds(off, out_blk), :] = jnp.concatenate(rows, axis=0)
            spare = rows_d - c_out * out_blk
            if spare:
                dst[pl.ds(out0 + c_out * out_blk, spare), :] = jnp.zeros((spare, LANE), F32)

    def unpack(i):
        w = waves[i]
        for h in range(2):
            for key in range(nz):
                agd[i, h, key].wait_recv()
        if w["kind"] == "attn":
            for m in range(c_attn):
                for t in range(tiles):
                    out_copies.append(pltpu.make_async_copy(
                        ag.at[:, :, pl.ds(m * attn_blk + t * attn_rows, attn_rows), :],
                        p_attn.at[m, :, :, :, pl.ds(LANE * t, LANE)], s_out.at[10 + m * tiles + t]))
                    out_copies[-1].start()
        elif w["kind"] == "in":
            for j in range(w["shared"]):
                sl = pl.ds(w["row0"] + small_blk * j, small_blk)
                for t in range(tiles):
                    devs = [groups * t + p for p in range(groups)]
                    got = lane_swap([ag[d // 2, d % 2, sl, :].astype(F32) for d in devs])
                    for q, (r, k) in enumerate(cuts):
                        stage_in[j, r:r + k, LANE * t:LANE * (t + 1)] = got[q][:k].astype(BF16)

            def body(j, carry):
                off = pl.multiple_of(w["quad0"] + quad * j, 16)
                first = c_si + groups * (w["first"] + j)
                for t in range(tiles):
                    devs = [groups * t + p for p in range(groups)]
                    got = lane_swap([ag[d // 2, d % 2, pl.ds(off, quad), :].astype(F32) for d in devs])
                    for p in range(groups):
                        stage_in[first + p, :, LANE * t:LANE * (t + 1)] = got[p].astype(BF16)
                return carry

            lax.fori_loop(0, w["quads"], body, 0)
            k = 10 + c_attn * tiles
            if w["shared"]:
                out_copy(stage_in.at[pl.ds(0, c_si)], p_si, k)
            first, cnt = groups * w["first"], groups * w["quads"]
            out_copy(stage_in.at[pl.ds(c_si + first, cnt)], p_ei.at[pl.ds(first, cnt)], k + 1 + (w["first"] > 0))
        else:
            def put(blk, m, first, d):
                for t in range(tiles):
                    r = out_blk * m + t * out_rows
                    raw_out[first + m, out_rows * d:out_rows * (d + 1), LANE * t:LANE * (t + 1)] = blk[r:r + out_rows]

            def body(j, carry):
                off = pl.multiple_of(out0 + groups * out_blk * j, 16)
                for d in range(n):
                    blk = ag[d // 2, d % 2, pl.ds(off, groups * out_blk), :].astype(F32)
                    for p in range(groups):
                        put(blk, p, groups * j, d)
                for p in range(groups):
                    stage_out[groups * j + p] = raw_out[groups * j + p].astype(BF16)
                return carry

            lax.fori_loop(0, cut_out, body, 0)
            for d in range(n):
                blk = ag[d // 2, d % 2, pl.ds(out0 + c_eo * out_blk, rows_d - c_eo * out_blk), :].astype(F32)
                for m in range(c_so):
                    put(blk, m, c_eo, d)
            for m in range(c_eo, c_out):
                stage_out[m] = raw_out[m].astype(BF16)
            k = 13 + c_attn * tiles
            out_copy(stage_out.at[pl.ds(c_eo, c_so)], p_so, k)
            out_copy(stage_out.at[pl.ds(0, c_eo)], p_eo, k + 1)

    def both(func, length, i, h, s):
        for dr in range(2):
            if s <= hops(h, dr) + length:
                func(i, h, dr, s)

    def own(i, part):
        begin, steps, end = ((True, NS_STEPS, True), (True, 1, False), (False, 2, False), (False, NS_STEPS - 3, True))[part]
        owner_work(i, begin, steps, end)

    acts = dict(pack=pack, nat=native_inputs, rs=functools.partial(both, rs_send, 0), fin=rs_finish, x=x_send, own=own,
                mas=master, ag=functools.partial(both, ag_send, 1), natout=native_outputs, un=unpack)
    start_loads()
    for name, *where in SCHEDULE:
        acts[name](*where)

    for cp in out_copies:
        cp.wait()
    for cp in pending:
        cp.wait_send()
    for i in range(n_waves):
        for k in range(nz):
            d2d_copy(i, k).wait_send()
        nrm_wait(i, s_nrm.at[i])
        for m in range(waves[i]["cnt"]):
            owner = (waves[i]["base"] + m) % n

            @pl.when(me != owner)
            def _():
                x_copy(i, m).wait_send()
        mine, yes = owned(i)

        @pl.when(yes)
        def _():
            view = otx[i].at[pl.ds(0, n - 1)]
            pltpu.make_async_copy(view, view, s_o.at[i]).wait()


def hand_over(shapes):
    count = len(shapes)
    pieces = []
    for k, x in enumerate(shapes):
        parts = next((p for p in (4, 2) if x.shape[0] % p == 0 and x.size > 400000), 1)
        step = x.shape[0] // parts
        pieces += [(k, p * step, step) for p in range(parts)]

    def kernel(*refs):
        src, dst, buf, sem_in, sem_out = refs[:count], refs[count:2 * count], refs[2 * count:3 * count], refs[-2], refs[-1]
        first = [pltpu.make_async_copy(src[k].at[pl.ds(r, m)], buf[k].at[pl.ds(r, m)], sem_in.at[i])
                 for i, (k, r, m) in enumerate(pieces)]
        second = [pltpu.make_async_copy(buf[k].at[pl.ds(r, m)], dst[k].at[pl.ds(r, m)], sem_out.at[i])
                  for i, (k, r, m) in enumerate(pieces)]
        for cp in first:
            cp.start()
        for one, two in zip(first, second):
            one.wait()
            two.start()
        for cp in second:
            cp.wait()

    any_spec = pl.BlockSpec(memory_space=pl.ANY)
    return pl.pallas_call(
        kernel, out_shape=shapes, in_specs=[any_spec] * count, out_specs=[any_spec] * count,
        scratch_shapes=[pltpu.VMEM(x.shape, x.dtype) for x in shapes]
        + [pltpu.SemaphoreType.DMA((len(pieces),)), pltpu.SemaphoreType.DMA((len(pieces),))],
        name="hand_over")


def solution(mesh):
    n = mesh.shape["data"]
    nz = n // 2

    def local_step(*arrays):
        grads, moms, masters = arrays[:5], arrays[5:10], arrays[10:]
        counts = tuple(m.shape[0] for m in moms)
        attn_rows, wide = moms[0].shape[1:]
        narrow = moms[1].shape[2]
        c_attn, c_si, c_so, c_ei, c_eo = counts
        c_in, c_out = c_si + c_ei, c_so + c_eo
        tiles = wide // LANE
        groups = LANE // (wide // n)
        out_blk = tiles * (narrow // n)
        small_blk = round_up(out_blk, 16)
        out_pad = round_up(narrow // n, 16)
        attn_blk = attn_rows * tiles
        rows = c_attn * attn_blk + c_si * small_blk + c_ei // groups * narrow + round_up(c_out * out_blk, 16)
        mats_b = c_si + groups * (c_ei // groups // 2)
        turn = lambda x: jnp.swapaxes(x, -1, -2)
        grads = [g[0] for g in grads]
        grads[1], grads[3] = turn(grads[1]), turn(grads[3])
        flip = lambda arrs: [jnp.swapaxes(x, 0, 1) if k in (2, 4) else x for k, x in enumerate(arrs)]
        moms, masters = flip(moms), flip(masters)
        grads[0] = grads[0].reshape(c_attn, nz, 2, attn_rows, wide)
        hops = nz // 2

        sds = jax.ShapeDtypeStruct
        out_shape = [sds(m.shape, F32) for m in moms] * 2
        out_shape += [sds((c_attn, nz, 2, attn_rows, wide), BF16)]
        out_shape += [sds((k, narrow, wide), BF16) for k in counts[1:]]
        w_cnt = (c_attn, mats_b, c_in - mats_b, c_out)
        w_blk = (attn_blk, small_blk, small_blk, out_pad * tiles)
        dma = lambda *shape: pltpu.SemaphoreType.DMA(shape)
        vm = pltpu.VMEM
        scratch = [
            vm((nz, 2, rows, LANE), F32),
            vm((nz, rows, LANE), F32),
            vm((2, hops, rows, LANE), F32),
            vm((nz, 2, rows, LANE), BF16),
            vm((rows, LANE), F32),
            vm((rows, LANE), F32),
            [vm(m.shape, F32) for m in moms],
            [vm(m.shape, F32) for m in moms],
            vm((4, n, 1, LANE), F32),
            [vm((k, b, LANE), BF16) for k, b in zip(w_cnt, w_blk)],
            [vm((n, b, LANE), BF16) for b in w_blk],
            [vm((n, b, LANE), BF16) for b in w_blk],
            [vm((k, b, LANE), BF16) for k, b in zip(w_cnt, w_blk)],
            vm((n * attn_rows, wide), BF16),
            vm((n * attn_rows, n * attn_rows), BF16),
            vm((n * attn_rows, n * attn_rows), BF16),
            vm((c_in, narrow, wide), F32),
            vm((c_out, narrow, wide), F32),
            vm((c_in, narrow, wide), BF16),
            vm((c_out, narrow, wide), BF16),
            dma(6), dma(2, 5), dma(2, 4, nz), dma(4, 4, hops), dma(4, 4, hops),
            dma(4), dma(4), dma(4, max(w_cnt)), dma(4), dma(4), dma(4),
            dma(4, 4, hops), dma(4, 4, hops), dma(4, 2, nz), dma(4, 2, nz),
            dma(15 + c_attn * tiles),
        ]
        any_spec = pl.BlockSpec(memory_space=pl.ANY)
        call = pl.pallas_call(
            functools.partial(fused_step, n, counts, attn_rows, wide, narrow),
            out_shape=out_shape,
            in_specs=[any_spec] * 15,
            out_specs=[any_spec] * 15,
            scratch_shapes=scratch,
            compiler_params=pltpu.CompilerParams(
                collective_id=0, has_side_effects=True, vmem_limit_bytes=67043328),
            name="muon_step",
        )
        outs = list(hand_over(out_shape)(*call(*grads, *moms, *masters)))
        outs[:5], outs[5:10] = flip(outs[:5]), flip(outs[5:10])
        outs[10] = outs[10].reshape(c_attn, n * attn_rows, wide)
        outs[11], outs[13] = turn(outs[11]), turn(outs[13])
        return tuple(outs)

    grad_spec = P(("stage", "data"), None, None, None)
    row_spec = P("stage", "data", None)
    full_spec = P("stage", None, None)
    in_specs = (grad_spec,) * 5 + (row_spec,) * 10
    out_specs = (row_spec,) * 10 + (full_spec,) * 5
    return jax.shard_map(local_step, mesh=mesh, in_specs=in_specs, out_specs=out_specs, check_vma=False)
```

```python
import functools
import math
import jax
import jax.numpy as jnp
from jax import lax
from jax.experimental import pallas as pl
from jax.experimental.pallas import tpu as pltpu
from jax.sharding import PartitionSpec as P

NS_STEPS = 5
MOMENTUM = 0.95
LEARN_RATE = 0.2
WEIGHT_DECAY = 0.25
NORM_EPS = 1e-7
COEF_A = 3.4445
COEF_B = -4.7750
COEF_C = 2.0315

SCHEDULE = (
    ("pack", 0), ("rs", 0, 0, 1), ("rs", 0, 1, 1), ("pack", 1), ("rs", 1, 1, 1), ("rs", 1, 0, 1), ("rs", 0, 0, 2),
    ("rs", 1, 1, 2), ("rs", 0, 1, 2), ("pack", 2), ("rs", 1, 0, 2), ("rs", 0, 0, 3), ("rs", 1, 0, 3),
    ("rs", 1, 1, 3), ("nat", 0), ("rs", 0, 0, 4), ("rs", 0, 1, 3), ("pack", 3), ("rs", 1, 1, 4), ("rs", 1, 0, 4),
    ("rs", 3, 1, 1), ("rs", 3, 0, 1), ("rs", 0, 1, 4), ("fin", 1), ("rs", 2, 0, 1), ("rs", 3, 1, 2), ("fin", 0),
    ("rs", 2, 1, 1), ("rs", 2, 0, 2), ("rs", 3, 0, 2), ("x", 0), ("x", 1), ("rs", 3, 0, 3), ("rs", 2, 0, 3),
    ("nat", 1), ("rs", 3, 1, 3), ("rs", 2, 1, 2), ("rs", 3, 0, 4), ("own", 0, 1), ("own", 0, 2), ("rs", 2, 0, 4),
    ("own", 0, 3), ("own", 1, 0), ("rs", 2, 1, 3), ("rs", 3, 1, 4), ("rs", 2, 1, 4), ("mas", 1), ("ag", 1, 0, 1),
    ("fin", 3), ("fin", 2), ("mas", 0), ("ag", 1, 1, 1), ("ag", 0, 1, 1), ("ag", 1, 0, 2), ("ag", 1, 1, 2),
    ("x", 2), ("x", 3), ("ag", 0, 1, 2), ("ag", 1, 1, 3), ("ag", 0, 0, 1), ("own", 2, 0), ("ag", 1, 0, 3),
    ("own", 3, 0), ("ag", 0, 0, 2), ("natout", 0), ("ag", 1, 1, 4), ("ag", 0, 1, 3), ("ag", 1, 0, 4), ("mas", 2),
    ("ag", 2, 0, 1), ("ag", 2, 1, 1), ("mas", 3), ("ag", 3, 0, 1), ("ag", 1, 1, 5), ("ag", 3, 1, 1),
    ("ag", 2, 0, 2), ("ag", 2, 1, 2), ("ag", 3, 0, 2), ("natout", 1), ("ag", 3, 1, 2), ("ag", 0, 1, 4),
    ("ag", 1, 0, 5), ("ag", 2, 1, 3), ("ag", 0, 0, 3), ("ag", 2, 0, 3), ("un", 1), ("ag", 3, 1, 3),
    ("ag", 0, 1, 5), ("ag", 3, 0, 3), ("ag", 2, 1, 4), ("ag", 2, 0, 4), ("ag", 0, 0, 4), ("ag", 3, 1, 4),
    ("ag", 3, 0, 4), ("ag", 2, 0, 5), ("ag", 2, 1, 5), ("ag", 0, 0, 5), ("ag", 3, 1, 5), ("ag", 3, 0, 5),
    ("un", 2), ("un", 3), ("un", 0),
)

FIRST_PART = 0.5

F32 = jnp.float32
BF16 = jnp.bfloat16
MESH = pl.DeviceIdType.MESH
LANE = 128
NT = (((1,), (1,)), ((), ()))


def round_up(value, step):
    return (value + step - 1) // step * step


def fused_step(n, counts, attn_rows, wide, narrow, *refs):
    c_attn, c_si, c_so, c_ei, c_eo = counts
    c_in, c_out = c_si + c_ei, c_so + c_eo
    nz = n // 2
    hops_far, hops_near = nz // 2, nz - 1 - nz // 2
    tiles = wide // LANE
    in_rows = wide // n
    groups = LANE // in_rows
    out_rows = narrow // n
    out_pad = round_up(out_rows, 16)
    attn_blk = attn_rows * tiles
    out_blk = tiles * out_rows
    small_blk = round_up(out_blk, 16)
    cuts = [(q * small_blk, min(small_blk, narrow - q * small_blk)) for q in range(groups)]

    it = iter(refs)
    take = lambda k: [next(it) for _ in range(k)]
    g_attn, g_si, g_so, g_ei, g_eo = take(5)
    m_in = take(5)
    w_in = take(5)
    m_out = take(5)
    w_out = take(5)
    p_attn, p_si, p_so, p_ei, p_eo = take(5)
    (gp, rx0, rxr, ag, mp, wp, nat_m, nat_w, nrm, xtx, rxx, otx, rxo, xb, ab, bb,
     raw_in, raw_out, stage_in, stage_out) = take(20)
    (s_load, s_nat, s_d2d, s_rs, r_rs, s_nrm, r_nrm, s_x, r_x, s_o, r_o, s_ag, r_ag, s_agd, r_agd, s_out) = take(16)

    quad = narrow
    n_quads = c_ei // groups
    quads_b = n_quads // 2
    mats_b, mats_c = c_si + groups * quads_b, groups * (n_quads - quads_b)
    rows_b, rows_c = c_si * small_blk + quads_b * quad, (n_quads - quads_b) * quad
    rows_d = round_up(c_out * out_blk, 16)
    waves = [dict(kind="attn", cnt=c_attn, rows=c_attn * attn_blk, base=(c_in + c_out) % n),
             dict(kind="in", cnt=mats_b, rows=rows_b, base=0, shared=c_si, quads=quads_b, first=0),
             dict(kind="in", cnt=mats_c, rows=rows_c, base=mats_b % n, shared=0, quads=n_quads - quads_b, first=quads_b),
             dict(kind="out", cnt=c_out, rows=rows_d, base=c_in % n)]
    n_waves = len(waves)
    start = 0
    for w in waves:
        w["row0"] = start
        start += w["rows"]
        split = int(w["rows"] * FIRST_PART / 16 + 0.5) * 16
        w["halves"] = (pl.ds(w["row0"], split), pl.ds(w["row0"] + split, w["rows"] - split))
        w["quad0"] = w["row0"] + w.get("shared", 0) * small_blk
    out0 = waves[3]["row0"]

    me = lax.axis_index("data")
    z = me // 2
    c = lax.rem(me, 2)
    zmod = lambda v: lax.rem(v + 2 * nz, nz)
    dev = lambda zz, cc: {"data": zz * 2 + cc}
    partner = {"data": z * 2 + (1 - c)}
    others = [lax.rem(me + k, n) for k in range(1, n)]

    def remote(src, dst, ss, rs, where):
        return pltpu.make_async_remote_copy(src_ref=src, dst_ref=dst, send_sem=ss, recv_sem=rs,
                                            device_id=where, device_id_type=MESH)

    barrier = pltpu.get_barrier_semaphore()
    for d in others:
        pl.semaphore_signal(barrier, inc=1, device_id={"data": d}, device_id_type=MESH)

    def nat_copies():
        return [pltpu.make_async_copy(srcs[k], dsts[k], s_nat.at[which, k])
                for which, (srcs, dsts) in enumerate(((m_in, nat_m), (w_in, nat_w))) for k in range(5)]

    def lane_swap(blocks):
        lane = lax.broadcasted_iota(jnp.int32, (1, LANE), 1)
        blocks = list(blocks)
        dist = groups // 2
        while dist:
            width = dist * in_rows
            low = lax.rem(lane // width, 2) == 0
            for q in range(groups):
                if (q // dist) % 2 == 0:
                    x, y = blocks[q], blocks[q + dist]
                    if 2 * width == LANE:
                        turned = pltpu.roll(jnp.where(low, y, x), width, axis=1)
                        blocks[q] = jnp.where(low, x, turned)
                        blocks[q + dist] = jnp.where(low, turned, y)
                    else:
                        blocks[q] = jnp.where(low, x, pltpu.roll(y, width, axis=1))
                        blocks[q + dist] = jnp.where(low, pltpu.roll(x, LANE - width, axis=1), y)
            dist //= 2
        return blocks

    def pad_rows(x, rows):
        if x.shape[0] == rows:
            return x
        return jnp.concatenate([x, jnp.zeros((rows - x.shape[0], x.shape[1]), x.dtype)], axis=0)

    cut_in, cut_out = groups * quads_b, c_eo // groups

    def loads():
        return [
            pltpu.make_async_copy(g_si, raw_in.at[pl.ds(0, c_si)], s_load.at[1]),
            pltpu.make_async_copy(g_ei.at[pl.ds(0, cut_in)], raw_in.at[pl.ds(c_si, cut_in)], s_load.at[2]),
            pltpu.make_async_copy(g_ei.at[pl.ds(cut_in, c_ei - cut_in)], raw_in.at[pl.ds(c_si + cut_in, c_ei - cut_in)], s_load.at[3]),
            pltpu.make_async_copy(g_so, raw_out.at[pl.ds(c_eo, c_so)], s_load.at[4]),
            pltpu.make_async_copy(g_eo, raw_out.at[pl.ds(0, c_eo)], s_load.at[5]),
        ]

    def start_loads():
        for m in range(c_attn):
            for t in range(tiles):
                pltpu.make_async_copy(
                    g_attn.at[m, :, :, :, pl.ds(LANE * t, LANE)],
                    gp.at[:, :, pl.ds(m * attn_blk + t * attn_rows, attn_rows), :], s_load.at[0]).start()
        for cp in loads() + nat_copies():
            cp.start()

    def pack_in(i):
        w = waves[i]
        for j in range(w["shared"]):
            for t in range(tiles):
                cols = slice(LANE * t, LANE * (t + 1))
                got = lane_swap([pad_rows(raw_in[j, r:r + k, cols], small_blk) for r, k in cuts])
                for p in range(groups):
                    d = groups * t + p
                    gp[d // 2, d % 2, pl.ds(w["row0"] + small_blk * j, small_blk), :] = got[p]

        def body(j, carry):
            off = pl.multiple_of(w["quad0"] + quad * j, 8)
            first = c_si + groups * (w["first"] + j)
            for t in range(tiles):
                got = lane_swap([raw_in[first + p, :, LANE * t:LANE * (t + 1)] for p in range(groups)])
                for p in range(groups):
                    d = groups * t + p
                    gp[d // 2, d % 2, pl.ds(off, quad), :] = got[p]
            return carry

        lax.fori_loop(0, w["quads"], body, 0)

    def out_piece(m, d):
        return [raw_out[m, out_rows * d:out_rows * (d + 1), LANE * t:LANE * (t + 1)] for t in range(tiles)]

    def pack_out():
        def body(j, carry):
            off = pl.multiple_of(out0 + groups * out_blk * j, 8)
            for d in range(n):
                rows = sum([out_piece(groups * j + p, d) for p in range(groups)], [])
                gp[d // 2, d % 2, pl.ds(off, groups * out_blk), :] = jnp.concatenate(rows, axis=0)
            return carry

        lax.fori_loop(0, cut_out, body, 0)
        tail = rows_d - c_eo * out_blk
        for d in range(n):
            rows = sum([out_piece(m, d) for m in range(c_eo, c_out)], [])
            gp[d // 2, d % 2, pl.ds(out0 + c_eo * out_blk, tail), :] = pad_rows(jnp.concatenate(rows, axis=0), tail)

    def pack(i):
        load = loads
        if i == 0:
            view = gp.at[:, :, pl.ds(0, waves[0]["rows"]), :]
            pltpu.make_async_copy(view, view, s_load.at[0]).wait()
            pl.semaphore_wait(barrier, n - 1)
        elif i == 1:
            load()[0].wait()
            load()[1].wait()
            pack_in(1)
        elif i == 2:
            load()[2].wait()
            pack_in(2)
        else:
            load()[3].wait()
            load()[4].wait()
            pack_out()
        for k in near_last:
            d2d_copy(i, k).start()

    pending = []

    near_last = [hops_far]
    for k in range(hops_near, 0, -1):
        near_last += [k, nz - k]
    near_last.append(0)
    d2d_seen = set()

    def d2d_copy(i, k):
        sl = pl.ds(waves[i]["row0"], waves[i]["rows"])
        dest = zmod(z + k)
        return remote(gp.at[dest, 1 - c, sl, :], rx0.at[dest, sl, :], s_d2d.at[0, i, k], s_d2d.at[1, i, k], partner)

    def d2d_wait(i, k):
        if (i, k) not in d2d_seen:
            d2d_seen.add((i, k))
            d2d_copy(i, k).wait_recv()

    def mat_rows(i):
        w = waves[i]
        if w["kind"] == "attn":
            return [(m, pl.ds(attn_blk * m, attn_blk), None) for m in range(w["cnt"])]
        if w["kind"] == "out":
            return [(m, pl.ds(out0 + out_blk * m, out_blk), None) for m in range(w["cnt"])]
        got = [(m, pl.ds(w["row0"] + small_blk * m, small_blk), None) for m in range(w["shared"])]
        for j in range(w["quads"]):
            got += [(w["shared"] + groups * j + p, pl.ds(w["quad0"] + quad * j, quad), p) for p in range(groups)]
        return got

    hops = lambda h, dr: hops_far if h == dr else hops_near
    rs = {}

    def rs_send(i, h, dr, s):
        w = waves[i]
        length = hops(h, dr)
        step = length - s + 1
        dest = zmod(z + step) if dr == 0 else zmod(z - step)
        d2d_wait(i, step if dr == 0 else nz - step)
        sl = w["halves"][h]
        val = gp[dest, c, sl, :] + rx0[dest, sl, :]
        if s > 1:
            rs[i, h, dr, s - 1].wait_recv()
            val = val + rxr[dr, s - 2, sl, :]
        gp[dest, c, sl, :] = val
        where = dev(zmod(z + 1), c) if dr == 0 else dev(zmod(z - 1), c)
        cp = remote(gp.at[dest, c, sl, :], rxr.at[dr, s - 1, sl, :],
                    s_rs.at[i, h * 2 + dr, s - 1], r_rs.at[i, h * 2 + dr, s - 1], where)
        cp.start()
        rs[i, h, dr, s] = cp
        pending.append(cp)

    def rs_finish(i):
        w = waves[i]
        d2d_wait(i, 0)
        for h in range(2):
            sl = w["halves"][h]
            total = gp[z, c, sl, :] + rx0[z, sl, :]
            for dr in range(2):
                last = hops(h, dr)
                rs[i, h, dr, last].wait_recv()
                total = total + rxr[dr, last - 1, sl, :]
            mp[sl, :] = MOMENTUM * mp[sl, :] + total / n
        lane = lax.broadcasted_iota(jnp.int32, (1, LANE), 1)
        part = jnp.zeros((1, LANE), F32)
        for m, where, keep in mat_rows(i):
            block = mp[where, :]
            sq = jnp.sum(block * block, axis=0, keepdims=True)
            if keep is not None:
                sq = jnp.where(lane // in_rows == keep, sq, 0.0)
            part = jnp.where(lane == m, jnp.sum(sq, axis=1, keepdims=True), part)
        nrm[i, me] = part
        for d in others:
            remote(nrm.at[i, me], nrm.at[i, me], s_nrm.at[i], r_nrm.at[i], {"data": d}).start()

    def nrm_wait(i, sem):
        view = nrm.at[i, pl.ds(0, n - 1)]
        pltpu.make_async_copy(view, view, sem).wait()

    def x_copy(i, m):
        w = waves[i]
        owner = (w["base"] + m) % n
        return remote(xtx[i].at[m], rxx[i].at[me], s_x.at[i, m], r_x.at[i], {"data": owner})

    def x_send(i):
        w = waves[i]
        nrm_wait(i, r_nrm.at[i])
        tot = jnp.zeros((1, LANE), F32)
        for d in range(n):
            tot = tot + nrm[i, d]
        lane = lax.broadcasted_iota(jnp.int32, (1, LANE), 1)
        norms = [jnp.sqrt(jnp.sum(jnp.where(lane == m, tot, 0.0), axis=1, keepdims=True)) + NORM_EPS for m in range(w["cnt"])]
        blocks = []
        if w["kind"] == "in":
            for m in range(w["shared"]):
                blocks.append(mp[pl.ds(w["row0"] + small_blk * m, small_blk), :] / norms[m])
            for j in range(w["quads"]):
                m = w["shared"] + groups * j
                norm = norms[m]
                for p in range(1, groups):
                    norm = jnp.where(lane // in_rows == p, norms[m + p], norm)
                x = mp[pl.ds(w["quad0"] + quad * j, quad), :] / norm
                blocks += lane_swap([pad_rows(x[r:r + k], small_blk) for r, k in cuts])
        else:
            for m, where, _ in mat_rows(i):
                x = mp[where, :] / norms[m]
                blocks.append(pad_rows(x, small_blk) if w["kind"] == "out" else x)
        for m, x in enumerate(blocks):
            x = x.astype(BF16)
            xtx[i][m] = x
            owner = (w["base"] + m) % n

            @pl.when(me != owner)
            def _():
                x_copy(i, m).start()

            @pl.when(me == owner)
            def _():
                rxx[i][me] = x

    def owned(i):
        w = waves[i]
        mine = lax.rem(me - w["base"] + n, n)
        return mine, mine < w["cnt"]

    def assemble(i):
        kind = waves[i]["kind"]
        rx = rxx[i]
        if kind == "attn":
            for t in range(tiles):
                xb[:, LANE * t:LANE * (t + 1)] = rx[:, attn_rows * t:attn_rows * (t + 1), :].reshape(n * attn_rows, LANE)
        elif kind == "out":
            for d in range(n):
                blk = rx[d].astype(F32)
                for t in range(tiles):
                    piece = pad_rows(blk[out_rows * t:out_rows * (t + 1)], out_pad)
                    xb[out_pad * d:out_pad * (d + 1), LANE * t:LANE * (t + 1)] = piece.astype(BF16)
        else:
            for t in range(tiles):
                got = lane_swap([rx[groups * t + p].astype(F32) for p in range(groups)])
                for q, (r, k) in enumerate(cuts):
                    xb[r:r + k, LANE * t:LANE * (t + 1)] = got[q][:k].astype(BF16)
            xb[narrow:n * out_pad, :] = jnp.zeros((n * out_pad - narrow, wide), BF16)

    def disassemble(i):
        kind = waves[i]["kind"]
        tx = otx[i]
        if kind == "attn":
            for t in range(tiles):
                tx[:, attn_rows * t:attn_rows * (t + 1), :] = xb[:, LANE * t:LANE * (t + 1)].reshape(n, attn_rows, LANE)
        elif kind == "out":
            for d in range(n):
                blk = xb[out_pad * d:out_pad * (d + 1), :].astype(F32)
                parts = [blk[:out_rows, LANE * t:LANE * (t + 1)] for t in range(tiles)]
                tx[d] = pad_rows(jnp.concatenate(parts, axis=0), small_blk).astype(BF16)
        else:
            for t in range(tiles):
                cols = slice(LANE * t, LANE * (t + 1))
                got = lane_swap([pad_rows(xb[r:r + k, cols].astype(F32), small_blk) for r, k in cuts])
                for p in range(groups):
                    tx[groups * t + p] = got[p].astype(BF16)

    def iterate(size, steps):
        cut = min(size, 256)

        def one(_, carry):
            for r in range(size // cut):
                sl = slice(r * cut, (r + 1) * cut)
                gram = lax.dot_general(xb[sl, :], xb[:size, :], NT, preferred_element_type=F32)
                ab[sl, :size] = gram.astype(BF16)
            for r in range(size // cut):
                sl = slice(r * cut, (r + 1) * cut)
                square = jnp.dot(ab[sl, :size], ab[:size, :size], preferred_element_type=F32)
                bb[sl, :size] = (COEF_B * ab[sl, :size].astype(F32) + COEF_C * square).astype(BF16)
            for r in range(wide // 256):
                sl = slice(r * 256, (r + 1) * 256)
                update = jnp.dot(bb[:size, :size], xb[:size, sl], preferred_element_type=F32)
                xb[:size, sl] = (COEF_A * xb[:size, sl].astype(F32) + update).astype(BF16)
            return carry

        lax.fori_loop(0, steps, one, 0)

    def o_copy(i, mine, d):
        return remote(otx[i].at[d], rxo[i].at[mine], s_o.at[i], r_o.at[i], {"data": d})

    def owner_work(i, begin, steps, end):
        mine, yes = owned(i)

        @pl.when(yes)
        def _():
            if begin:
                view = rxx[i].at[pl.ds(0, n - 1)]
                pltpu.make_async_copy(view, view, r_x.at[i]).wait()
                assemble(i)
            iterate(n * attn_rows if waves[i]["kind"] == "attn" else n * out_pad, steps)
            if end:
                disassemble(i)
                for d in others:
                    o_copy(i, mine, d).start()
                rxo[i][mine] = otx[i][me]

    def master(i):
        w = waves[i]
        mine, yes = owned(i)
        cnt = w["cnt"]

        @pl.when(yes)
        def _():
            view = rxo[i].at[pl.ds(0, cnt - 1)]
            pltpu.make_async_copy(view, view, r_o.at[i]).wait()

        @pl.when(jnp.logical_not(yes))
        def _():
            pltpu.make_async_copy(rxo[i], rxo[i], r_o.at[i]).wait()

        step_scale = 0.2 * math.sqrt(wide)

        def update(where, o):
            old = wp[where, :]
            wp[where, :] = old - LEARN_RATE * (step_scale * o + WEIGHT_DECAY * old)

        if w["kind"] == "in":
            for m in range(w["shared"]):
                update(pl.ds(w["row0"] + small_blk * m, small_blk), rxo[i][m].astype(F32))
            for j in range(w["quads"]):
                m = w["shared"] + groups * j
                got = lane_swap([rxo[i][m + p].astype(F32) for p in range(groups)])
                o = jnp.concatenate([got[q][:k] for q, (r, k) in enumerate(cuts)], axis=0)
                update(pl.ds(w["quad0"] + quad * j, quad), o)
        else:
            for m, where, _ in mat_rows(i):
                o = rxo[i][m].astype(F32)
                update(where, o[:out_blk] if w["kind"] == "out" else o)
        sl = pl.ds(w["row0"], w["rows"])
        ag[z, c, sl, :] = wp[sl, :].astype(BF16)

    agc = {}
    agd = {}

    def ag_rows(i, h):
        return waves[i]["halves"][h]

    def ag_to_partner(i, h, src, key):
        part = ag.at[src, c, ag_rows(i, h), :]
        cp = remote(part, part, s_agd.at[i, h, key], r_agd.at[i, h, key], partner)
        cp.start()
        agd[i, h, key] = cp
        pending.append(cp)

    def ag_send(i, h, dr, s):
        length = hops(h, dr)
        src = z if s == 1 else (zmod(z - (s - 1)) if dr == 0 else zmod(z + (s - 1)))
        if s > 1:
            agc[i, h, dr, s - 1].wait_recv()
        if s <= length:
            part = ag.at[src, c, ag_rows(i, h), :]
            where = dev(zmod(z + 1), c) if dr == 0 else dev(zmod(z - 1), c)
            cp = remote(part, part, s_ag.at[i, h * 2 + dr, s - 1], r_ag.at[i, h * 2 + dr, s - 1], where)
            cp.start()
            agc[i, h, dr, s] = cp
            pending.append(cp)
        if s > 1:
            ag_to_partner(i, h, src, (s - 1) if dr == 0 else nz - (s - 1))
        elif dr == 0:
            ag_to_partner(i, h, src, 0)

    out_copies = []

    def out_copy(src, dst, k):
        cp = pltpu.make_async_copy(src, dst, s_out.at[k])
        cp.start()
        out_copies.append(cp)

    def quad_row(j):
        return waves[1]["quad0"] + quad * j if j < quads_b else waves[2]["quad0"] + quad * (j - quads_b)

    def out_rows_of():
        return [(4, m, out0 + out_blk * m) for m in range(c_eo)] + [(2, m, out0 + out_blk * (c_eo + m)) for m in range(c_so)]

    def native_outputs(which):
        for src, nat, outs in (((mp, nat_m, m_out), (wp, nat_w, w_out))[which],):
            for m in range(c_attn):
                for t in range(tiles):
                    nat[0][m, :, LANE * t:LANE * (t + 1)] = src[pl.ds(m * attn_blk + t * attn_rows, attn_rows), :]
            some = c_si
            off = waves[1]["row0"]
            got = [src[off + small_blk * p:off + small_blk * (p + 1), :] for p in range(some)]
            got += [jnp.zeros((small_blk, LANE), F32)] * (groups - some)
            block = pad_rows(jnp.concatenate(lane_swap(got), axis=0), 2 * LANE).T
            for p in range(some):
                nat[1][p] = block[in_rows * p:in_rows * (p + 1), :narrow]
            for j in range(n_quads):
                block = pad_rows(src[pl.ds(quad_row(j), quad), :], 2 * LANE).T
                for p in range(groups):
                    nat[3][groups * j + p] = block[in_rows * p:in_rows * (p + 1), :narrow]
            for k, m, off in out_rows_of():
                for t in range(tiles):
                    nat[k][:, m, LANE * t:LANE * (t + 1)] = src[off + t * out_rows:off + (t + 1) * out_rows, :]
            for k in range(5):
                out_copy(nat[k], outs[k], which * 5 + k)

    def native_inputs(which):
        for cp in nat_copies()[5 * which:5 * which + 5]:
            cp.wait()
        for nat, dst in (((nat_m, mp), (nat_w, wp))[which],):
            for m in range(c_attn):
                for t in range(tiles):
                    dst[pl.ds(m * attn_blk + t * attn_rows, attn_rows), :] = nat[0][m, :, LANE * t:LANE * (t + 1)]
            wider = lambda x: jnp.concatenate([x, jnp.zeros((LANE, 2 * LANE - narrow), F32)], axis=1)
            block = pad_rows(jnp.concatenate([nat[1][p] for p in range(c_si)], axis=0), LANE)
            block = wider(block).T
            got = lane_swap([block[small_blk * q:small_blk * (q + 1)] for q in range(groups)])
            for p in range(c_si):
                dst[pl.ds(waves[1]["row0"] + small_blk * p, small_blk), :] = got[p]
            for j in range(n_quads):
                block = jnp.concatenate([nat[3][groups * j + p] for p in range(groups)], axis=0)
                dst[pl.ds(quad_row(j), quad), :] = wider(block).T[:quad]
            for k, m, off in out_rows_of():
                rows = [nat[k][:, m, LANE * t:LANE * (t + 1)] for t in range(tiles)]
                dst[pl.ds(off, out_blk), :] = jnp.concatenate(rows, axis=0)
            spare = rows_d - c_out * out_blk
            if spare:
                dst[pl.ds(out0 + c_out * out_blk, spare), :] = jnp.zeros((spare, LANE), F32)

    def unpack(i):
        w = waves[i]
        for h in range(2):
            for key in range(nz):
                agd[i, h, key].wait_recv()
        if w["kind"] == "attn":
            for m in range(c_attn):
                for t in range(tiles):
                    out_copies.append(pltpu.make_async_copy(
                        ag.at[:, :, pl.ds(m * attn_blk + t * attn_rows, attn_rows), :],
                        p_attn.at[m, :, :, :, pl.ds(LANE * t, LANE)], s_out.at[10 + m * tiles + t]))
                    out_copies[-1].start()
        elif w["kind"] == "in":
            for j in range(w["shared"]):
                sl = pl.ds(w["row0"] + small_blk * j, small_blk)
                for t in range(tiles):
                    devs = [groups * t + p for p in range(groups)]
                    got = lane_swap([ag[d // 2, d % 2, sl, :].astype(F32) for d in devs])
                    for q, (r, k) in enumerate(cuts):
                        stage_in[j, r:r + k, LANE * t:LANE * (t + 1)] = got[q][:k].astype(BF16)

            def body(j, carry):
                off = pl.multiple_of(w["quad0"] + quad * j, 16)
                first = c_si + groups * (w["first"] + j)
                for t in range(tiles):
                    devs = [groups * t + p for p in range(groups)]
                    got = lane_swap([ag[d // 2, d % 2, pl.ds(off, quad), :].astype(F32) for d in devs])
                    for p in range(groups):
                        stage_in[first + p, :, LANE * t:LANE * (t + 1)] = got[p].astype(BF16)
                return carry

            lax.fori_loop(0, w["quads"], body, 0)
            k = 10 + c_attn * tiles
            if w["shared"]:
                out_copy(stage_in.at[pl.ds(0, c_si)], p_si, k)
            first, cnt = groups * w["first"], groups * w["quads"]
            out_copy(stage_in.at[pl.ds(c_si + first, cnt)], p_ei.at[pl.ds(first, cnt)], k + 1 + (w["first"] > 0))
        else:
            def put(blk, m, first, d):
                for t in range(tiles):
                    r = out_blk * m + t * out_rows
                    raw_out[first + m, out_rows * d:out_rows * (d + 1), LANE * t:LANE * (t + 1)] = blk[r:r + out_rows]

            def body(j, carry):
                off = pl.multiple_of(out0 + groups * out_blk * j, 16)
                for d in range(n):
                    blk = ag[d // 2, d % 2, pl.ds(off, groups * out_blk), :].astype(F32)
                    for p in range(groups):
                        put(blk, p, groups * j, d)
                for p in range(groups):
                    stage_out[groups * j + p] = raw_out[groups * j + p].astype(BF16)
                return carry

            lax.fori_loop(0, cut_out, body, 0)
            for d in range(n):
                blk = ag[d // 2, d % 2, pl.ds(out0 + c_eo * out_blk, rows_d - c_eo * out_blk), :].astype(F32)
                for m in range(c_so):
                    put(blk, m, c_eo, d)
            for m in range(c_eo, c_out):
                stage_out[m] = raw_out[m].astype(BF16)
            k = 13 + c_attn * tiles
            out_copy(stage_out.at[pl.ds(c_eo, c_so)], p_so, k)
            out_copy(stage_out.at[pl.ds(0, c_eo)], p_eo, k + 1)

    def both(func, length, i, h, s):
        for dr in range(2):
            if s <= hops(h, dr) + length:
                func(i, h, dr, s)

    def own(i, part):
        begin, steps, end = ((True, NS_STEPS, True), (True, 1, False), (False, 2, False), (False, NS_STEPS - 3, True))[part]
        owner_work(i, begin, steps, end)

    acts = dict(pack=pack, nat=native_inputs, rs=functools.partial(both, rs_send, 0), fin=rs_finish, x=x_send, own=own,
                mas=master, ag=functools.partial(both, ag_send, 1), natout=native_outputs, un=unpack)
    start_loads()
    for name, *where in SCHEDULE:
        acts[name](*where)

    for cp in out_copies:
        cp.wait()
    for cp in pending:
        cp.wait_send()
    for i in range(n_waves):
        for k in range(nz):
            d2d_copy(i, k).wait_send()
        nrm_wait(i, s_nrm.at[i])
        for m in range(waves[i]["cnt"]):
            owner = (waves[i]["base"] + m) % n

            @pl.when(me != owner)
            def _():
                x_copy(i, m).wait_send()
        mine, yes = owned(i)

        @pl.when(yes)
        def _():
            view = otx[i].at[pl.ds(0, n - 1)]
            pltpu.make_async_copy(view, view, s_o.at[i]).wait()


def hand_over(shapes):
    count = len(shapes)
    pieces = []
    for k, x in enumerate(shapes):
        parts = next((p for p in (4, 2) if x.shape[0] % p == 0 and x.size > 400000), 1)
        step = x.shape[0] // parts
        pieces += [(k, p * step, step) for p in range(parts)]

    def kernel(*refs):
        src, dst, buf, sem_in, sem_out = refs[:count], refs[count:2 * count], refs[2 * count:3 * count], refs[-2], refs[-1]
        first = [pltpu.make_async_copy(src[k].at[pl.ds(r, m)], buf[k].at[pl.ds(r, m)], sem_in.at[i])
                 for i, (k, r, m) in enumerate(pieces)]
        second = [pltpu.make_async_copy(buf[k].at[pl.ds(r, m)], dst[k].at[pl.ds(r, m)], sem_out.at[i])
                  for i, (k, r, m) in enumerate(pieces)]
        for cp in first:
            cp.start()
        for one, two in zip(first, second):
            one.wait()
            two.start()
        for cp in second:
            cp.wait()

    any_spec = pl.BlockSpec(memory_space=pl.ANY)
    return pl.pallas_call(
        kernel, out_shape=shapes, in_specs=[any_spec] * count, out_specs=[any_spec] * count,
        scratch_shapes=[pltpu.VMEM(x.shape, x.dtype) for x in shapes]
        + [pltpu.SemaphoreType.DMA((len(pieces),)), pltpu.SemaphoreType.DMA((len(pieces),))],
        name="hand_over")


def solution(mesh):
    n = mesh.shape["data"]
    nz = n // 2

    def local_step(*arrays):
        grads, moms, masters = arrays[:5], arrays[5:10], arrays[10:]
        counts = tuple(m.shape[0] for m in moms)
        attn_rows, wide = moms[0].shape[1:]
        narrow = moms[1].shape[2]
        c_attn, c_si, c_so, c_ei, c_eo = counts
        c_in, c_out = c_si + c_ei, c_so + c_eo
        tiles = wide // LANE
        groups = LANE // (wide // n)
        out_blk = tiles * (narrow // n)
        small_blk = round_up(out_blk, 16)
        out_pad = round_up(narrow // n, 16)
        attn_blk = attn_rows * tiles
        rows = c_attn * attn_blk + c_si * small_blk + c_ei // groups * narrow + round_up(c_out * out_blk, 16)
        mats_b = c_si + groups * (c_ei // groups // 2)
        turn = lambda x: jnp.swapaxes(x, -1, -2)
        grads = [g[0] for g in grads]
        grads[1], grads[3] = turn(grads[1]), turn(grads[3])
        flip = lambda arrs: [jnp.swapaxes(x, 0, 1) if k in (2, 4) else x for k, x in enumerate(arrs)]
        moms, masters = flip(moms), flip(masters)
        grads[0] = grads[0].reshape(c_attn, nz, 2, attn_rows, wide)
        hops = nz // 2

        sds = jax.ShapeDtypeStruct
        out_shape = [sds(m.shape, F32) for m in moms] * 2
        out_shape += [sds((c_attn, nz, 2, attn_rows, wide), BF16)]
        out_shape += [sds((k, narrow, wide), BF16) for k in counts[1:]]
        w_cnt = (c_attn, mats_b, c_in - mats_b, c_out)
        w_blk = (attn_blk, small_blk, small_blk, small_blk)
        dma = lambda *shape: pltpu.SemaphoreType.DMA(shape)
        vm = pltpu.VMEM
        scratch = [
            vm((nz, 2, rows, LANE), F32),
            vm((nz, rows, LANE), F32),
            vm((2, hops, rows, LANE), F32),
            vm((nz, 2, rows, LANE), BF16),
            vm((rows, LANE), F32),
            vm((rows, LANE), F32),
            [vm(m.shape, F32) for m in moms],
            [vm(m.shape, F32) for m in moms],
            vm((4, n, 1, LANE), F32),
            [vm((k, b, LANE), BF16) for k, b in zip(w_cnt, w_blk)],
            [vm((n, b, LANE), BF16) for b in w_blk],
            [vm((n, b, LANE), BF16) for b in w_blk],
            [vm((k, b, LANE), BF16) for k, b in zip(w_cnt, w_blk)],
            vm((n * attn_rows, wide), BF16),
            vm((n * attn_rows, n * attn_rows), BF16),
            vm((n * attn_rows, n * attn_rows), BF16),
            vm((c_in, narrow, wide), F32),
            vm((c_out, narrow, wide), F32),
            vm((c_in, narrow, wide), BF16),
            vm((c_out, narrow, wide), BF16),
            dma(6), dma(2, 5), dma(2, 4, nz), dma(4, 4, hops), dma(4, 4, hops),
            dma(4), dma(4), dma(4, max(w_cnt)), dma(4), dma(4), dma(4),
            dma(4, 4, hops), dma(4, 4, hops), dma(4, 2, nz), dma(4, 2, nz),
            dma(15 + c_attn * tiles),
        ]
        any_spec = pl.BlockSpec(memory_space=pl.ANY)
        call = pl.pallas_call(
            functools.partial(fused_step, n, counts, attn_rows, wide, narrow),
            out_shape=out_shape,
            in_specs=[any_spec] * 15,
            out_specs=[any_spec] * 15,
            scratch_shapes=scratch,
            compiler_params=pltpu.CompilerParams(
                collective_id=0, has_side_effects=True, vmem_limit_bytes=67043328),
            name="muon_step",
        )
        outs = list(hand_over(out_shape)(*call(*grads, *moms, *masters)))
        outs[:5], outs[5:10] = flip(outs[:5]), flip(outs[5:10])
        outs[10] = outs[10].reshape(c_attn, n * attn_rows, wide)
        outs[11], outs[13] = turn(outs[11]), turn(outs[13])
        return tuple(outs)

    grad_spec = P(("stage", "data"), None, None, None)
    row_spec = P("stage", "data", None)
    full_spec = P("stage", None, None)
    in_specs = (grad_spec,) * 5 + (row_spec,) * 10
    out_specs = (row_spec,) * 10 + (full_spec,) * 5
    return jax.shard_map(local_step, mesh=mesh, in_specs=in_specs, out_specs=out_specs, check_vma=False)
```

```python
import functools
import math
import jax
import jax.numpy as jnp
from jax import lax
from jax.experimental import pallas as pl
from jax.experimental.pallas import tpu as pltpu
from jax.sharding import PartitionSpec as P

NS_STEPS = 5
MOMENTUM = 0.95
LEARN_RATE = 0.2
WEIGHT_DECAY = 0.25
NORM_EPS = 1e-7
COEF_A = 3.4445
COEF_B = -4.7750
COEF_C = 2.0315

SCHEDULE = (
    ("pack", 0), ("nat", 0), ("rs", 0, 1, 1), ("pack", 1), ("rs", 0, 0, 1), ("rs", 1, 1, 1), ("rs", 0, 1, 2),
    ("pack", 2), ("rs", 1, 0, 1), ("rs", 0, 0, 2), ("rs", 0, 1, 3), ("rs", 1, 1, 2), ("rs", 1, 0, 2),
    ("rs", 0, 0, 3), ("rs", 1, 1, 3), ("rs", 1, 0, 3), ("rs", 0, 0, 4), ("rs", 1, 1, 4), ("rs", 0, 1, 4),
    ("pack", 3), ("rs", 2, 0, 1), ("rs", 1, 0, 4), ("rs", 3, 0, 1), ("rs", 2, 1, 1), ("fin", 1), ("fin", 0),
    ("rs", 3, 0, 2), ("rs", 2, 1, 2), ("rs", 3, 1, 1), ("x", 0), ("rs", 2, 0, 2), ("rs", 2, 1, 3), ("x", 1),
    ("rs", 3, 1, 2), ("nat", 1), ("own", 0, 1), ("own", 0, 2), ("rs", 3, 0, 3), ("rs", 2, 0, 3), ("own", 0, 3),
    ("rs", 3, 1, 3), ("own", 1, 0), ("rs", 2, 1, 4), ("rs", 3, 1, 4), ("rs", 2, 0, 4), ("rs", 3, 0, 4), ("fin", 2),
    ("mas", 1), ("ag", 1, 1, 1), ("fin", 3), ("mas", 0), ("ag", 0, 1, 1), ("ag", 1, 0, 1), ("ag", 1, 1, 2),
    ("ag", 0, 0, 1), ("x", 2), ("x", 3), ("ag", 0, 1, 2), ("ag", 1, 1, 3), ("ag", 1, 0, 2), ("own", 2, 0),
    ("ag", 0, 0, 2), ("own", 3, 0), ("ag", 1, 0, 3), ("ag", 1, 1, 4), ("ag", 0, 1, 3), ("ag", 0, 0, 3), ("mas", 2),
    ("ag", 2, 0, 1), ("mas", 3), ("ag", 3, 1, 1), ("ag", 1, 1, 5), ("ag", 3, 0, 1), ("ag", 2, 1, 1),
    ("ag", 1, 0, 4), ("natout", 0), ("ag", 2, 0, 2), ("ag", 3, 1, 2), ("ag", 3, 0, 2), ("ag", 0, 1, 4),
    ("ag", 1, 0, 5), ("ag", 2, 1, 2), ("natout", 1), ("ag", 2, 0, 3), ("ag", 3, 1, 3), ("ag", 3, 0, 3), ("un", 1),
    ("ag", 2, 1, 3), ("ag", 3, 1, 4), ("ag", 3, 0, 4), ("ag", 0, 1, 5), ("ag", 0, 0, 4), ("ag", 2, 0, 4),
    ("ag", 2, 1, 4), ("ag", 3, 0, 5), ("ag", 3, 1, 5), ("ag", 0, 0, 5), ("ag", 2, 0, 5), ("ag", 2, 1, 5),
    ("un", 3), ("un", 0), ("un", 2),
)

FIRST_PART = 0.4

F32 = jnp.float32
BF16 = jnp.bfloat16
MESH = pl.DeviceIdType.MESH
LANE = 128
NT = (((1,), (1,)), ((), ()))


def round_up(value, step):
    return (value + step - 1) // step * step


def fused_step(n, counts, attn_rows, wide, narrow, *refs):
    c_attn, c_si, c_so, c_ei, c_eo = counts
    c_in, c_out = c_si + c_ei, c_so + c_eo
    nz = n // 2
    hops_far, hops_near = nz // 2, nz - 1 - nz // 2
    tiles = wide // LANE
    in_rows = wide // n
    groups = LANE // in_rows
    out_rows = narrow // n
    out_pad = round_up(out_rows, 16)
    attn_blk = attn_rows * tiles
    out_blk = tiles * out_rows
    small_blk = round_up(out_blk, 16)
    cuts = [(q * small_blk, min(small_blk, narrow - q * small_blk)) for q in range(groups)]

    it = iter(refs)
    take = lambda k: [next(it) for _ in range(k)]
    g_attn, g_si, g_so, g_ei, g_eo = take(5)
    m_in = take(5)
    w_in = take(5)
    m_out = take(5)
    w_out = take(5)
    p_attn, p_si, p_so, p_ei, p_eo = take(5)
    (gp, rx0, rxr, ag, mp, wp, nat_m, nat_w, nrm, xtx, rxx, otx, rxo, xb, ab, bb,
     raw_in, raw_out, stage_in, stage_out) = take(20)
    (s_load, s_nat, s_d2d, s_rs, r_rs, s_nrm, r_nrm, s_x, r_x, s_o, r_o, s_ag, r_ag, s_agd, r_agd, s_out) = take(16)

    quad = narrow
    n_quads = c_ei // groups
    quads_b = n_quads // 2
    mats_b, mats_c = c_si + groups * quads_b, groups * (n_quads - quads_b)
    rows_b, rows_c = c_si * small_blk + quads_b * quad, (n_quads - quads_b) * quad
    rows_d = round_up(c_out * out_blk, 16)
    waves = [dict(kind="attn", cnt=c_attn, rows=c_attn * attn_blk, base=(c_in + c_out) % n),
             dict(kind="in", cnt=mats_b, rows=rows_b, base=0, shared=c_si, quads=quads_b, first=0),
             dict(kind="in", cnt=mats_c, rows=rows_c, base=mats_b % n, shared=0, quads=n_quads - quads_b, first=quads_b),
             dict(kind="out", cnt=c_out, rows=rows_d, base=c_in % n)]
    n_waves = len(waves)
    start = 0
    for w in waves:
        w["row0"] = start
        start += w["rows"]
        split = int(w["rows"] * FIRST_PART / 16 + 0.5) * 16
        w["halves"] = (pl.ds(w["row0"], split), pl.ds(w["row0"] + split, w["rows"] - split))
        w["quad0"] = w["row0"] + w.get("shared", 0) * small_blk
    out0 = waves[3]["row0"]

    me = lax.axis_index("data")
    z = me // 2
    c = lax.rem(me, 2)
    zmod = lambda v: lax.rem(v + 2 * nz, nz)
    dev = lambda zz, cc: {"data": zz * 2 + cc}
    partner = {"data": z * 2 + (1 - c)}
    others = [lax.rem(me + k, n) for k in range(1, n)]

    def remote(src, dst, ss, rs, where):
        return pltpu.make_async_remote_copy(src_ref=src, dst_ref=dst, send_sem=ss, recv_sem=rs,
                                            device_id=where, device_id_type=MESH)

    barrier = pltpu.get_barrier_semaphore()
    for d in others:
        pl.semaphore_signal(barrier, inc=1, device_id={"data": d}, device_id_type=MESH)

    def nat_copies():
        return [pltpu.make_async_copy(srcs[k], dsts[k], s_nat.at[which, k])
                for which, (srcs, dsts) in enumerate(((m_in, nat_m), (w_in, nat_w))) for k in range(5)]

    def lane_swap(blocks):
        lane = lax.broadcasted_iota(jnp.int32, (1, LANE), 1)
        blocks = list(blocks)
        dist = groups // 2
        while dist:
            width = dist * in_rows
            low = lax.rem(lane // width, 2) == 0
            for q in range(groups):
                if (q // dist) % 2 == 0:
                    x, y = blocks[q], blocks[q + dist]
                    if 2 * width == LANE:
                        turned = pltpu.roll(jnp.where(low, y, x), width, axis=1)
                        blocks[q] = jnp.where(low, x, turned)
                        blocks[q + dist] = jnp.where(low, turned, y)
                    else:
                        blocks[q] = jnp.where(low, x, pltpu.roll(y, width, axis=1))
                        blocks[q + dist] = jnp.where(low, pltpu.roll(x, LANE - width, axis=1), y)
            dist //= 2
        return blocks

    def pad_rows(x, rows):
        if x.shape[0] == rows:
            return x
        return jnp.concatenate([x, jnp.zeros((rows - x.shape[0], x.shape[1]), x.dtype)], axis=0)

    cut_in, cut_out = groups * quads_b, c_eo // groups

    def loads():
        return [
            pltpu.make_async_copy(g_si, raw_in.at[pl.ds(0, c_si)], s_load.at[1]),
            pltpu.make_async_copy(g_ei.at[pl.ds(0, cut_in)], raw_in.at[pl.ds(c_si, cut_in)], s_load.at[2]),
            pltpu.make_async_copy(g_ei.at[pl.ds(cut_in, c_ei - cut_in)], raw_in.at[pl.ds(c_si + cut_in, c_ei - cut_in)], s_load.at[3]),
            pltpu.make_async_copy(g_so, raw_out.at[pl.ds(c_eo, c_so)], s_load.at[4]),
            pltpu.make_async_copy(g_eo, raw_out.at[pl.ds(0, c_eo)], s_load.at[5]),
        ]

    def start_loads():
        for m in range(c_attn):
            for t in range(tiles):
                pltpu.make_async_copy(
                    g_attn.at[m, :, :, :, pl.ds(LANE * t, LANE)],
                    gp.at[:, :, pl.ds(m * attn_blk + t * attn_rows, attn_rows), :], s_load.at[0]).start()
        for cp in loads() + nat_copies():
            cp.start()

    def pack_in(i):
        w = waves[i]
        for j in range(w["shared"]):
            for t in range(tiles):
                cols = slice(LANE * t, LANE * (t + 1))
                got = lane_swap([pad_rows(raw_in[j, r:r + k, cols], small_blk) for r, k in cuts])
                for p in range(groups):
                    d = groups * t + p
                    gp[d // 2, d % 2, pl.ds(w["row0"] + small_blk * j, small_blk), :] = got[p]

        def body(j, carry):
            off = pl.multiple_of(w["quad0"] + quad * j, 8)
            first = c_si + groups * (w["first"] + j)
            for t in range(tiles):
                got = lane_swap([raw_in[first + p, :, LANE * t:LANE * (t + 1)] for p in range(groups)])
                for p in range(groups):
                    d = groups * t + p
                    gp[d // 2, d % 2, pl.ds(off, quad), :] = got[p]
            return carry

        lax.fori_loop(0, w["quads"], body, 0)

    def out_piece(m, d):
        return [raw_out[m, out_rows * d:out_rows * (d + 1), LANE * t:LANE * (t + 1)] for t in range(tiles)]

    def pack_out():
        def body(j, carry):
            off = pl.multiple_of(out0 + groups * out_blk * j, 8)
            for d in range(n):
                rows = sum([out_piece(groups * j + p, d) for p in range(groups)], [])
                gp[d // 2, d % 2, pl.ds(off, groups * out_blk), :] = jnp.concatenate(rows, axis=0)
            return carry

        lax.fori_loop(0, cut_out, body, 0)
        tail = rows_d - c_eo * out_blk
        for d in range(n):
            rows = sum([out_piece(m, d) for m in range(c_eo, c_out)], [])
            gp[d // 2, d % 2, pl.ds(out0 + c_eo * out_blk, tail), :] = pad_rows(jnp.concatenate(rows, axis=0), tail)

    def pack(i):
        load = loads
        if i == 0:
            view = gp.at[:, :, pl.ds(0, waves[0]["rows"]), :]
            pltpu.make_async_copy(view, view, s_load.at[0]).wait()
            pl.semaphore_wait(barrier, n - 1)
        elif i == 1:
            load()[0].wait()
            load()[1].wait()
            pack_in(1)
        elif i == 2:
            load()[2].wait()
            pack_in(2)
        else:
            load()[3].wait()
            load()[4].wait()
            pack_out()
        for k in near_last:
            d2d_copy(i, k).start()

    pending = []

    near_last = [hops_far]
    for k in range(hops_near, 0, -1):
        near_last += [k, nz - k]
    near_last.append(0)
    d2d_seen = set()

    def d2d_copy(i, k):
        sl = pl.ds(waves[i]["row0"], waves[i]["rows"])
        dest = zmod(z + k)
        return remote(gp.at[dest, 1 - c, sl, :], rx0.at[dest, sl, :], s_d2d.at[0, i, k], s_d2d.at[1, i, k], partner)

    def d2d_wait(i, k):
        if (i, k) not in d2d_seen:
            d2d_seen.add((i, k))
            d2d_copy(i, k).wait_recv()

    def mat_rows(i):
        w = waves[i]
        if w["kind"] == "attn":
            return [(m, pl.ds(attn_blk * m, attn_blk), None) for m in range(w["cnt"])]
        if w["kind"] == "out":
            return [(m, pl.ds(out0 + out_blk * m, out_blk), None) for m in range(w["cnt"])]
        got = [(m, pl.ds(w["row0"] + small_blk * m, small_blk), None) for m in range(w["shared"])]
        for j in range(w["quads"]):
            got += [(w["shared"] + groups * j + p, pl.ds(w["quad0"] + quad * j, quad), p) for p in range(groups)]
        return got

    hops = lambda h, dr: hops_far if h == dr else hops_near
    rs = {}

    def rs_send(i, h, dr, s):
        w = waves[i]
        length = hops(h, dr)
        step = length - s + 1
        dest = zmod(z + step) if dr == 0 else zmod(z - step)
        d2d_wait(i, step if dr == 0 else nz - step)
        sl = w["halves"][h]
        val = gp[dest, c, sl, :] + rx0[dest, sl, :]
        if s > 1:
            rs[i, h, dr, s - 1].wait_recv()
            val = val + rxr[dr, s - 2, sl, :]
        gp[dest, c, sl, :] = val
        where = dev(zmod(z + 1), c) if dr == 0 else dev(zmod(z - 1), c)
        cp = remote(gp.at[dest, c, sl, :], rxr.at[dr, s - 1, sl, :],
                    s_rs.at[i, h * 2 + dr, s - 1], r_rs.at[i, h * 2 + dr, s - 1], where)
        cp.start()
        rs[i, h, dr, s] = cp
        pending.append(cp)

    def rs_finish(i):
        w = waves[i]
        d2d_wait(i, 0)
        for h in range(2):
            sl = w["halves"][h]
            total = gp[z, c, sl, :] + rx0[z, sl, :]
            for dr in range(2):
                last = hops(h, dr)
                rs[i, h, dr, last].wait_recv()
                total = total + rxr[dr, last - 1, sl, :]
            mp[sl, :] = MOMENTUM * mp[sl, :] + total / n
        lane = lax.broadcasted_iota(jnp.int32, (1, LANE), 1)
        part = jnp.zeros((1, LANE), F32)
        for m, where, keep in mat_rows(i):
            block = mp[where, :]
            sq = jnp.sum(block * block, axis=0, keepdims=True)
            if keep is not None:
                sq = jnp.where(lane // in_rows == keep, sq, 0.0)
            part = jnp.where(lane == m, jnp.sum(sq, axis=1, keepdims=True), part)
        nrm[i, me] = part
        for d in others:
            remote(nrm.at[i, me], nrm.at[i, me], s_nrm.at[i], r_nrm.at[i], {"data": d}).start()

    def nrm_wait(i, sem):
        view = nrm.at[i, pl.ds(0, n - 1)]
        pltpu.make_async_copy(view, view, sem).wait()

    def x_copy(i, m):
        w = waves[i]
        owner = (w["base"] + m) % n
        return remote(xtx[i].at[m], rxx[i].at[me], s_x.at[i, m], r_x.at[i], {"data": owner})

    def x_send(i):
        w = waves[i]
        nrm_wait(i, r_nrm.at[i])
        tot = jnp.zeros((1, LANE), F32)
        for d in range(n):
            tot = tot + nrm[i, d]
        lane = lax.broadcasted_iota(jnp.int32, (1, LANE), 1)
        norms = [jnp.sqrt(jnp.sum(jnp.where(lane == m, tot, 0.0), axis=1, keepdims=True)) + NORM_EPS for m in range(w["cnt"])]
        blocks = []
        if w["kind"] == "in":
            for m in range(w["shared"]):
                blocks.append(mp[pl.ds(w["row0"] + small_blk * m, small_blk), :] / norms[m])
            for j in range(w["quads"]):
                m = w["shared"] + groups * j
                norm = norms[m]
                for p in range(1, groups):
                    norm = jnp.where(lane // in_rows == p, norms[m + p], norm)
                x = mp[pl.ds(w["quad0"] + quad * j, quad), :] / norm
                blocks += lane_swap([pad_rows(x[r:r + k], small_blk) for r, k in cuts])
        else:
            for m, where, _ in mat_rows(i):
                x = mp[where, :] / norms[m]
                blocks.append(pad_rows(x, small_blk) if w["kind"] == "out" else x)
        for m, x in enumerate(blocks):
            x = x.astype(BF16)
            xtx[i][m] = x
            owner = (w["base"] + m) % n

            @pl.when(me != owner)
            def _():
                x_copy(i, m).start()

            @pl.when(me == owner)
            def _():
                rxx[i][me] = x

    def owned(i):
        w = waves[i]
        mine = lax.rem(me - w["base"] + n, n)
        return mine, mine < w["cnt"]

    def assemble(i):
        kind = waves[i]["kind"]
        rx = rxx[i]
        if kind == "attn":
            for t in range(tiles):
                xb[:, LANE * t:LANE * (t + 1)] = rx[:, attn_rows * t:attn_rows * (t + 1), :].reshape(n * attn_rows, LANE)
        elif kind == "out":
            for d in range(n):
                blk = rx[d].astype(F32)
                for t in range(tiles):
                    piece = pad_rows(blk[out_rows * t:out_rows * (t + 1)], out_pad)
                    xb[out_pad * d:out_pad * (d + 1), LANE * t:LANE * (t + 1)] = piece.astype(BF16)
        else:
            for t in range(tiles):
                got = lane_swap([rx[groups * t + p].astype(F32) for p in range(groups)])
                for q, (r, k) in enumerate(cuts):
                    xb[r:r + k, LANE * t:LANE * (t + 1)] = got[q][:k].astype(BF16)
            xb[narrow:n * out_pad, :] = jnp.zeros((n * out_pad - narrow, wide), BF16)

    def disassemble(i):
        kind = waves[i]["kind"]
        tx = otx[i]
        if kind == "attn":
            for t in range(tiles):
                tx[:, attn_rows * t:attn_rows * (t + 1), :] = xb[:, LANE * t:LANE * (t + 1)].reshape(n, attn_rows, LANE)
        elif kind == "out":
            for d in range(n):
                blk = xb[out_pad * d:out_pad * (d + 1), :].astype(F32)
                parts = [blk[:out_rows, LANE * t:LANE * (t + 1)] for t in range(tiles)]
                tx[d] = pad_rows(jnp.concatenate(parts, axis=0), small_blk).astype(BF16)
        else:
            for t in range(tiles):
                cols = slice(LANE * t, LANE * (t + 1))
                got = lane_swap([pad_rows(xb[r:r + k, cols].astype(F32), small_blk) for r, k in cuts])
                for p in range(groups):
                    tx[groups * t + p] = got[p].astype(BF16)

    def iterate(size, steps):
        cut = min(size, 256)

        def one(_, carry):
            for r in range(size // cut):
                sl = slice(r * cut, (r + 1) * cut)
                gram = lax.dot_general(xb[sl, :], xb[:size, :], NT, preferred_element_type=F32)
                ab[sl, :size] = gram.astype(BF16)
            for r in range(size // cut):
                sl = slice(r * cut, (r + 1) * cut)
                square = jnp.dot(ab[sl, :size], ab[:size, :size], preferred_element_type=F32)
                bb[sl, :size] = (COEF_B * ab[sl, :size].astype(F32) + COEF_C * square).astype(BF16)
            for r in range(wide // 256):
                sl = slice(r * 256, (r + 1) * 256)
                update = jnp.dot(bb[:size, :size], xb[:size, sl], preferred_element_type=F32)
                xb[:size, sl] = (COEF_A * xb[:size, sl].astype(F32) + update).astype(BF16)
            return carry

        lax.fori_loop(0, steps, one, 0)

    def o_copy(i, mine, d):
        return remote(otx[i].at[d], rxo[i].at[mine], s_o.at[i], r_o.at[i], {"data": d})

    def owner_work(i, begin, steps, end):
        mine, yes = owned(i)

        @pl.when(yes)
        def _():
            if begin:
                view = rxx[i].at[pl.ds(0, n - 1)]
                pltpu.make_async_copy(view, view, r_x.at[i]).wait()
                assemble(i)
            iterate(n * attn_rows if waves[i]["kind"] == "attn" else n * out_pad, steps)
            if end:
                disassemble(i)
                for d in others:
                    o_copy(i, mine, d).start()
                rxo[i][mine] = otx[i][me]

    def master(i):
        w = waves[i]
        mine, yes = owned(i)
        cnt = w["cnt"]

        @pl.when(yes)
        def _():
            view = rxo[i].at[pl.ds(0, cnt - 1)]
            pltpu.make_async_copy(view, view, r_o.at[i]).wait()

        @pl.when(jnp.logical_not(yes))
        def _():
            pltpu.make_async_copy(rxo[i], rxo[i], r_o.at[i]).wait()

        step_scale = 0.2 * math.sqrt(wide)

        def update(where, o):
            old = wp[where, :]
            wp[where, :] = old - LEARN_RATE * (step_scale * o + WEIGHT_DECAY * old)

        if w["kind"] == "in":
            for m in range(w["shared"]):
                update(pl.ds(w["row0"] + small_blk * m, small_blk), rxo[i][m].astype(F32))
            for j in range(w["quads"]):
                m = w["shared"] + groups * j
                got = lane_swap([rxo[i][m + p].astype(F32) for p in range(groups)])
                o = jnp.concatenate([got[q][:k] for q, (r, k) in enumerate(cuts)], axis=0)
                update(pl.ds(w["quad0"] + quad * j, quad), o)
        else:
            for m, where, _ in mat_rows(i):
                o = rxo[i][m].astype(F32)
                update(where, o[:out_blk] if w["kind"] == "out" else o)
        sl = pl.ds(w["row0"], w["rows"])
        ag[z, c, sl, :] = wp[sl, :].astype(BF16)

    agc = {}
    agd = {}

    def ag_rows(i, h):
        return waves[i]["halves"][h]

    def ag_to_partner(i, h, src, key):
        part = ag.at[src, c, ag_rows(i, h), :]
        cp = remote(part, part, s_agd.at[i, h, key], r_agd.at[i, h, key], partner)
        cp.start()
        agd[i, h, key] = cp
        pending.append(cp)

    def ag_send(i, h, dr, s):
        length = hops(h, dr)
        src = z if s == 1 else (zmod(z - (s - 1)) if dr == 0 else zmod(z + (s - 1)))
        if s > 1:
            agc[i, h, dr, s - 1].wait_recv()
        if s <= length:
            part = ag.at[src, c, ag_rows(i, h), :]
            where = dev(zmod(z + 1), c) if dr == 0 else dev(zmod(z - 1), c)
            cp = remote(part, part, s_ag.at[i, h * 2 + dr, s - 1], r_ag.at[i, h * 2 + dr, s - 1], where)
            cp.start()
            agc[i, h, dr, s] = cp
            pending.append(cp)
        if s > 1:
            ag_to_partner(i, h, src, (s - 1) if dr == 0 else nz - (s - 1))
        elif dr == 0:
            ag_to_partner(i, h, src, 0)

    out_copies = []

    def out_copy(src, dst, k):
        cp = pltpu.make_async_copy(src, dst, s_out.at[k])
        cp.start()
        out_copies.append(cp)

    def quad_row(j):
        return waves[1]["quad0"] + quad * j if j < quads_b else waves[2]["quad0"] + quad * (j - quads_b)

    def out_rows_of():
        return [(4, m, out0 + out_blk * m) for m in range(c_eo)] + [(2, m, out0 + out_blk * (c_eo + m)) for m in range(c_so)]

    def native_outputs(which):
        for src, nat, outs in (((mp, nat_m, m_out), (wp, nat_w, w_out))[which],):
            for m in range(c_attn):
                for t in range(tiles):
                    nat[0][m, :, LANE * t:LANE * (t + 1)] = src[pl.ds(m * attn_blk + t * attn_rows, attn_rows), :]
            some = c_si
            off = waves[1]["row0"]
            got = [src[off + small_blk * p:off + small_blk * (p + 1), :] for p in range(some)]
            got += [jnp.zeros((small_blk, LANE), F32)] * (groups - some)
            block = pad_rows(jnp.concatenate(lane_swap(got), axis=0), 2 * LANE).T
            for p in range(some):
                nat[1][p] = block[in_rows * p:in_rows * (p + 1), :narrow]
            for j in range(n_quads):
                block = pad_rows(src[pl.ds(quad_row(j), quad), :], 2 * LANE).T
                for p in range(groups):
                    nat[3][groups * j + p] = block[in_rows * p:in_rows * (p + 1), :narrow]
            for k, m, off in out_rows_of():
                for t in range(tiles):
                    nat[k][:, m, LANE * t:LANE * (t + 1)] = src[off + t * out_rows:off + (t + 1) * out_rows, :]
            for k in range(5):
                out_copy(nat[k], outs[k], which * 5 + k)

    def native_inputs(which):
        for cp in nat_copies()[5 * which:5 * which + 5]:
            cp.wait()
        for nat, dst in (((nat_m, mp), (nat_w, wp))[which],):
            for m in range(c_attn):
                for t in range(tiles):
                    dst[pl.ds(m * attn_blk + t * attn_rows, attn_rows), :] = nat[0][m, :, LANE * t:LANE * (t + 1)]
            wider = lambda x: jnp.concatenate([x, jnp.zeros((LANE, 2 * LANE - narrow), F32)], axis=1)
            block = pad_rows(jnp.concatenate([nat[1][p] for p in range(c_si)], axis=0), LANE)
            block = wider(block).T
            got = lane_swap([block[small_blk * q:small_blk * (q + 1)] for q in range(groups)])
            for p in range(c_si):
                dst[pl.ds(waves[1]["row0"] + small_blk * p, small_blk), :] = got[p]
            for j in range(n_quads):
                block = jnp.concatenate([nat[3][groups * j + p] for p in range(groups)], axis=0)
                dst[pl.ds(quad_row(j), quad), :] = wider(block).T[:quad]
            for k, m, off in out_rows_of():
                rows = [nat[k][:, m, LANE * t:LANE * (t + 1)] for t in range(tiles)]
                dst[pl.ds(off, out_blk), :] = jnp.concatenate(rows, axis=0)
            spare = rows_d - c_out * out_blk
            if spare:
                dst[pl.ds(out0 + c_out * out_blk, spare), :] = jnp.zeros((spare, LANE), F32)

    def unpack(i):
        w = waves[i]
        for h in range(2):
            for key in range(nz):
                agd[i, h, key].wait_recv()
        if w["kind"] == "attn":
            for m in range(c_attn):
                for t in range(tiles):
                    out_copies.append(pltpu.make_async_copy(
                        ag.at[:, :, pl.ds(m * attn_blk + t * attn_rows, attn_rows), :],
                        p_attn.at[m, :, :, :, pl.ds(LANE * t, LANE)], s_out.at[10 + m * tiles + t]))
                    out_copies[-1].start()
        elif w["kind"] == "in":
            for j in range(w["shared"]):
                sl = pl.ds(w["row0"] + small_blk * j, small_blk)
                for t in range(tiles):
                    devs = [groups * t + p for p in range(groups)]
                    got = lane_swap([ag[d // 2, d % 2, sl, :].astype(F32) for d in devs])
                    for q, (r, k) in enumerate(cuts):
                        stage_in[j, r:r + k, LANE * t:LANE * (t + 1)] = got[q][:k].astype(BF16)

            def body(j, carry):
                off = pl.multiple_of(w["quad0"] + quad * j, 16)
                first = c_si + groups * (w["first"] + j)
                for t in range(tiles):
                    devs = [groups * t + p for p in range(groups)]
                    got = lane_swap([ag[d // 2, d % 2, pl.ds(off, quad), :].astype(F32) for d in devs])
                    for p in range(groups):
                        stage_in[first + p, :, LANE * t:LANE * (t + 1)] = got[p].astype(BF16)
                return carry

            lax.fori_loop(0, w["quads"], body, 0)
            k = 10 + c_attn * tiles
            if w["shared"]:
                out_copy(stage_in.at[pl.ds(0, c_si)], p_si, k)
            first, cnt = groups * w["first"], groups * w["quads"]
            out_copy(stage_in.at[pl.ds(c_si + first, cnt)], p_ei.at[pl.ds(first, cnt)], k + 1 + (w["first"] > 0))
        else:
            def put(blk, m, first, d):
                for t in range(tiles):
                    r = out_blk * m + t * out_rows
                    raw_out[first + m, out_rows * d:out_rows * (d + 1), LANE * t:LANE * (t + 1)] = blk[r:r + out_rows]

            def body(j, carry):
                off = pl.multiple_of(out0 + groups * out_blk * j, 16)
                for d in range(n):
                    blk = ag[d // 2, d % 2, pl.ds(off, groups * out_blk), :].astype(F32)
                    for p in range(groups):
                        put(blk, p, groups * j, d)
                for p in range(groups):
                    stage_out[groups * j + p] = raw_out[groups * j + p].astype(BF16)
                return carry

            lax.fori_loop(0, cut_out, body, 0)
            for d in range(n):
                blk = ag[d // 2, d % 2, pl.ds(out0 + c_eo * out_blk, rows_d - c_eo * out_blk), :].astype(F32)
                for m in range(c_so):
                    put(blk, m, c_eo, d)
            for m in range(c_eo, c_out):
                stage_out[m] = raw_out[m].astype(BF16)
            k = 13 + c_attn * tiles
            out_copy(stage_out.at[pl.ds(c_eo, c_so)], p_so, k)
            out_copy(stage_out.at[pl.ds(0, c_eo)], p_eo, k + 1)

    def both(func, length, i, h, s):
        for dr in range(2):
            if s <= hops(h, dr) + length:
                func(i, h, dr, s)

    def own(i, part):
        begin, steps, end = ((True, NS_STEPS, True), (True, 1, False), (False, 2, False), (False, NS_STEPS - 3, True))[part]
        owner_work(i, begin, steps, end)

    acts = dict(pack=pack, nat=native_inputs, rs=functools.partial(both, rs_send, 0), fin=rs_finish, x=x_send, own=own,
                mas=master, ag=functools.partial(both, ag_send, 1), natout=native_outputs, un=unpack)
    start_loads()
    for name, *where in SCHEDULE:
        acts[name](*where)

    for cp in out_copies:
        cp.wait()
    for cp in pending:
        cp.wait_send()
    for i in range(n_waves):
        for k in range(nz):
            d2d_copy(i, k).wait_send()
        nrm_wait(i, s_nrm.at[i])
        for m in range(waves[i]["cnt"]):
            owner = (waves[i]["base"] + m) % n

            @pl.when(me != owner)
            def _():
                x_copy(i, m).wait_send()
        mine, yes = owned(i)

        @pl.when(yes)
        def _():
            view = otx[i].at[pl.ds(0, n - 1)]
            pltpu.make_async_copy(view, view, s_o.at[i]).wait()


def hand_over(shapes):
    count = len(shapes)
    pieces = []
    for k, x in enumerate(shapes):
        parts = next((p for p in (4, 2) if x.shape[0] % p == 0 and x.size > 400000), 1)
        step = x.shape[0] // parts
        pieces += [(k, p * step, step) for p in range(parts)]

    def kernel(*refs):
        src, dst, buf, sem_in, sem_out = refs[:count], refs[count:2 * count], refs[2 * count:3 * count], refs[-2], refs[-1]
        first = [pltpu.make_async_copy(src[k].at[pl.ds(r, m)], buf[k].at[pl.ds(r, m)], sem_in.at[i])
                 for i, (k, r, m) in enumerate(pieces)]
        second = [pltpu.make_async_copy(buf[k].at[pl.ds(r, m)], dst[k].at[pl.ds(r, m)], sem_out.at[i])
                  for i, (k, r, m) in enumerate(pieces)]
        for cp in first:
            cp.start()
        for one, two in zip(first, second):
            one.wait()
            two.start()
        for cp in second:
            cp.wait()

    any_spec = pl.BlockSpec(memory_space=pl.ANY)
    return pl.pallas_call(
        kernel, out_shape=shapes, in_specs=[any_spec] * count, out_specs=[any_spec] * count,
        scratch_shapes=[pltpu.VMEM(x.shape, x.dtype) for x in shapes]
        + [pltpu.SemaphoreType.DMA((len(pieces),)), pltpu.SemaphoreType.DMA((len(pieces),))],
        name="hand_over")


def solution(mesh):
    n = mesh.shape["data"]
    nz = n // 2

    def local_step(*arrays):
        grads, moms, masters = arrays[:5], arrays[5:10], arrays[10:]
        counts = tuple(m.shape[0] for m in moms)
        attn_rows, wide = moms[0].shape[1:]
        narrow = moms[1].shape[2]
        c_attn, c_si, c_so, c_ei, c_eo = counts
        c_in, c_out = c_si + c_ei, c_so + c_eo
        tiles = wide // LANE
        groups = LANE // (wide // n)
        out_blk = tiles * (narrow // n)
        small_blk = round_up(out_blk, 16)
        out_pad = round_up(narrow // n, 16)
        attn_blk = attn_rows * tiles
        rows = c_attn * attn_blk + c_si * small_blk + c_ei // groups * narrow + round_up(c_out * out_blk, 16)
        mats_b = c_si + groups * (c_ei // groups // 2)
        turn = lambda x: jnp.swapaxes(x, -1, -2)
        grads = [g[0] for g in grads]
        grads[1], grads[3] = turn(grads[1]), turn(grads[3])
        flip = lambda arrs: [jnp.swapaxes(x, 0, 1) if k in (2, 4) else x for k, x in enumerate(arrs)]
        moms, masters = flip(moms), flip(masters)
        grads[0] = grads[0].reshape(c_attn, nz, 2, attn_rows, wide)
        hops = nz // 2

        sds = jax.ShapeDtypeStruct
        out_shape = [sds(m.shape, F32) for m in moms] * 2
        out_shape += [sds((c_attn, nz, 2, attn_rows, wide), BF16)]
        out_shape += [sds((k, narrow, wide), BF16) for k in counts[1:]]
        w_cnt = (c_attn, mats_b, c_in - mats_b, c_out)
        w_blk = (attn_blk, small_blk, small_blk, small_blk)
        dma = lambda *shape: pltpu.SemaphoreType.DMA(shape)
        vm = pltpu.VMEM
        scratch = [
            vm((nz, 2, rows, LANE), F32),
            vm((nz, rows, LANE), F32),
            vm((2, hops, rows, LANE), F32),
            vm((nz, 2, rows, LANE), BF16),
            vm((rows, LANE), F32),
            vm((rows, LANE), F32),
            [vm(m.shape, F32) for m in moms],
            [vm(m.shape, F32) for m in moms],
            vm((4, n, 1, LANE), F32),
            [vm((k, b, LANE), BF16) for k, b in zip(w_cnt, w_blk)],
            [vm((n, b, LANE), BF16) for b in w_blk],
            [vm((n, b, LANE), BF16) for b in w_blk],
            [vm((k, b, LANE), BF16) for k, b in zip(w_cnt, w_blk)],
            vm((n * attn_rows, wide), BF16),
            vm((n * attn_rows, n * attn_rows), BF16),
            vm((n * attn_rows, n * attn_rows), BF16),
            vm((c_in, narrow, wide), F32),
            vm((c_out, narrow, wide), F32),
            vm((c_in, narrow, wide), BF16),
            vm((c_out, narrow, wide), BF16),
            dma(6), dma(2, 5), dma(2, 4, nz), dma(4, 4, hops), dma(4, 4, hops),
            dma(4), dma(4), dma(4, max(w_cnt)), dma(4), dma(4), dma(4),
            dma(4, 4, hops), dma(4, 4, hops), dma(4, 2, nz), dma(4, 2, nz),
            dma(15 + c_attn * tiles),
        ]
        any_spec = pl.BlockSpec(memory_space=pl.ANY)
        call = pl.pallas_call(
            functools.partial(fused_step, n, counts, attn_rows, wide, narrow),
            out_shape=out_shape,
            in_specs=[any_spec] * 15,
            out_specs=[any_spec] * 15,
            scratch_shapes=scratch,
            compiler_params=pltpu.CompilerParams(
                collective_id=0, has_side_effects=True, vmem_limit_bytes=67043328),
            name="muon_step",
        )
        outs = list(hand_over(out_shape)(*call(*grads, *moms, *masters)))
        outs[:5], outs[5:10] = flip(outs[:5]), flip(outs[5:10])
        outs[10] = outs[10].reshape(c_attn, n * attn_rows, wide)
        outs[11], outs[13] = turn(outs[11]), turn(outs[13])
        return tuple(outs)

    grad_spec = P(("stage", "data"), None, None, None)
    row_spec = P("stage", "data", None)
    full_spec = P("stage", None, None)
    in_specs = (grad_spec,) * 5 + (row_spec,) * 10
    out_specs = (row_spec,) * 10 + (full_spec,) * 5
    return jax.shard_map(local_step, mesh=mesh, in_specs=in_specs, out_specs=out_specs, check_vma=False)
```

```python
import functools
import math
import types
import jax
import jax.numpy as jnp
from jax import lax
from jax.experimental import pallas as pl
from jax.experimental.pallas import tpu as pltpu
from jax.sharding import PartitionSpec as P

NS_STEPS = 5
MOMENTUM = 0.95
LEARN_RATE = 0.2
WEIGHT_DECAY = 0.25
NORM_EPS = 1e-7
COEF_A = 3.4445
COEF_B = -4.7750
COEF_C = 2.0315

SCHEDULE = (
    ("pack", 0), ("rs", 0, 0, 1), ("rs", 0, 1, 1), ("pack", 1), ("rs", 1, 1, 1), ("rs", 1, 0, 1), ("rs", 0, 0, 2),
    ("rs", 1, 1, 2), ("rs", 0, 1, 2), ("pack", 2), ("rs", 1, 0, 2), ("rs", 0, 0, 3), ("rs", 1, 0, 3),
    ("rs", 1, 1, 3), ("nat", 0), ("rs", 0, 0, 4), ("rs", 0, 1, 3), ("pack", 3), ("rs", 1, 1, 4), ("rs", 1, 0, 4),
    ("rs", 3, 1, 1), ("rs", 3, 0, 1), ("rs", 0, 1, 4), ("fin", 1), ("rs", 2, 0, 1), ("rs", 3, 1, 2), ("fin", 0),
    ("rs", 2, 1, 1), ("rs", 2, 0, 2), ("rs", 3, 0, 2), ("x", 0), ("x", 1), ("rs", 3, 0, 3), ("rs", 2, 0, 3),
    ("nat", 1), ("rs", 3, 1, 3), ("rs", 2, 1, 2), ("rs", 3, 0, 4), ("own", 0, 1), ("own", 0, 2), ("rs", 2, 0, 4),
    ("own", 0, 3), ("own", 1, 0), ("rs", 2, 1, 3), ("rs", 3, 1, 4), ("rs", 2, 1, 4), ("mas", 1), ("ag", 1, 0, 1),
    ("fin", 3), ("fin", 2), ("mas", 0), ("ag", 1, 1, 1), ("ag", 0, 1, 1), ("ag", 1, 0, 2), ("ag", 1, 1, 2),
    ("x", 2), ("x", 3), ("ag", 0, 1, 2), ("ag", 1, 1, 3), ("ag", 0, 0, 1), ("own", 2, 0), ("ag", 1, 0, 3),
    ("own", 3, 0), ("ag", 0, 0, 2), ("natout", 0), ("ag", 1, 1, 4), ("ag", 0, 1, 3), ("ag", 1, 0, 4), ("mas", 2),
    ("ag", 2, 0, 1), ("ag", 2, 1, 1), ("mas", 3), ("ag", 3, 0, 1), ("ag", 1, 1, 5), ("ag", 3, 1, 1),
    ("ag", 2, 0, 2), ("ag", 2, 1, 2), ("ag", 3, 0, 2), ("natout", 1), ("ag", 3, 1, 2), ("ag", 0, 1, 4),
    ("ag", 1, 0, 5), ("ag", 2, 1, 3), ("ag", 0, 0, 3), ("ag", 2, 0, 3), ("un", 1), ("ag", 3, 1, 3),
    ("ag", 0, 1, 5), ("ag", 3, 0, 3), ("ag", 2, 1, 4), ("ag", 2, 0, 4), ("ag", 0, 0, 4), ("ag", 3, 1, 4),
    ("ag", 3, 0, 4), ("ag", 2, 0, 5), ("ag", 2, 1, 5), ("ag", 0, 0, 5), ("ag", 3, 1, 5), ("ag", 3, 0, 5),
    ("un", 2), ("un", 3), ("un", 0),
)

FIRST_PART = 0.5

F32 = jnp.float32
BF16 = jnp.bfloat16
MESH = pl.DeviceIdType.MESH
LANE = 128
NT = (((1,), (1,)), ((), ()))


def round_up(value, step):
    return (value + step - 1) // step * step


def plan(n, counts, attn_rows, wide, narrow):
    c_attn, c_si, c_so, c_ei, c_eo = counts
    c_in, c_out = c_si + c_ei, c_so + c_eo
    nz = n // 2
    hops_far, hops_near = nz // 2, nz - 1 - nz // 2
    tiles = wide // LANE
    in_rows = wide // n
    groups = LANE // in_rows
    out_rows = narrow // n
    out_pad = round_up(out_rows, 16)
    attn_blk = attn_rows * tiles
    out_blk = tiles * out_rows
    small_blk = round_up(out_blk, 16)
    cuts = [(q * small_blk, min(small_blk, narrow - q * small_blk)) for q in range(groups)]
    quad = narrow
    n_quads = c_ei // groups
    quads_b = n_quads // 2
    mats_b, mats_c = c_si + groups * quads_b, groups * (n_quads - quads_b)
    rows_b, rows_c = c_si * small_blk + quads_b * quad, (n_quads - quads_b) * quad
    rows_d = round_up(c_out * out_blk, 16)
    waves = [dict(kind="attn", cnt=c_attn, rows=c_attn * attn_blk, base=(c_in + c_out) % n),
             dict(kind="in", cnt=mats_b, rows=rows_b, base=0, shared=c_si, quads=quads_b, first=0),
             dict(kind="in", cnt=mats_c, rows=rows_c, base=mats_b % n, shared=0, quads=n_quads - quads_b, first=quads_b),
             dict(kind="out", cnt=c_out, rows=rows_d, base=c_in % n)]
    n_waves = len(waves)
    start = 0
    for w in waves:
        w["row0"] = start
        start += w["rows"]
        split = int(w["rows"] * FIRST_PART / 16 + 0.5) * 16
        w["halves"] = (pl.ds(w["row0"], split), pl.ds(w["row0"] + split, w["rows"] - split))
        w["quad0"] = w["row0"] + w.get("shared", 0) * small_blk
    out0 = waves[3]["row0"]
    cut_in, cut_out = groups * quads_b, c_eo // groups
    return types.SimpleNamespace(**locals())


def lane_swap(blocks):
    groups, in_rows = len(blocks), LANE // len(blocks)
    lane = lax.broadcasted_iota(jnp.int32, (1, LANE), 1)
    blocks = list(blocks)
    dist = groups // 2
    while dist:
        width = dist * in_rows
        low = lax.rem(lane // width, 2) == 0
        for q in range(groups):
            if (q // dist) % 2 == 0:
                x, y = blocks[q], blocks[q + dist]
                if 2 * width == LANE:
                    turned = pltpu.roll(jnp.where(low, y, x), width, axis=1)
                    blocks[q] = jnp.where(low, x, turned)
                    blocks[q + dist] = jnp.where(low, turned, y)
                else:
                    blocks[q] = jnp.where(low, x, pltpu.roll(y, width, axis=1))
                    blocks[q + dist] = jnp.where(low, pltpu.roll(x, LANE - width, axis=1), y)
        dist //= 2
    return blocks

def pad_rows(x, rows):
    if x.shape[0] == rows:
        return x
    return jnp.concatenate([x, jnp.zeros((rows - x.shape[0], x.shape[1]), x.dtype)], axis=0)


def fused_step(n, counts, attn_rows, wide, narrow, *refs):
    g = plan(n, counts, attn_rows, wide, narrow)
    c_attn, c_si, c_so, c_ei, c_eo, c_in, c_out = g.c_attn, g.c_si, g.c_so, g.c_ei, g.c_eo, g.c_in, g.c_out
    nz, hops_far, hops_near, tiles, in_rows, groups, out_rows = g.nz, g.hops_far, g.hops_near, g.tiles, g.in_rows, g.groups, g.out_rows
    out_pad, attn_blk, out_blk, small_blk, cuts, quad, n_quads = g.out_pad, g.attn_blk, g.out_blk, g.small_blk, g.cuts, g.quad, g.n_quads
    quads_b, rows_d, waves, n_waves, out0, cut_in, cut_out = g.quads_b, g.rows_d, g.waves, g.n_waves, g.out0, g.cut_in, g.cut_out

    it = iter(refs)
    take = lambda k: [next(it) for _ in range(k)]
    g_attn, g_si, g_so, g_ei, g_eo = take(5)
    m_in = take(5)
    w_in = take(5)
    m_out = take(5)
    w_out = take(5)
    p_raw, = take(1)
    (gp, rx0, rxr, ag, mp, wp, nat_m, nat_w, nrm, xtx, rxx, otx, rxo, xb, ab, bb,
     raw_in, raw_out) = take(18)
    (s_load, s_nat, s_d2d, s_rs, r_rs, s_nrm, r_nrm, s_x, r_x, s_o, r_o, s_ag, r_ag, s_agd, r_agd, s_out) = take(16)

    me = lax.axis_index("data")
    z = me // 2
    c = lax.rem(me, 2)
    zmod = lambda v: lax.rem(v + 2 * nz, nz)
    dev = lambda zz, cc: {"data": zz * 2 + cc}
    partner = {"data": z * 2 + (1 - c)}
    others = [lax.rem(me + k, n) for k in range(1, n)]

    def remote(src, dst, ss, rs, where):
        return pltpu.make_async_remote_copy(src_ref=src, dst_ref=dst, send_sem=ss, recv_sem=rs,
                                            device_id=where, device_id_type=MESH)

    barrier = pltpu.get_barrier_semaphore()
    for d in others:
        pl.semaphore_signal(barrier, inc=1, device_id={"data": d}, device_id_type=MESH)

    def nat_copies():
        return [pltpu.make_async_copy(srcs[k], dsts[k], s_nat.at[which, k])
                for which, (srcs, dsts) in enumerate(((m_in, nat_m), (w_in, nat_w))) for k in range(5)]


    def loads():
        return [
            pltpu.make_async_copy(g_si, raw_in.at[pl.ds(0, c_si)], s_load.at[1]),
            pltpu.make_async_copy(g_ei.at[pl.ds(0, cut_in)], raw_in.at[pl.ds(c_si, cut_in)], s_load.at[2]),
            pltpu.make_async_copy(g_ei.at[pl.ds(cut_in, c_ei - cut_in)], raw_in.at[pl.ds(c_si + cut_in, c_ei - cut_in)], s_load.at[3]),
            pltpu.make_async_copy(g_so, raw_out.at[pl.ds(c_eo, c_so)], s_load.at[4]),
            pltpu.make_async_copy(g_eo, raw_out.at[pl.ds(0, c_eo)], s_load.at[5]),
        ]

    def start_loads():
        for m in range(c_attn):
            for t in range(tiles):
                pltpu.make_async_copy(
                    g_attn.at[m, :, :, :, pl.ds(LANE * t, LANE)],
                    gp.at[:, :, pl.ds(m * attn_blk + t * attn_rows, attn_rows), :], s_load.at[0]).start()
        for cp in loads() + nat_copies():
            cp.start()

    def pack_in(i):
        w = waves[i]
        for j in range(w["shared"]):
            for t in range(tiles):
                cols = slice(LANE * t, LANE * (t + 1))
                got = lane_swap([pad_rows(raw_in[j, r:r + k, cols], small_blk) for r, k in cuts])
                for p in range(groups):
                    d = groups * t + p
                    gp[d // 2, d % 2, pl.ds(w["row0"] + small_blk * j, small_blk), :] = got[p]

        def body(j, carry):
            off = pl.multiple_of(w["quad0"] + quad * j, 8)
            first = c_si + groups * (w["first"] + j)
            for t in range(tiles):
                got = lane_swap([raw_in[first + p, :, LANE * t:LANE * (t + 1)] for p in range(groups)])
                for p in range(groups):
                    d = groups * t + p
                    gp[d // 2, d % 2, pl.ds(off, quad), :] = got[p]
            return carry

        lax.fori_loop(0, w["quads"], body, 0)

    def out_piece(m, d):
        return [raw_out[m, out_rows * d:out_rows * (d + 1), LANE * t:LANE * (t + 1)] for t in range(tiles)]

    def pack_out():
        def body(j, carry):
            off = pl.multiple_of(out0 + groups * out_blk * j, 8)
            for d in range(n):
                rows = sum([out_piece(groups * j + p, d) for p in range(groups)], [])
                gp[d // 2, d % 2, pl.ds(off, groups * out_blk), :] = jnp.concatenate(rows, axis=0)
            return carry

        lax.fori_loop(0, cut_out, body, 0)
        tail = rows_d - c_eo * out_blk
        for d in range(n):
            rows = sum([out_piece(m, d) for m in range(c_eo, c_out)], [])
            gp[d // 2, d % 2, pl.ds(out0 + c_eo * out_blk, tail), :] = pad_rows(jnp.concatenate(rows, axis=0), tail)

    def pack(i):
        load = loads
        if i == 0:
            view = gp.at[:, :, pl.ds(0, waves[0]["rows"]), :]
            pltpu.make_async_copy(view, view, s_load.at[0]).wait()
            pl.semaphore_wait(barrier, n - 1)
        elif i == 1:
            load()[0].wait()
            load()[1].wait()
            pack_in(1)
        elif i == 2:
            load()[2].wait()
            pack_in(2)
        else:
            load()[3].wait()
            load()[4].wait()
            pack_out()
        for k in near_last:
            d2d_copy(i, k).start()

    pending = []

    near_last = [hops_far]
    for k in range(hops_near, 0, -1):
        near_last += [k, nz - k]
    near_last.append(0)
    d2d_seen = set()

    def d2d_copy(i, k):
        sl = pl.ds(waves[i]["row0"], waves[i]["rows"])
        dest = zmod(z + k)
        return remote(gp.at[dest, 1 - c, sl, :], rx0.at[dest, sl, :], s_d2d.at[0, i, k], s_d2d.at[1, i, k], partner)

    def d2d_wait(i, k):
        if (i, k) not in d2d_seen:
            d2d_seen.add((i, k))
            d2d_copy(i, k).wait_recv()

    def mat_rows(i):
        w = waves[i]
        if w["kind"] == "attn":
            return [(m, pl.ds(attn_blk * m, attn_blk), None) for m in range(w["cnt"])]
        if w["kind"] == "out":
            return [(m, pl.ds(out0 + out_blk * m, out_blk), None) for m in range(w["cnt"])]
        got = [(m, pl.ds(w["row0"] + small_blk * m, small_blk), None) for m in range(w["shared"])]
        for j in range(w["quads"]):
            got += [(w["shared"] + groups * j + p, pl.ds(w["quad0"] + quad * j, quad), p) for p in range(groups)]
        return got

    hops = lambda h, dr: hops_far if h == dr else hops_near
    rs = {}

    def rs_send(i, h, dr, s):
        w = waves[i]
        length = hops(h, dr)
        step = length - s + 1
        dest = zmod(z + step) if dr == 0 else zmod(z - step)
        d2d_wait(i, step if dr == 0 else nz - step)
        sl = w["halves"][h]
        val = gp[dest, c, sl, :] + rx0[dest, sl, :]
        if s > 1:
            rs[i, h, dr, s - 1].wait_recv()
            val = val + rxr[dr, s - 2, sl, :]
        gp[dest, c, sl, :] = val
        where = dev(zmod(z + 1), c) if dr == 0 else dev(zmod(z - 1), c)
        cp = remote(gp.at[dest, c, sl, :], rxr.at[dr, s - 1, sl, :],
                    s_rs.at[i, h * 2 + dr, s - 1], r_rs.at[i, h * 2 + dr, s - 1], where)
        cp.start()
        rs[i, h, dr, s] = cp
        pending.append(cp)

    def rs_finish(i):
        w = waves[i]
        d2d_wait(i, 0)
        for h in range(2):
            sl = w["halves"][h]
            total = gp[z, c, sl, :] + rx0[z, sl, :]
            for dr in range(2):
                last = hops(h, dr)
                rs[i, h, dr, last].wait_recv()
                total = total + rxr[dr, last - 1, sl, :]
            mp[sl, :] = MOMENTUM * mp[sl, :] + total / n
        lane = lax.broadcasted_iota(jnp.int32, (1, LANE), 1)
        part = jnp.zeros((1, LANE), F32)
        for m, where, keep in mat_rows(i):
            block = mp[where, :]
            sq = jnp.sum(block * block, axis=0, keepdims=True)
            if keep is not None:
                sq = jnp.where(lane // in_rows == keep, sq, 0.0)
            part = jnp.where(lane == m, jnp.sum(sq, axis=1, keepdims=True), part)
        nrm[i, me] = part
        for d in others:
            remote(nrm.at[i, me], nrm.at[i, me], s_nrm.at[i], r_nrm.at[i], {"data": d}).start()

    def nrm_wait(i, sem):
        view = nrm.at[i, pl.ds(0, n - 1)]
        pltpu.make_async_copy(view, view, sem).wait()

    def x_copy(i, m):
        w = waves[i]
        owner = (w["base"] + m) % n
        return remote(xtx[i].at[m], rxx[i].at[me], s_x.at[i, m], r_x.at[i], {"data": owner})

    def x_send(i):
        w = waves[i]
        nrm_wait(i, r_nrm.at[i])
        tot = jnp.zeros((1, LANE), F32)
        for d in range(n):
            tot = tot + nrm[i, d]
        lane = lax.broadcasted_iota(jnp.int32, (1, LANE), 1)
        norms = [jnp.sqrt(jnp.sum(jnp.where(lane == m, tot, 0.0), axis=1, keepdims=True)) + NORM_EPS for m in range(w["cnt"])]
        blocks = []
        if w["kind"] == "in":
            for m in range(w["shared"]):
                blocks.append(mp[pl.ds(w["row0"] + small_blk * m, small_blk), :] / norms[m])
            for j in range(w["quads"]):
                m = w["shared"] + groups * j
                norm = norms[m]
                for p in range(1, groups):
                    norm = jnp.where(lane // in_rows == p, norms[m + p], norm)
                x = mp[pl.ds(w["quad0"] + quad * j, quad), :] / norm
                blocks += lane_swap([pad_rows(x[r:r + k], small_blk) for r, k in cuts])
        else:
            for m, where, _ in mat_rows(i):
                x = mp[where, :] / norms[m]
                blocks.append(pad_rows(x, small_blk) if w["kind"] == "out" else x)
        for m, x in enumerate(blocks):
            x = x.astype(BF16)
            xtx[i][m] = x
            owner = (w["base"] + m) % n

            @pl.when(me != owner)
            def _():
                x_copy(i, m).start()

            @pl.when(me == owner)
            def _():
                rxx[i][me] = x

    def owned(i):
        w = waves[i]
        mine = lax.rem(me - w["base"] + n, n)
        return mine, mine < w["cnt"]

    def assemble(i):
        kind = waves[i]["kind"]
        rx = rxx[i]
        if kind == "attn":
            for t in range(tiles):
                xb[:, LANE * t:LANE * (t + 1)] = rx[:, attn_rows * t:attn_rows * (t + 1), :].reshape(n * attn_rows, LANE)
        elif kind == "out":
            for d in range(n):
                blk = rx[d].astype(F32)
                for t in range(tiles):
                    piece = pad_rows(blk[out_rows * t:out_rows * (t + 1)], out_pad)
                    xb[out_pad * d:out_pad * (d + 1), LANE * t:LANE * (t + 1)] = piece.astype(BF16)
        else:
            for t in range(tiles):
                got = lane_swap([rx[groups * t + p].astype(F32) for p in range(groups)])
                for q, (r, k) in enumerate(cuts):
                    xb[r:r + k, LANE * t:LANE * (t + 1)] = got[q][:k].astype(BF16)
            xb[narrow:n * out_pad, :] = jnp.zeros((n * out_pad - narrow, wide), BF16)

    def disassemble(i):
        kind = waves[i]["kind"]
        tx = otx[i]
        if kind == "attn":
            for t in range(tiles):
                tx[:, attn_rows * t:attn_rows * (t + 1), :] = xb[:, LANE * t:LANE * (t + 1)].reshape(n, attn_rows, LANE)
        elif kind == "out":
            for d in range(n):
                blk = xb[out_pad * d:out_pad * (d + 1), :].astype(F32)
                parts = [blk[:out_rows, LANE * t:LANE * (t + 1)] for t in range(tiles)]
                tx[d] = pad_rows(jnp.concatenate(parts, axis=0), small_blk).astype(BF16)
        else:
            for t in range(tiles):
                cols = slice(LANE * t, LANE * (t + 1))
                got = lane_swap([pad_rows(xb[r:r + k, cols].astype(F32), small_blk) for r, k in cuts])
                for p in range(groups):
                    tx[groups * t + p] = got[p].astype(BF16)

    def iterate(size, steps):
        cut = min(size, 256)

        def one(_, carry):
            for r in range(size // cut):
                sl = slice(r * cut, (r + 1) * cut)
                gram = lax.dot_general(xb[sl, :], xb[:size, :], NT, preferred_element_type=F32)
                ab[sl, :size] = gram.astype(BF16)
            for r in range(size // cut):
                sl = slice(r * cut, (r + 1) * cut)
                square = jnp.dot(ab[sl, :size], ab[:size, :size], preferred_element_type=F32)
                bb[sl, :size] = (COEF_B * ab[sl, :size].astype(F32) + COEF_C * square).astype(BF16)
            for r in range(wide // 256):
                sl = slice(r * 256, (r + 1) * 256)
                update = jnp.dot(bb[:size, :size], xb[:size, sl], preferred_element_type=F32)
                xb[:size, sl] = (COEF_A * xb[:size, sl].astype(F32) + update).astype(BF16)
            return carry

        lax.fori_loop(0, steps, one, 0)

    def o_copy(i, mine, d):
        return remote(otx[i].at[d], rxo[i].at[mine], s_o.at[i], r_o.at[i], {"data": d})

    def owner_work(i, begin, steps, end):
        mine, yes = owned(i)

        @pl.when(yes)
        def _():
            if begin:
                view = rxx[i].at[pl.ds(0, n - 1)]
                pltpu.make_async_copy(view, view, r_x.at[i]).wait()
                assemble(i)
            iterate(n * attn_rows if waves[i]["kind"] == "attn" else n * out_pad, steps)
            if end:
                disassemble(i)
                for d in others:
                    o_copy(i, mine, d).start()
                rxo[i][mine] = otx[i][me]

    def master(i):
        w = waves[i]
        mine, yes = owned(i)
        cnt = w["cnt"]

        @pl.when(yes)
        def _():
            view = rxo[i].at[pl.ds(0, cnt - 1)]
            pltpu.make_async_copy(view, view, r_o.at[i]).wait()

        @pl.when(jnp.logical_not(yes))
        def _():
            pltpu.make_async_copy(rxo[i], rxo[i], r_o.at[i]).wait()

        step_scale = 0.2 * math.sqrt(wide)

        def update(where, o):
            old = wp[where, :]
            wp[where, :] = old - LEARN_RATE * (step_scale * o + WEIGHT_DECAY * old)

        if w["kind"] == "in":
            for m in range(w["shared"]):
                update(pl.ds(w["row0"] + small_blk * m, small_blk), rxo[i][m].astype(F32))
            for j in range(w["quads"]):
                m = w["shared"] + groups * j
                got = lane_swap([rxo[i][m + p].astype(F32) for p in range(groups)])
                o = jnp.concatenate([got[q][:k] for q, (r, k) in enumerate(cuts)], axis=0)
                update(pl.ds(w["quad0"] + quad * j, quad), o)
        else:
            for m, where, _ in mat_rows(i):
                o = rxo[i][m].astype(F32)
                update(where, o[:out_blk] if w["kind"] == "out" else o)
        sl = pl.ds(w["row0"], w["rows"])
        ag[z, c, sl, :] = wp[sl, :].astype(BF16)

    agc = {}
    agd = {}

    def ag_rows(i, h):
        return waves[i]["halves"][h]

    def ag_to_partner(i, h, src, key):
        part = ag.at[src, c, ag_rows(i, h), :]
        cp = remote(part, part, s_agd.at[i, h, key], r_agd.at[i, h, key], partner)
        cp.start()
        agd[i, h, key] = cp
        pending.append(cp)

    def ag_send(i, h, dr, s):
        length = hops(h, dr)
        src = z if s == 1 else (zmod(z - (s - 1)) if dr == 0 else zmod(z + (s - 1)))
        if s > 1:
            agc[i, h, dr, s - 1].wait_recv()
        if s <= length:
            part = ag.at[src, c, ag_rows(i, h), :]
            where = dev(zmod(z + 1), c) if dr == 0 else dev(zmod(z - 1), c)
            cp = remote(part, part, s_ag.at[i, h * 2 + dr, s - 1], r_ag.at[i, h * 2 + dr, s - 1], where)
            cp.start()
            agc[i, h, dr, s] = cp
            pending.append(cp)
        if s > 1:
            ag_to_partner(i, h, src, (s - 1) if dr == 0 else nz - (s - 1))
        elif dr == 0:
            ag_to_partner(i, h, src, 0)

    out_copies = []

    def out_copy(src, dst, k):
        cp = pltpu.make_async_copy(src, dst, s_out.at[k])
        cp.start()
        out_copies.append(cp)

    def quad_row(j):
        return waves[1]["quad0"] + quad * j if j < quads_b else waves[2]["quad0"] + quad * (j - quads_b)

    def out_rows_of():
        return [(4, m, out0 + out_blk * m) for m in range(c_eo)] + [(2, m, out0 + out_blk * (c_eo + m)) for m in range(c_so)]

    def native_outputs(which):
        for src, nat, outs in (((mp, nat_m, m_out), (wp, nat_w, w_out))[which],):
            for m in range(c_attn):
                for t in range(tiles):
                    nat[0][m, :, LANE * t:LANE * (t + 1)] = src[pl.ds(m * attn_blk + t * attn_rows, attn_rows), :]
            some = c_si
            off = waves[1]["row0"]
            got = [src[off + small_blk * p:off + small_blk * (p + 1), :] for p in range(some)]
            got += [jnp.zeros((small_blk, LANE), F32)] * (groups - some)
            block = pad_rows(jnp.concatenate(lane_swap(got), axis=0), 2 * LANE).T
            for p in range(some):
                nat[1][p] = block[in_rows * p:in_rows * (p + 1), :narrow]
            for j in range(n_quads):
                block = pad_rows(src[pl.ds(quad_row(j), quad), :], 2 * LANE).T
                for p in range(groups):
                    nat[3][groups * j + p] = block[in_rows * p:in_rows * (p + 1), :narrow]
            for k, m, off in out_rows_of():
                for t in range(tiles):
                    nat[k][:, m, LANE * t:LANE * (t + 1)] = src[off + t * out_rows:off + (t + 1) * out_rows, :]
            for k in range(5):
                out_copy(nat[k], outs[k], which * 5 + k)

    def native_inputs(which):
        for cp in nat_copies()[5 * which:5 * which + 5]:
            cp.wait()
        for nat, dst in (((nat_m, mp), (nat_w, wp))[which],):
            for m in range(c_attn):
                for t in range(tiles):
                    dst[pl.ds(m * attn_blk + t * attn_rows, attn_rows), :] = nat[0][m, :, LANE * t:LANE * (t + 1)]
            wider = lambda x: jnp.concatenate([x, jnp.zeros((LANE, 2 * LANE - narrow), F32)], axis=1)
            block = pad_rows(jnp.concatenate([nat[1][p] for p in range(c_si)], axis=0), LANE)
            block = wider(block).T
            got = lane_swap([block[small_blk * q:small_blk * (q + 1)] for q in range(groups)])
            for p in range(c_si):
                dst[pl.ds(waves[1]["row0"] + small_blk * p, small_blk), :] = got[p]
            for j in range(n_quads):
                block = jnp.concatenate([nat[3][groups * j + p] for p in range(groups)], axis=0)
                dst[pl.ds(quad_row(j), quad), :] = wider(block).T[:quad]
            for k, m, off in out_rows_of():
                rows = [nat[k][:, m, LANE * t:LANE * (t + 1)] for t in range(tiles)]
                dst[pl.ds(off, out_blk), :] = jnp.concatenate(rows, axis=0)
            spare = rows_d - c_out * out_blk
            if spare:
                dst[pl.ds(out0 + c_out * out_blk, spare), :] = jnp.zeros((spare, LANE), F32)

    def unpack(i):
        w = waves[i]
        for h in range(2):
            for key in range(nz):
                agd[i, h, key].wait_recv()
        sl = pl.ds(w["row0"], w["rows"])
        out_copy(ag.at[:, :, sl, :], p_raw.at[:, :, sl, :], 10 + i)

    def both(func, length, i, h, s):
        for dr in range(2):
            if s <= hops(h, dr) + length:
                func(i, h, dr, s)

    def own(i, part):
        begin, steps, end = ((True, NS_STEPS, True), (True, 1, False), (False, 2, False), (False, NS_STEPS - 3, True))[part]
        owner_work(i, begin, steps, end)

    acts = dict(pack=pack, nat=native_inputs, rs=functools.partial(both, rs_send, 0), fin=rs_finish, x=x_send, own=own,
                mas=master, ag=functools.partial(both, ag_send, 1), natout=native_outputs, un=unpack)
    start_loads()
    for name, *where in SCHEDULE:
        acts[name](*where)

    for cp in out_copies:
        cp.wait()
    for cp in pending:
        cp.wait_send()
    for i in range(n_waves):
        for k in range(nz):
            d2d_copy(i, k).wait_send()
        nrm_wait(i, s_nrm.at[i])
        for m in range(waves[i]["cnt"]):
            owner = (waves[i]["base"] + m) % n

            @pl.when(me != owner)
            def _():
                x_copy(i, m).wait_send()
        mine, yes = owned(i)

        @pl.when(yes)
        def _():
            view = otx[i].at[pl.ds(0, n - 1)]
            pltpu.make_async_copy(view, view, s_o.at[i]).wait()


def hand_over(g, shapes, params, raw):
    n, count = g.n, len(shapes)
    c_attn, c_si, c_so, c_ei, c_eo = g.counts
    nz, tiles, groups, cuts, attn_rows, attn_blk, out_rows, out_blk = (
        g.nz, g.tiles, g.groups, g.cuts, g.attn_rows, g.attn_blk, g.out_rows, g.out_blk)
    small_blk, quad, out0, rows_d, cut_out, c_in, c_out = g.small_blk, g.quad, g.out0, g.rows_d, g.cut_out, g.c_in, g.c_out
    n_out = count + c_attn * tiles + 5

    def kernel(*refs):
        src, raw_ref = refs[:count], refs[count]
        dst = refs[count + 1:2 * count + 1]
        p_attn, p_si, p_so, p_ei, p_eo = refs[2 * count + 1:2 * count + 6]
        bufs = refs[2 * count + 6:3 * count + 6]
        ag, raw_out, stage_in, stage_out, s_in, s_out = refs[3 * count + 6:]
        out_copies = []

        def out_copy(a, b, k):
            out_copies.append(pltpu.make_async_copy(a, b, s_out.at[k]))
            out_copies[-1].start()

        first = []
        for i in (1, 2, 3, 0):
            sl = pl.ds(g.waves[i]["row0"], g.waves[i]["rows"])
            first.append((i, pltpu.make_async_copy(raw_ref.at[:, :, sl, :], ag.at[:, :, sl, :], s_in.at[count + i])))
            first[-1][1].start()
        plain = [pltpu.make_async_copy(src[k], bufs[k], s_in.at[k]) for k in range(count)]
        for cp in plain:
            cp.start()
        for i, cp in first:
            w = g.waves[i]
            cp.wait()
            if w["kind"] == "attn":
                for m in range(c_attn):
                    for t in range(tiles):
                        out_copies.append(pltpu.make_async_copy(
                            ag.at[:, :, pl.ds(m * attn_blk + t * attn_rows, attn_rows), :],
                            p_attn.at[m, :, :, :, pl.ds(LANE * t, LANE)], s_out.at[len(shapes) + m * tiles + t]))
                        out_copies[-1].start()
            elif w["kind"] == "in":
                for j in range(w["shared"]):
                    sl = pl.ds(w["row0"] + small_blk * j, small_blk)
                    for t in range(tiles):
                        devs = [groups * t + p for p in range(groups)]
                        got = lane_swap([ag[d // 2, d % 2, sl, :].astype(F32) for d in devs])
                        for q, (r, k) in enumerate(cuts):
                            stage_in[j, r:r + k, LANE * t:LANE * (t + 1)] = got[q][:k].astype(BF16)

                def body(j, carry):
                    off = pl.multiple_of(w["quad0"] + quad * j, 16)
                    first = c_si + groups * (w["first"] + j)
                    for t in range(tiles):
                        devs = [groups * t + p for p in range(groups)]
                        got = lane_swap([ag[d // 2, d % 2, pl.ds(off, quad), :].astype(F32) for d in devs])
                        for p in range(groups):
                            stage_in[first + p, :, LANE * t:LANE * (t + 1)] = got[p].astype(BF16)
                    return carry

                lax.fori_loop(0, w["quads"], body, 0)
                k = len(shapes) + c_attn * tiles
                if w["shared"]:
                    out_copy(stage_in.at[pl.ds(0, c_si)], p_si, k)
                first, cnt = groups * w["first"], groups * w["quads"]
                out_copy(stage_in.at[pl.ds(c_si + first, cnt)], p_ei.at[pl.ds(first, cnt)], k + 1 + (w["first"] > 0))
            else:
                def put(blk, m, first, d):
                    for t in range(tiles):
                        r = out_blk * m + t * out_rows
                        raw_out[first + m, out_rows * d:out_rows * (d + 1), LANE * t:LANE * (t + 1)] = blk[r:r + out_rows]

                def body(j, carry):
                    off = pl.multiple_of(out0 + groups * out_blk * j, 16)
                    for d in range(n):
                        blk = ag[d // 2, d % 2, pl.ds(off, groups * out_blk), :].astype(F32)
                        for p in range(groups):
                            put(blk, p, groups * j, d)
                    for p in range(groups):
                        stage_out[groups * j + p] = raw_out[groups * j + p].astype(BF16)
                    return carry

                lax.fori_loop(0, cut_out, body, 0)
                for d in range(n):
                    blk = ag[d // 2, d % 2, pl.ds(out0 + c_eo * out_blk, rows_d - c_eo * out_blk), :].astype(F32)
                    for m in range(c_so):
                        put(blk, m, c_eo, d)
                for m in range(c_eo, c_out):
                    stage_out[m] = raw_out[m].astype(BF16)
                k = len(shapes) + 3 + c_attn * tiles
                out_copy(stage_out.at[pl.ds(c_eo, c_so)], p_so, k)
                out_copy(stage_out.at[pl.ds(0, c_eo)], p_eo, k + 1)
        for k in range(count):
            plain[k].wait()
            out_copy(bufs[k], dst[k], k)
        for cp in out_copies:
            cp.wait()

    any_spec = pl.BlockSpec(memory_space=pl.ANY)
    vm = pltpu.VMEM
    return pl.pallas_call(
        kernel, out_shape=shapes + params, in_specs=[any_spec] * (count + 1), out_specs=[any_spec] * (count + len(params)),
        scratch_shapes=[vm(x.shape, x.dtype) for x in shapes]
        + [vm(raw.shape, BF16), vm((c_out, g.narrow, g.wide), F32), vm((c_in, g.narrow, g.wide), BF16),
           vm((c_out, g.narrow, g.wide), BF16)]
        + [pltpu.SemaphoreType.DMA((count + 4,)), pltpu.SemaphoreType.DMA((n_out,))],
        name="hand_over")


def solution(mesh):
    n = mesh.shape["data"]
    nz = n // 2

    def local_step(*arrays):
        grads, moms, masters = arrays[:5], arrays[5:10], arrays[10:]
        counts = tuple(m.shape[0] for m in moms)
        attn_rows, wide = moms[0].shape[1:]
        narrow = moms[1].shape[2]
        c_attn, c_si, c_so, c_ei, c_eo = counts
        c_in, c_out = c_si + c_ei, c_so + c_eo
        tiles = wide // LANE
        groups = LANE // (wide // n)
        out_blk = tiles * (narrow // n)
        small_blk = round_up(out_blk, 16)
        out_pad = round_up(narrow // n, 16)
        attn_blk = attn_rows * tiles
        rows = c_attn * attn_blk + c_si * small_blk + c_ei // groups * narrow + round_up(c_out * out_blk, 16)
        mats_b = c_si + groups * (c_ei // groups // 2)
        turn = lambda x: jnp.swapaxes(x, -1, -2)
        grads = [g[0] for g in grads]
        grads[1], grads[3] = turn(grads[1]), turn(grads[3])
        flip = lambda arrs: [jnp.swapaxes(x, 0, 1) if k in (2, 4) else x for k, x in enumerate(arrs)]
        moms, masters = flip(moms), flip(masters)
        grads[0] = grads[0].reshape(c_attn, nz, 2, attn_rows, wide)
        hops = nz // 2

        sds = jax.ShapeDtypeStruct
        out_shape = [sds(m.shape, F32) for m in moms] * 2
        params = [sds((c_attn, nz, 2, attn_rows, wide), BF16)] + [sds((k, narrow, wide), BF16) for k in counts[1:]]
        raw = sds((nz, 2, rows, LANE), BF16)
        w_cnt = (c_attn, mats_b, c_in - mats_b, c_out)
        w_blk = (attn_blk, small_blk, small_blk, small_blk)
        dma = lambda *shape: pltpu.SemaphoreType.DMA(shape)
        vm = pltpu.VMEM
        scratch = [
            vm((nz, 2, rows, LANE), F32),
            vm((nz, rows, LANE), F32),
            vm((2, hops, rows, LANE), F32),
            vm((nz, 2, rows, LANE), BF16),
            vm((rows, LANE), F32),
            vm((rows, LANE), F32),
            [vm(m.shape, F32) for m in moms],
            [vm(m.shape, F32) for m in moms],
            vm((4, n, 1, LANE), F32),
            [vm((k, b, LANE), BF16) for k, b in zip(w_cnt, w_blk)],
            [vm((n, b, LANE), BF16) for b in w_blk],
            [vm((n, b, LANE), BF16) for b in w_blk],
            [vm((k, b, LANE), BF16) for k, b in zip(w_cnt, w_blk)],
            vm((n * attn_rows, wide), BF16),
            vm((n * attn_rows, n * attn_rows), BF16),
            vm((n * attn_rows, n * attn_rows), BF16),
            vm((c_in, narrow, wide), F32),
            vm((c_out, narrow, wide), F32),
            dma(6), dma(2, 5), dma(2, 4, nz), dma(4, 4, hops), dma(4, 4, hops),
            dma(4), dma(4), dma(4, max(w_cnt)), dma(4), dma(4), dma(4),
            dma(4, 4, hops), dma(4, 4, hops), dma(4, 2, nz), dma(4, 2, nz),
            dma(14),
        ]
        any_spec = pl.BlockSpec(memory_space=pl.ANY)
        call = pl.pallas_call(
            functools.partial(fused_step, n, counts, attn_rows, wide, narrow),
            out_shape=out_shape + [raw],
            in_specs=[any_spec] * 15,
            out_specs=[any_spec] * 11,
            scratch_shapes=scratch,
            compiler_params=pltpu.CompilerParams(
                collective_id=0, has_side_effects=True, vmem_limit_bytes=67043328),
            name="muon_step",
        )
        outs = list(hand_over(plan(n, counts, attn_rows, wide, narrow), out_shape, params, raw)(*call(*grads, *moms, *masters)))
        outs[:5], outs[5:10] = flip(outs[:5]), flip(outs[5:10])
        outs[10] = outs[10].reshape(c_attn, n * attn_rows, wide)
        outs[11], outs[13] = turn(outs[11]), turn(outs[13])
        return tuple(outs)

    grad_spec = P(("stage", "data"), None, None, None)
    row_spec = P("stage", "data", None)
    full_spec = P("stage", None, None)
    in_specs = (grad_spec,) * 5 + (row_spec,) * 10
    out_specs = (row_spec,) * 10 + (full_spec,) * 5
    return jax.shard_map(local_step, mesh=mesh, in_specs=in_specs, out_specs=out_specs, check_vma=False)
```

```python
import functools
import math
import types
import jax
import jax.numpy as jnp
from jax import lax
from jax.experimental import pallas as pl
from jax.experimental.pallas import tpu as pltpu
from jax.sharding import PartitionSpec as P

NS_STEPS = 5
MOMENTUM = 0.95
LEARN_RATE = 0.2
WEIGHT_DECAY = 0.25
NORM_EPS = 1e-7
COEF_A = 3.4445
COEF_B = -4.7750
COEF_C = 2.0315

SCHEDULE = (
    ("pack", 0), ("rs", 0, 0, 1), ("rs", 0, 1, 1), ("pack", 1), ("rs", 1, 0, 1), ("rs", 0, 0, 2), ("rs", 0, 1, 2),
    ("rs", 1, 1, 1), ("rs", 0, 0, 3), ("rs", 1, 0, 2), ("pack", 2), ("nat", 0), ("rs", 1, 1, 2), ("rs", 2, 1, 1),
    ("rs", 1, 0, 3), ("rs", 1, 1, 3), ("pack", 3), ("rs", 3, 0, 1), ("rs", 1, 0, 4), ("rs", 0, 0, 4),
    ("rs", 0, 1, 3), ("rs", 2, 1, 2), ("rs", 3, 1, 1), ("rs", 0, 1, 4), ("rs", 2, 0, 1), ("rs", 1, 1, 4),
    ("fin", 0), ("rs", 3, 0, 2), ("nat", 1), ("rs", 2, 1, 3), ("fin", 1), ("rs", 2, 0, 2), ("x", 0),
    ("rs", 3, 1, 2), ("rs", 2, 1, 4), ("rs", 2, 0, 3), ("x", 1), ("rs", 3, 0, 3), ("own", 0, 1), ("rs", 3, 1, 3),
    ("own", 0, 2), ("own", 0, 3), ("rs", 2, 0, 4), ("own", 1, 0), ("rs", 3, 0, 4), ("rs", 3, 1, 4), ("fin", 2),
    ("mas", 1), ("ag", 1, 1, 1), ("mas", 0), ("ag", 0, 0, 1), ("fin", 3), ("ag", 0, 1, 1), ("ag", 1, 0, 1),
    ("ag", 0, 0, 2), ("x", 2), ("x", 3), ("ag", 1, 1, 2), ("ag", 1, 0, 2), ("ag", 0, 1, 2), ("ag", 0, 0, 3),
    ("own", 2, 0), ("own", 3, 0), ("ag", 1, 1, 3), ("ag", 1, 0, 3), ("ag", 0, 1, 3), ("ag", 1, 1, 4),
    ("ag", 0, 0, 4), ("mas", 2), ("mas", 3), ("ag", 3, 1, 1), ("ag", 2, 1, 1), ("natout", 0), ("ag", 3, 0, 1),
    ("ag", 2, 0, 1), ("natout", 1), ("ag", 0, 1, 4), ("ag", 3, 1, 2), ("ag", 2, 1, 2), ("ag", 1, 0, 4),
    ("ag", 0, 0, 5), ("ag", 3, 0, 2), ("ag", 1, 1, 5), ("ag", 2, 0, 2), ("ag", 0, 1, 5), ("ag", 1, 0, 5),
    ("ag", 3, 1, 3), ("ag", 3, 0, 3), ("ag", 2, 1, 3), ("ag", 2, 0, 3), ("un", 1), ("ag", 3, 1, 4),
    ("ag", 3, 0, 4), ("ag", 2, 0, 4), ("ag", 2, 1, 4), ("un", 0), ("ag", 3, 1, 5), ("ag", 3, 0, 5),
    ("ag", 2, 0, 5), ("ag", 2, 1, 5), ("un", 3), ("un", 2),
)

FIRST_PART = 0.5

F32 = jnp.float32
BF16 = jnp.bfloat16
MESH = pl.DeviceIdType.MESH
LANE = 128
NT = (((1,), (1,)), ((), ()))


def round_up(value, step):
    return (value + step - 1) // step * step


def plan(n, counts, attn_rows, wide, narrow):
    c_attn, c_si, c_so, c_ei, c_eo = counts
    c_in, c_out = c_si + c_ei, c_so + c_eo
    nz = n // 2
    hops_far, hops_near = nz // 2, nz - 1 - nz // 2
    tiles = wide // LANE
    in_rows = wide // n
    groups = LANE // in_rows
    out_rows = narrow // n
    out_pad = round_up(out_rows, 16)
    attn_blk = attn_rows * tiles
    out_blk = tiles * out_rows
    small_blk = round_up(out_blk, 16)
    cuts = [(q * small_blk, min(small_blk, narrow - q * small_blk)) for q in range(groups)]
    quad = narrow
    n_quads = c_ei // groups
    quads_b = n_quads // 2
    mats_b, mats_c = c_si + groups * quads_b, groups * (n_quads - quads_b)
    rows_b, rows_c = c_si * small_blk + quads_b * quad, (n_quads - quads_b) * quad
    rows_d = round_up(c_out * out_blk, 16)
    waves = [dict(kind="attn", cnt=c_attn, rows=c_attn * attn_blk, base=(c_in + c_out) % n),
             dict(kind="in", cnt=mats_b, rows=rows_b, base=0, shared=c_si, quads=quads_b, first=0),
             dict(kind="in", cnt=mats_c, rows=rows_c, base=mats_b % n, shared=0, quads=n_quads - quads_b, first=quads_b),
             dict(kind="out", cnt=c_out, rows=rows_d, base=c_in % n)]
    n_waves = len(waves)
    start = 0
    for w in waves:
        w["row0"] = start
        start += w["rows"]
        split = int(w["rows"] * FIRST_PART / 16 + 0.5) * 16
        w["halves"] = (pl.ds(w["row0"], split), pl.ds(w["row0"] + split, w["rows"] - split))
        w["quad0"] = w["row0"] + w.get("shared", 0) * small_blk
    out0 = waves[3]["row0"]
    cut_in, cut_out = groups * quads_b, c_eo // groups
    return types.SimpleNamespace(**locals())


def lane_swap(blocks):
    groups, in_rows = len(blocks), LANE // len(blocks)
    lane = lax.broadcasted_iota(jnp.int32, (1, LANE), 1)
    blocks = list(blocks)
    dist = groups // 2
    while dist:
        width = dist * in_rows
        low = lax.rem(lane // width, 2) == 0
        for q in range(groups):
            if (q // dist) % 2 == 0:
                x, y = blocks[q], blocks[q + dist]
                if 2 * width == LANE:
                    turned = pltpu.roll(jnp.where(low, y, x), width, axis=1)
                    blocks[q] = jnp.where(low, x, turned)
                    blocks[q + dist] = jnp.where(low, turned, y)
                else:
                    blocks[q] = jnp.where(low, x, pltpu.roll(y, width, axis=1))
                    blocks[q + dist] = jnp.where(low, pltpu.roll(x, LANE - width, axis=1), y)
        dist //= 2
    return blocks

def pad_rows(x, rows):
    if x.shape[0] == rows:
        return x
    return jnp.concatenate([x, jnp.zeros((rows - x.shape[0], x.shape[1]), x.dtype)], axis=0)


def fused_step(n, counts, attn_rows, wide, narrow, *refs):
    g = plan(n, counts, attn_rows, wide, narrow)
    c_attn, c_si, c_so, c_ei, c_eo, c_in, c_out = g.c_attn, g.c_si, g.c_so, g.c_ei, g.c_eo, g.c_in, g.c_out
    nz, hops_far, hops_near, tiles, in_rows, groups, out_rows = g.nz, g.hops_far, g.hops_near, g.tiles, g.in_rows, g.groups, g.out_rows
    out_pad, attn_blk, out_blk, small_blk, cuts, quad, n_quads = g.out_pad, g.attn_blk, g.out_blk, g.small_blk, g.cuts, g.quad, g.n_quads
    quads_b, rows_d, waves, n_waves, out0, cut_in, cut_out = g.quads_b, g.rows_d, g.waves, g.n_waves, g.out0, g.cut_in, g.cut_out

    it = iter(refs)
    take = lambda k: [next(it) for _ in range(k)]
    g_attn, g_si, g_so, g_ei, g_eo = take(5)
    m_in = take(5)
    w_in = take(5)
    m_out = take(5)
    w_out = take(5)
    p_raw, = take(1)
    (gp, rx0, rxr, ag, mp, wp, nat_m, nat_w, nrm, xtx, rxx, otx, rxo, xb, ab, bb,
     raw_in, raw_out) = take(18)
    (s_load, s_nat, s_d2d, s_rs, r_rs, s_nrm, r_nrm, s_x, r_x, s_o, r_o, s_ag, r_ag, s_agd, r_agd, s_out) = take(16)

    me = lax.axis_index("data")
    z = me // 2
    c = lax.rem(me, 2)
    zmod = lambda v: lax.rem(v + 2 * nz, nz)
    dev = lambda zz, cc: {"data": zz * 2 + cc}
    partner = {"data": z * 2 + (1 - c)}
    others = [lax.rem(me + k, n) for k in range(1, n)]

    def remote(src, dst, ss, rs, where):
        return pltpu.make_async_remote_copy(src_ref=src, dst_ref=dst, send_sem=ss, recv_sem=rs,
                                            device_id=where, device_id_type=MESH)

    barrier = pltpu.get_barrier_semaphore()
    for d in others:
        pl.semaphore_signal(barrier, inc=1, device_id={"data": d}, device_id_type=MESH)

    def nat_copies():
        return [pltpu.make_async_copy(srcs[k], dsts[k], s_nat.at[which, k])
                for which, (srcs, dsts) in enumerate(((m_in, nat_m), (w_in, nat_w))) for k in range(5)]


    def loads():
        return [
            pltpu.make_async_copy(g_si, raw_in.at[pl.ds(0, c_si)], s_load.at[1]),
            pltpu.make_async_copy(g_ei.at[pl.ds(0, cut_in)], raw_in.at[pl.ds(c_si, cut_in)], s_load.at[2]),
            pltpu.make_async_copy(g_ei.at[pl.ds(cut_in, c_ei - cut_in)], raw_in.at[pl.ds(c_si + cut_in, c_ei - cut_in)], s_load.at[3]),
            pltpu.make_async_copy(g_so, raw_out.at[pl.ds(c_eo, c_so)], s_load.at[4]),
            pltpu.make_async_copy(g_eo, raw_out.at[pl.ds(0, c_eo)], s_load.at[5]),
        ]

    def start_loads():
        for m in range(c_attn):
            for t in range(tiles):
                pltpu.make_async_copy(
                    g_attn.at[m, :, :, :, pl.ds(LANE * t, LANE)],
                    gp.at[:, :, pl.ds(m * attn_blk + t * attn_rows, attn_rows), :], s_load.at[0]).start()
        for cp in loads() + nat_copies():
            cp.start()

    def pack_in(i):
        w = waves[i]
        for j in range(w["shared"]):
            for t in range(tiles):
                cols = slice(LANE * t, LANE * (t + 1))
                got = lane_swap([pad_rows(raw_in[j, r:r + k, cols], small_blk) for r, k in cuts])
                for p in range(groups):
                    d = groups * t + p
                    gp[d // 2, d % 2, pl.ds(w["row0"] + small_blk * j, small_blk), :] = got[p]

        def body(j, carry):
            off = pl.multiple_of(w["quad0"] + quad * j, 8)
            first = c_si + groups * (w["first"] + j)
            for t in range(tiles):
                got = lane_swap([raw_in[first + p, :, LANE * t:LANE * (t + 1)] for p in range(groups)])
                for p in range(groups):
                    d = groups * t + p
                    gp[d // 2, d % 2, pl.ds(off, quad), :] = got[p]
            return carry

        lax.fori_loop(0, w["quads"], body, 0)

    def out_piece(m, d):
        return [raw_out[m, out_rows * d:out_rows * (d + 1), LANE * t:LANE * (t + 1)] for t in range(tiles)]

    def pack_out():
        def body(j, carry):
            off = pl.multiple_of(out0 + groups * out_blk * j, 8)
            for d in range(n):
                rows = sum([out_piece(groups * j + p, d) for p in range(groups)], [])
                gp[d // 2, d % 2, pl.ds(off, groups * out_blk), :] = jnp.concatenate(rows, axis=0)
            return carry

        lax.fori_loop(0, cut_out, body, 0)
        tail = rows_d - c_eo * out_blk
        for d in range(n):
            rows = sum([out_piece(m, d) for m in range(c_eo, c_out)], [])
            gp[d // 2, d % 2, pl.ds(out0 + c_eo * out_blk, tail), :] = pad_rows(jnp.concatenate(rows, axis=0), tail)

    def pack(i):
        load = loads
        if i == 0:
            view = gp.at[:, :, pl.ds(0, waves[0]["rows"]), :]
            pltpu.make_async_copy(view, view, s_load.at[0]).wait()
            pl.semaphore_wait(barrier, n - 1)
        elif i == 1:
            load()[0].wait()
            load()[1].wait()
            pack_in(1)
        elif i == 2:
            load()[2].wait()
            pack_in(2)
        else:
            load()[3].wait()
            load()[4].wait()
            pack_out()
        for k in near_last:
            d2d_copy(i, k).start()

    pending = []

    near_last = [hops_far]
    for k in range(hops_near, 0, -1):
        near_last += [k, nz - k]
    near_last.append(0)
    d2d_seen = set()

    def d2d_copy(i, k):
        sl = pl.ds(waves[i]["row0"], waves[i]["rows"])
        dest = zmod(z + k)
        return remote(gp.at[dest, 1 - c, sl, :], rx0.at[dest, sl, :], s_d2d.at[0, i, k], s_d2d.at[1, i, k], partner)

    def d2d_wait(i, k):
        if (i, k) not in d2d_seen:
            d2d_seen.add((i, k))
            d2d_copy(i, k).wait_recv()

    def mat_rows(i):
        w = waves[i]
        if w["kind"] == "attn":
            return [(m, pl.ds(attn_blk * m, attn_blk), None) for m in range(w["cnt"])]
        if w["kind"] == "out":
            return [(m, pl.ds(out0 + out_blk * m, out_blk), None) for m in range(w["cnt"])]
        got = [(m, pl.ds(w["row0"] + small_blk * m, small_blk), None) for m in range(w["shared"])]
        for j in range(w["quads"]):
            got += [(w["shared"] + groups * j + p, pl.ds(w["quad0"] + quad * j, quad), p) for p in range(groups)]
        return got

    hops = lambda h, dr: hops_far if h == dr else hops_near
    rs = {}

    def rs_send(i, h, dr, s):
        w = waves[i]
        length = hops(h, dr)
        step = length - s + 1
        dest = zmod(z + step) if dr == 0 else zmod(z - step)
        d2d_wait(i, step if dr == 0 else nz - step)
        sl = w["halves"][h]
        val = gp[dest, c, sl, :] + rx0[dest, sl, :]
        if s > 1:
            rs[i, h, dr, s - 1].wait_recv()
            val = val + rxr[dr, s - 2, sl, :]
        gp[dest, c, sl, :] = val
        where = dev(zmod(z + 1), c) if dr == 0 else dev(zmod(z - 1), c)
        cp = remote(gp.at[dest, c, sl, :], rxr.at[dr, s - 1, sl, :],
                    s_rs.at[i, h * 2 + dr, s - 1], r_rs.at[i, h * 2 + dr, s - 1], where)
        cp.start()
        rs[i, h, dr, s] = cp
        pending.append(cp)

    def rs_finish(i):
        w = waves[i]
        d2d_wait(i, 0)
        for h in range(2):
            sl = w["halves"][h]
            total = gp[z, c, sl, :] + rx0[z, sl, :]
            for dr in range(2):
                last = hops(h, dr)
                rs[i, h, dr, last].wait_recv()
                total = total + rxr[dr, last - 1, sl, :]
            mp[sl, :] = MOMENTUM * mp[sl, :] + total / n
        lane = lax.broadcasted_iota(jnp.int32, (1, LANE), 1)
        part = jnp.zeros((1, LANE), F32)
        for m, where, keep in mat_rows(i):
            block = mp[where, :]
            sq = jnp.sum(block * block, axis=0, keepdims=True)
            if keep is not None:
                sq = jnp.where(lane // in_rows == keep, sq, 0.0)
            part = jnp.where(lane == m, jnp.sum(sq, axis=1, keepdims=True), part)
        nrm[i, me] = part
        for d in others:
            remote(nrm.at[i, me], nrm.at[i, me], s_nrm.at[i], r_nrm.at[i], {"data": d}).start()

    def nrm_wait(i, sem):
        view = nrm.at[i, pl.ds(0, n - 1)]
        pltpu.make_async_copy(view, view, sem).wait()

    def x_copy(i, m):
        w = waves[i]
        owner = (w["base"] + m) % n
        return remote(xtx[i].at[m], rxx[i].at[me], s_x.at[i, m], r_x.at[i], {"data": owner})

    def x_send(i):
        w = waves[i]
        nrm_wait(i, r_nrm.at[i])
        tot = jnp.zeros((1, LANE), F32)
        for d in range(n):
            tot = tot + nrm[i, d]
        lane = lax.broadcasted_iota(jnp.int32, (1, LANE), 1)
        norms = [jnp.sqrt(jnp.sum(jnp.where(lane == m, tot, 0.0), axis=1, keepdims=True)) + NORM_EPS for m in range(w["cnt"])]
        blocks = []
        if w["kind"] == "in":
            for m in range(w["shared"]):
                blocks.append(mp[pl.ds(w["row0"] + small_blk * m, small_blk), :] / norms[m])
            for j in range(w["quads"]):
                m = w["shared"] + groups * j
                norm = norms[m]
                for p in range(1, groups):
                    norm = jnp.where(lane // in_rows == p, norms[m + p], norm)
                x = mp[pl.ds(w["quad0"] + quad * j, quad), :] / norm
                blocks += lane_swap([pad_rows(x[r:r + k], small_blk) for r, k in cuts])
        else:
            for m, where, _ in mat_rows(i):
                x = mp[where, :] / norms[m]
                blocks.append(pad_rows(x, small_blk) if w["kind"] == "out" else x)
        for m, x in enumerate(blocks):
            x = x.astype(BF16)
            xtx[i][m] = x
            owner = (w["base"] + m) % n

            @pl.when(me != owner)
            def _():
                x_copy(i, m).start()

            @pl.when(me == owner)
            def _():
                rxx[i][me] = x

    def owned(i):
        w = waves[i]
        mine = lax.rem(me - w["base"] + n, n)
        return mine, mine < w["cnt"]

    def assemble(i):
        kind = waves[i]["kind"]
        rx = rxx[i]
        if kind == "attn":
            for t in range(tiles):
                xb[:, LANE * t:LANE * (t + 1)] = rx[:, attn_rows * t:attn_rows * (t + 1), :].reshape(n * attn_rows, LANE)
        elif kind == "out":
            for d in range(n):
                blk = rx[d].astype(F32)
                for t in range(tiles):
                    piece = pad_rows(blk[out_rows * t:out_rows * (t + 1)], out_pad)
                    xb[out_pad * d:out_pad * (d + 1), LANE * t:LANE * (t + 1)] = piece.astype(BF16)
        else:
            for t in range(tiles):
                got = lane_swap([rx[groups * t + p].astype(F32) for p in range(groups)])
                for q, (r, k) in enumerate(cuts):
                    xb[r:r + k, LANE * t:LANE * (t + 1)] = got[q][:k].astype(BF16)
            xb[narrow:n * out_pad, :] = jnp.zeros((n * out_pad - narrow, wide), BF16)

    def disassemble(i):
        kind = waves[i]["kind"]
        tx = otx[i]
        if kind == "attn":
            for t in range(tiles):
                tx[:, attn_rows * t:attn_rows * (t + 1), :] = xb[:, LANE * t:LANE * (t + 1)].reshape(n, attn_rows, LANE)
        elif kind == "out":
            for d in range(n):
                blk = xb[out_pad * d:out_pad * (d + 1), :].astype(F32)
                parts = [blk[:out_rows, LANE * t:LANE * (t + 1)] for t in range(tiles)]
                tx[d] = pad_rows(jnp.concatenate(parts, axis=0), small_blk).astype(BF16)
        else:
            for t in range(tiles):
                cols = slice(LANE * t, LANE * (t + 1))
                got = lane_swap([pad_rows(xb[r:r + k, cols].astype(F32), small_blk) for r, k in cuts])
                for p in range(groups):
                    tx[groups * t + p] = got[p].astype(BF16)

    def iterate(size, steps):
        cut = min(size, 256)

        def one(_, carry):
            for r in range(size // cut):
                sl = slice(r * cut, (r + 1) * cut)
                gram = lax.dot_general(xb[sl, :], xb[:size, :], NT, preferred_element_type=F32)
                ab[sl, :size] = gram.astype(BF16)
            for r in range(size // cut):
                sl = slice(r * cut, (r + 1) * cut)
                square = jnp.dot(ab[sl, :size], ab[:size, :size], preferred_element_type=F32)
                bb[sl, :size] = (COEF_B * ab[sl, :size].astype(F32) + COEF_C * square).astype(BF16)
            for r in range(wide // 256):
                sl = slice(r * 256, (r + 1) * 256)
                update = jnp.dot(bb[:size, :size], xb[:size, sl], preferred_element_type=F32)
                xb[:size, sl] = (COEF_A * xb[:size, sl].astype(F32) + update).astype(BF16)
            return carry

        lax.fori_loop(0, steps, one, 0)

    def o_copy(i, mine, d):
        return remote(otx[i].at[d], rxo[i].at[mine], s_o.at[i], r_o.at[i], {"data": d})

    def owner_work(i, begin, steps, end):
        mine, yes = owned(i)

        @pl.when(yes)
        def _():
            if begin:
                view = rxx[i].at[pl.ds(0, n - 1)]
                pltpu.make_async_copy(view, view, r_x.at[i]).wait()
                assemble(i)
            iterate(n * attn_rows if waves[i]["kind"] == "attn" else n * out_pad, steps)
            if end:
                disassemble(i)
                for d in others:
                    o_copy(i, mine, d).start()
                rxo[i][mine] = otx[i][me]

    def master(i):
        w = waves[i]
        mine, yes = owned(i)
        cnt = w["cnt"]

        @pl.when(yes)
        def _():
            view = rxo[i].at[pl.ds(0, cnt - 1)]
            pltpu.make_async_copy(view, view, r_o.at[i]).wait()

        @pl.when(jnp.logical_not(yes))
        def _():
            pltpu.make_async_copy(rxo[i], rxo[i], r_o.at[i]).wait()

        step_scale = 0.2 * math.sqrt(wide)

        def update(where, o):
            old = wp[where, :]
            wp[where, :] = old - LEARN_RATE * (step_scale * o + WEIGHT_DECAY * old)

        if w["kind"] == "in":
            for m in range(w["shared"]):
                update(pl.ds(w["row0"] + small_blk * m, small_blk), rxo[i][m].astype(F32))
            for j in range(w["quads"]):
                m = w["shared"] + groups * j
                got = lane_swap([rxo[i][m + p].astype(F32) for p in range(groups)])
                o = jnp.concatenate([got[q][:k] for q, (r, k) in enumerate(cuts)], axis=0)
                update(pl.ds(w["quad0"] + quad * j, quad), o)
        else:
            for m, where, _ in mat_rows(i):
                o = rxo[i][m].astype(F32)
                update(where, o[:out_blk] if w["kind"] == "out" else o)
        sl = pl.ds(w["row0"], w["rows"])
        ag[z, c, sl, :] = wp[sl, :].astype(BF16)

    agc = {}
    agd = {}

    def ag_rows(i, h):
        return waves[i]["halves"][h]

    def ag_to_partner(i, h, src, key):
        part = ag.at[src, c, ag_rows(i, h), :]
        cp = remote(part, part, s_agd.at[i, h, key], r_agd.at[i, h, key], partner)
        cp.start()
        agd[i, h, key] = cp
        pending.append(cp)

    def ag_send(i, h, dr, s):
        length = hops(h, dr)
        src = z if s == 1 else (zmod(z - (s - 1)) if dr == 0 else zmod(z + (s - 1)))
        if s > 1:
            agc[i, h, dr, s - 1].wait_recv()
        if s <= length:
            part = ag.at[src, c, ag_rows(i, h), :]
            where = dev(zmod(z + 1), c) if dr == 0 else dev(zmod(z - 1), c)
            cp = remote(part, part, s_ag.at[i, h * 2 + dr, s - 1], r_ag.at[i, h * 2 + dr, s - 1], where)
            cp.start()
            agc[i, h, dr, s] = cp
            pending.append(cp)
        if s > 1:
            ag_to_partner(i, h, src, (s - 1) if dr == 0 else nz - (s - 1))
        elif dr == 0:
            ag_to_partner(i, h, src, 0)

    out_copies = []

    def out_copy(src, dst, k):
        cp = pltpu.make_async_copy(src, dst, s_out.at[k])
        cp.start()
        out_copies.append(cp)

    def quad_row(j):
        return waves[1]["quad0"] + quad * j if j < quads_b else waves[2]["quad0"] + quad * (j - quads_b)

    def out_rows_of():
        return [(4, m, out0 + out_blk * m) for m in range(c_eo)] + [(2, m, out0 + out_blk * (c_eo + m)) for m in range(c_so)]

    def native_outputs(which):
        for src, nat, outs in (((mp, nat_m, m_out), (wp, nat_w, w_out))[which],):
            for m in range(c_attn):
                for t in range(tiles):
                    nat[0][m, :, LANE * t:LANE * (t + 1)] = src[pl.ds(m * attn_blk + t * attn_rows, attn_rows), :]
            some = c_si
            off = waves[1]["row0"]
            got = [src[off + small_blk * p:off + small_blk * (p + 1), :] for p in range(some)]
            got += [jnp.zeros((small_blk, LANE), F32)] * (groups - some)
            block = pad_rows(jnp.concatenate(lane_swap(got), axis=0), 2 * LANE).T
            for p in range(some):
                nat[1][p] = block[in_rows * p:in_rows * (p + 1), :narrow]
            for j in range(n_quads):
                block = pad_rows(src[pl.ds(quad_row(j), quad), :], 2 * LANE).T
                for p in range(groups):
                    nat[3][groups * j + p] = block[in_rows * p:in_rows * (p + 1), :narrow]
            for k, m, off in out_rows_of():
                for t in range(tiles):
                    nat[k][:, m, LANE * t:LANE * (t + 1)] = src[off + t * out_rows:off + (t + 1) * out_rows, :]
            for k in range(5):
                out_copy(nat[k], outs[k], which * 5 + k)

    def native_inputs(which):
        for cp in nat_copies()[5 * which:5 * which + 5]:
            cp.wait()
        for nat, dst in (((nat_m, mp), (nat_w, wp))[which],):
            for m in range(c_attn):
                for t in range(tiles):
                    dst[pl.ds(m * attn_blk + t * attn_rows, attn_rows), :] = nat[0][m, :, LANE * t:LANE * (t + 1)]
            wider = lambda x: jnp.concatenate([x, jnp.zeros((LANE, 2 * LANE - narrow), F32)], axis=1)
            block = pad_rows(jnp.concatenate([nat[1][p] for p in range(c_si)], axis=0), LANE)
            block = wider(block).T
            got = lane_swap([block[small_blk * q:small_blk * (q + 1)] for q in range(groups)])
            for p in range(c_si):
                dst[pl.ds(waves[1]["row0"] + small_blk * p, small_blk), :] = got[p]
            for j in range(n_quads):
                block = jnp.concatenate([nat[3][groups * j + p] for p in range(groups)], axis=0)
                dst[pl.ds(quad_row(j), quad), :] = wider(block).T[:quad]
            for k, m, off in out_rows_of():
                rows = [nat[k][:, m, LANE * t:LANE * (t + 1)] for t in range(tiles)]
                dst[pl.ds(off, out_blk), :] = jnp.concatenate(rows, axis=0)
            spare = rows_d - c_out * out_blk
            if spare:
                dst[pl.ds(out0 + c_out * out_blk, spare), :] = jnp.zeros((spare, LANE), F32)

    def unpack(i):
        w = waves[i]
        for h in range(2):
            for key in range(nz):
                agd[i, h, key].wait_recv()
        sl = pl.ds(w["row0"], w["rows"])
        out_copy(ag.at[:, :, sl, :], p_raw.at[:, :, sl, :], 10 + i)

    def both(func, length, i, h, s):
        for dr in range(2):
            if s <= hops(h, dr) + length:
                func(i, h, dr, s)

    def own(i, part):
        begin, steps, end = ((True, NS_STEPS, True), (True, 1, False), (False, 2, False), (False, NS_STEPS - 3, True))[part]
        owner_work(i, begin, steps, end)

    acts = dict(pack=pack, nat=native_inputs, rs=functools.partial(both, rs_send, 0), fin=rs_finish, x=x_send, own=own,
                mas=master, ag=functools.partial(both, ag_send, 1), natout=native_outputs, un=unpack)
    start_loads()
    for name, *where in SCHEDULE:
        acts[name](*where)

    for cp in out_copies:
        cp.wait()
    for cp in pending:
        cp.wait_send()
    for i in range(n_waves):
        for k in range(nz):
            d2d_copy(i, k).wait_send()
        nrm_wait(i, s_nrm.at[i])
        for m in range(waves[i]["cnt"]):
            owner = (waves[i]["base"] + m) % n

            @pl.when(me != owner)
            def _():
                x_copy(i, m).wait_send()
        mine, yes = owned(i)

        @pl.when(yes)
        def _():
            view = otx[i].at[pl.ds(0, n - 1)]
            pltpu.make_async_copy(view, view, s_o.at[i]).wait()


def hand_over(g, shapes, params, raw):
    n, count = g.n, len(shapes)
    c_attn, c_si, c_so, c_ei, c_eo = g.counts
    nz, tiles, groups, cuts, attn_rows, attn_blk, out_rows, out_blk = (
        g.nz, g.tiles, g.groups, g.cuts, g.attn_rows, g.attn_blk, g.out_rows, g.out_blk)
    small_blk, quad, out0, rows_d, cut_out, c_in, c_out = g.small_blk, g.quad, g.out0, g.rows_d, g.cut_out, g.c_in, g.c_out
    n_out = count + c_attn * tiles + 5

    def kernel(*refs):
        src, raw_ref = refs[:count], refs[count]
        dst = refs[count + 1:2 * count + 1]
        p_attn, p_si, p_so, p_ei, p_eo = refs[2 * count + 1:2 * count + 6]
        bufs = refs[2 * count + 6:3 * count + 6]
        ag, raw_out, stage_in, stage_out, s_in, s_out = refs[3 * count + 6:]
        out_copies = []

        def out_copy(a, b, k):
            out_copies.append(pltpu.make_async_copy(a, b, s_out.at[k]))
            out_copies[-1].start()

        first = []
        for i in (1, 2, 3, 0):
            sl = pl.ds(g.waves[i]["row0"], g.waves[i]["rows"])
            first.append((i, pltpu.make_async_copy(raw_ref.at[:, :, sl, :], ag.at[:, :, sl, :], s_in.at[count + i])))
            first[-1][1].start()
        plain = [pltpu.make_async_copy(src[k], bufs[k], s_in.at[k]) for k in range(count)]
        for cp in plain:
            cp.start()
        for i, cp in first:
            w = g.waves[i]
            cp.wait()
            if w["kind"] == "attn":
                for m in range(c_attn):
                    for t in range(tiles):
                        out_copies.append(pltpu.make_async_copy(
                            ag.at[:, :, pl.ds(m * attn_blk + t * attn_rows, attn_rows), :],
                            p_attn.at[m, :, :, :, pl.ds(LANE * t, LANE)], s_out.at[len(shapes) + m * tiles + t]))
                        out_copies[-1].start()
            elif w["kind"] == "in":
                for j in range(w["shared"]):
                    sl = pl.ds(w["row0"] + small_blk * j, small_blk)
                    for t in range(tiles):
                        devs = [groups * t + p for p in range(groups)]
                        got = lane_swap([ag[d // 2, d % 2, sl, :].astype(F32) for d in devs])
                        for q, (r, k) in enumerate(cuts):
                            stage_in[j, r:r + k, LANE * t:LANE * (t + 1)] = got[q][:k].astype(BF16)

                def body(j, carry):
                    off = pl.multiple_of(w["quad0"] + quad * j, 16)
                    first = c_si + groups * (w["first"] + j)
                    for t in range(tiles):
                        devs = [groups * t + p for p in range(groups)]
                        got = lane_swap([ag[d // 2, d % 2, pl.ds(off, quad), :].astype(F32) for d in devs])
                        for p in range(groups):
                            stage_in[first + p, :, LANE * t:LANE * (t + 1)] = got[p].astype(BF16)
                    return carry

                lax.fori_loop(0, w["quads"], body, 0)
                k = len(shapes) + c_attn * tiles
                if w["shared"]:
                    out_copy(stage_in.at[pl.ds(0, c_si)], p_si, k)
                first, cnt = groups * w["first"], groups * w["quads"]
                out_copy(stage_in.at[pl.ds(c_si + first, cnt)], p_ei.at[pl.ds(first, cnt)], k + 1 + (w["first"] > 0))
            else:
                def put(blk, m, first, d):
                    for t in range(tiles):
                        r = out_blk * m + t * out_rows
                        raw_out[first + m, out_rows * d:out_rows * (d + 1), LANE * t:LANE * (t + 1)] = blk[r:r + out_rows]

                def body(j, carry):
                    off = pl.multiple_of(out0 + groups * out_blk * j, 16)
                    for d in range(n):
                        blk = ag[d // 2, d % 2, pl.ds(off, groups * out_blk), :].astype(F32)
                        for p in range(groups):
                            put(blk, p, groups * j, d)
                    for p in range(groups):
                        stage_out[groups * j + p] = raw_out[groups * j + p].astype(BF16)
                    return carry

                lax.fori_loop(0, cut_out, body, 0)
                for d in range(n):
                    blk = ag[d // 2, d % 2, pl.ds(out0 + c_eo * out_blk, rows_d - c_eo * out_blk), :].astype(F32)
                    for m in range(c_so):
                        put(blk, m, c_eo, d)
                for m in range(c_eo, c_out):
                    stage_out[m] = raw_out[m].astype(BF16)
                k = len(shapes) + 3 + c_attn * tiles
                out_copy(stage_out.at[pl.ds(c_eo, c_so)], p_so, k)
                out_copy(stage_out.at[pl.ds(0, c_eo)], p_eo, k + 1)
        for k in range(count):
            plain[k].wait()
            out_copy(bufs[k], dst[k], k)
        for cp in out_copies:
            cp.wait()

    any_spec = pl.BlockSpec(memory_space=pl.ANY)
    vm = pltpu.VMEM
    return pl.pallas_call(
        kernel, out_shape=shapes + params, in_specs=[any_spec] * (count + 1), out_specs=[any_spec] * (count + len(params)),
        scratch_shapes=[vm(x.shape, x.dtype) for x in shapes]
        + [vm(raw.shape, BF16), vm((c_out, g.narrow, g.wide), F32), vm((c_in, g.narrow, g.wide), BF16),
           vm((c_out, g.narrow, g.wide), BF16)]
        + [pltpu.SemaphoreType.DMA((count + 4,)), pltpu.SemaphoreType.DMA((n_out,))],
        name="hand_over")


def solution(mesh):
    n = mesh.shape["data"]
    nz = n // 2

    def local_step(*arrays):
        grads, moms, masters = arrays[:5], arrays[5:10], arrays[10:]
        counts = tuple(m.shape[0] for m in moms)
        attn_rows, wide = moms[0].shape[1:]
        narrow = moms[1].shape[2]
        c_attn, c_si, c_so, c_ei, c_eo = counts
        c_in, c_out = c_si + c_ei, c_so + c_eo
        tiles = wide // LANE
        groups = LANE // (wide // n)
        out_blk = tiles * (narrow // n)
        small_blk = round_up(out_blk, 16)
        out_pad = round_up(narrow // n, 16)
        attn_blk = attn_rows * tiles
        rows = c_attn * attn_blk + c_si * small_blk + c_ei // groups * narrow + round_up(c_out * out_blk, 16)
        mats_b = c_si + groups * (c_ei // groups // 2)
        turn = lambda x: jnp.swapaxes(x, -1, -2)
        grads = [g[0] for g in grads]
        grads[1], grads[3] = turn(grads[1]), turn(grads[3])
        flip = lambda arrs: [jnp.swapaxes(x, 0, 1) if k in (2, 4) else x for k, x in enumerate(arrs)]
        moms, masters = flip(moms), flip(masters)
        grads[0] = grads[0].reshape(c_attn, nz, 2, attn_rows, wide)
        hops = nz // 2

        sds = jax.ShapeDtypeStruct
        out_shape = [sds(m.shape, F32) for m in moms] * 2
        params = [sds((c_attn, nz, 2, attn_rows, wide), BF16)] + [sds((k, narrow, wide), BF16) for k in counts[1:]]
        raw = sds((nz, 2, rows, LANE), BF16)
        w_cnt = (c_attn, mats_b, c_in - mats_b, c_out)
        w_blk = (attn_blk, small_blk, small_blk, small_blk)
        dma = lambda *shape: pltpu.SemaphoreType.DMA(shape)
        vm = pltpu.VMEM
        scratch = [
            vm((nz, 2, rows, LANE), F32),
            vm((nz, rows, LANE), F32),
            vm((2, hops, rows, LANE), F32),
            vm((nz, 2, rows, LANE), BF16),
            vm((rows, LANE), F32),
            vm((rows, LANE), F32),
            [vm(m.shape, F32) for m in moms],
            [vm(m.shape, F32) for m in moms],
            vm((4, n, 1, LANE), F32),
            [vm((k, b, LANE), BF16) for k, b in zip(w_cnt, w_blk)],
            [vm((n, b, LANE), BF16) for b in w_blk],
            [vm((n, b, LANE), BF16) for b in w_blk],
            [vm((k, b, LANE), BF16) for k, b in zip(w_cnt, w_blk)],
            vm((n * attn_rows, wide), BF16),
            vm((n * attn_rows, n * attn_rows), BF16),
            vm((n * attn_rows, n * attn_rows), BF16),
            vm((c_in, narrow, wide), F32),
            vm((c_out, narrow, wide), F32),
            dma(6), dma(2, 5), dma(2, 4, nz), dma(4, 4, hops), dma(4, 4, hops),
            dma(4), dma(4), dma(4, max(w_cnt)), dma(4), dma(4), dma(4),
            dma(4, 4, hops), dma(4, 4, hops), dma(4, 2, nz), dma(4, 2, nz),
            dma(14),
        ]
        any_spec = pl.BlockSpec(memory_space=pl.ANY)
        call = pl.pallas_call(
            functools.partial(fused_step, n, counts, attn_rows, wide, narrow),
            out_shape=out_shape + [raw],
            in_specs=[any_spec] * 15,
            out_specs=[any_spec] * 11,
            scratch_shapes=scratch,
            compiler_params=pltpu.CompilerParams(
                collective_id=0, has_side_effects=True, vmem_limit_bytes=67043328),
            name="muon_step",
        )
        outs = list(hand_over(plan(n, counts, attn_rows, wide, narrow), out_shape, params, raw)(*call(*grads, *moms, *masters)))
        outs[:5], outs[5:10] = flip(outs[:5]), flip(outs[5:10])
        outs[10] = outs[10].reshape(c_attn, n * attn_rows, wide)
        outs[11], outs[13] = turn(outs[11]), turn(outs[13])
        return tuple(outs)

    grad_spec = P(("stage", "data"), None, None, None)
    row_spec = P("stage", "data", None)
    full_spec = P("stage", None, None)
    in_specs = (grad_spec,) * 5 + (row_spec,) * 10
    out_specs = (row_spec,) * 10 + (full_spec,) * 5
    return jax.shard_map(local_step, mesh=mesh, in_specs=in_specs, out_specs=out_specs, check_vma=False)
```
